32 devices in a mesh: dp: 8 (over y, x, core), expert: 4 (over z).
Axes of the slice: x: 2, y: 2, z: 4, core: 2. Of those that a mesh axis runs over, the one named last changes fastest.
Arguments:
- inputs: bfloat16 [2, 6304, 384], P(None, ('dp', 'expert')), may hold values from -6 to 6
- first_gain: float32 [384], replicated, may hold values from 0.25 to 1.75
- w_qkv: bfloat16 [384, 1152], replicated, may hold values from -0.3125 to 0.3125
- w_attn: bfloat16 [384, 384], replicated, may hold values from -1.75 to 1.75
- second_gain: float32 [384], replicated, may hold values from 0.25 to 1.75
- w_router: bfloat16 [384, 16], replicated, may hold values from -0.625 to 0.625
- expert_in: bfloat16 [16, 384, 1536], P('expert'), may hold values from -0.3125 to 0.3125
- expert_out: bfloat16 [16, 1536, 384], P('expert'), may hold values from -2.5 to 2.5
- expert_ids: int32 [2, 6304, 2], P(None, ('dp', 'expert')), may hold values from 0 to 15, as said below
- slot_ids: int32 [2, 6304, 2], P(None, ('dp', 'expert')), may hold values from 0 to 15, as said below
- dropped: int32 [2, 6304, 2], P(None, ('dp', 'expert')), may hold values from 0 to 1, as said below
- out_grad: bfloat16 [2, 6304, 384], P(None, ('dp', 'expert')), may hold values from -6 to 6
Outputs:
- block_out: float32 [2, 6304, 384], P(None, ('dp', 'expert'))
- input_grad: float32 [2, 6304, 384], P(None, ('dp', 'expert'))
- first_gain_grad: float32 [384], replicated
- w_qkv_grad: float32 [384, 1152], replicated
- w_attn_grad: float32 [384, 384], replicated
- second_gain_grad: float32 [384], replicated
- w_router_grad: float32 [384, 16], replicated
- expert_in_grad: float32 [16, 384, 1536], P('expert', None, 'dp')
- expert_out_grad: float32 [16, 1536, 384], P('expert', 'dp')
The draws below stay inside these ranges and needn't reach their ends.
Inputs may be any that keep to these rules, and one draw needn't show every extreme that they name: `expert_ids`: the two experts of a token differ. `slot_ids`: in each micro-batch and each device's block of 197 tokens, the pairs are taken in order (first choices of all tokens in token order, then second choices); a pair gets the number of earlier pairs of the block naming its expert as slot if that is under 16, else it is dropped and has slot 0. `dropped`: 1 exactly where the pair's expert already had 16 pairs of the block before it.
All inputs are finite; a program needn't handle non-finite values.
Results may differ from the reference program's by a relative error of at most 0.015.
The reference program's roundings to bfloat16 on the way count: a program that leaves them out, or rounds other values in their place, can miss the bound.
Values may be sent and summed in bfloat16 or wider, within the bound.
A program may use at most 128 MiB of HBM per device.

```python
import jax
import jax.numpy as jnp
from jax import lax

D = 384
HEADS = 6
HD = 64
FF = 1536
SEQ = 197
IMG = 1
MB = 2
EXPERTS = 16
TOKB = 197
CAP = 16
TOKENS = 6304
N_EXPERT = 4


def routing_tables(base_key):
    blocks = TOKENS // TOKB
    id_parts = []
    slot_parts = []
    drop_parts = []
    for micro_idx in range(MB):
        micro_key = jax.random.fold_in(base_key, 101 + micro_idx)
        order_key, first_key, shift_key = jax.random.split(micro_key, 3)
        key_left, key_right = jax.random.split(first_key)
        ranking = jax.random.permutation(order_key, EXPERTS).astype(jnp.int32)
        first_raw = jnp.minimum(jax.random.randint(key_left, (blocks, TOKB), 0, EXPERTS), jax.random.randint(key_right, (blocks, TOKB), 0, EXPERTS)).astype(jnp.int32)
        position = jnp.arange(TOKB, dtype=jnp.int32)[None, :]
        first_raw = jnp.where(position < CAP, 0, first_raw)
        second_raw = (first_raw + jax.random.randint(shift_key, (blocks, TOKB), 1, EXPERTS).astype(jnp.int32)) % EXPERTS
        chosen = ranking[jnp.stack([first_raw, second_raw], axis=-1)]
        ordered = jnp.transpose(chosen, (0, 2, 1)).reshape(blocks, 2 * TOKB)
        onehot = (ordered[:, :, None] == jnp.arange(EXPERTS, dtype=jnp.int32)[None, None, :]).astype(jnp.int32)
        before = jnp.cumsum(onehot, axis=1) - onehot
        pair_rank = jnp.sum(before * onehot, axis=-1)
        pair_rank = jnp.transpose(pair_rank.reshape(blocks, 2, TOKB), (0, 2, 1))
        dropped_now = (pair_rank >= CAP).astype(jnp.int32)
        slot_now = jnp.where(pair_rank >= CAP, 0, pair_rank).astype(jnp.int32)
        id_parts.append(chosen.reshape(TOKENS, 2))
        slot_parts.append(slot_now.reshape(TOKENS, 2))
        drop_parts.append(dropped_now.reshape(TOKENS, 2))
    return (jnp.stack(id_parts, axis=0), jnp.stack(slot_parts, axis=0), jnp.stack(drop_parts, axis=0))


def draw_expert_ids(key, part):
    return routing_tables(jax.random.fold_in(key, 7))[0]


def draw_slot_ids(key, part):
    return routing_tables(jax.random.fold_in(key, 7))[1]


def draw_dropped(key, part):
    return routing_tables(jax.random.fold_in(key, 7))[2]


def level_of(rng, dims, shards, low, high):
    gain, own = 1.0, jax.random.fold_in(rng, 6)
    for dim, parts in shards:
        steps = jnp.exp(jax.random.uniform(jax.random.fold_in(own, dim), (parts,), jnp.float32, low / len(shards), high / len(shards)))
        gain = gain * jnp.repeat(steps, dims[dim] // parts).reshape([-1 if axis == dim else 1 for axis in range(len(dims))])
    return gain


def gaussian(stream_key, shape, scale, bound, cuts=(), kind=jnp.bfloat16):
    loudness = level_of(stream_key, shape, cuts, -0.22, 0.18) if cuts else 1.0
    values = jax.random.normal(stream_key, shape, jnp.float32) * scale * loudness
    return jnp.minimum(jnp.maximum(values, -bound), bound).astype(kind)


def setup_inputs(seed: int = 0) -> dict:
    key_list = jax.random.split(jax.random.key(seed), 13)
    return {
        "inputs": gaussian(key_list[0], (MB, TOKENS, D), 1.0, 6.0, ((1, 32),)),
        "first_gain": jnp.clip(1.0 + 0.15 * jax.random.normal(key_list[1], (D,), jnp.float32), 0.25, 1.75),
        "w_qkv": gaussian(key_list[2], (D, 3 * D), D ** -0.5, 0.3125),
        "w_attn": gaussian(key_list[3], (D, D), (D // 32) ** -0.5, 1.75),
        "second_gain": jnp.clip(1.0 + 0.15 * jax.random.normal(key_list[4], (D,), jnp.float32), 0.25, 1.75),
        "w_router": gaussian(key_list[5], (D, EXPERTS), (D // 4) ** -0.5, 0.625),
        "expert_in": gaussian(key_list[6], (EXPERTS, D, FF), D ** -0.5, 0.3125, ((0, 4),)),
        "expert_out": gaussian(key_list[7], (EXPERTS, FF, D), (max(FF // 256, 1)) ** -0.5, 2.5, ((0, 4),)),
        "expert_ids": draw_expert_ids(jax.random.fold_in(key_list[12], 71), 0),
        "slot_ids": draw_slot_ids(jax.random.fold_in(key_list[12], 71), 0),
        "dropped": draw_dropped(jax.random.fold_in(key_list[12], 71), 0),
        "out_grad": gaussian(key_list[11], (MB, TOKENS, D), 1.0, 6.0, ((1, 32),)),
    }


@jax.custom_vjp
def low(v):
    return lax.optimization_barrier(v.astype(jnp.bfloat16)).astype(jnp.float32)

@jax.custom_vjp
def low_back(v):
    return v

def low_keep(v):
    return (low(v), None)

def low_pass(kept, grad):
    return (grad,)

def back_keep(v):
    return (v, None)

def back_low(kept, grad):
    return (low(grad),)
low.defvjp(low_keep, low_pass)
low_back.defvjp(back_keep, back_low)
EPS = 1e-06
HIGH = lax.Precision.HIGHEST

def layer_norm(features, gain_vec):
    row_mean = lax.optimization_barrier(jnp.mean(features, axis=-1, keepdims=True))
    centered = features - row_mean
    variance = lax.optimization_barrier(jnp.mean(centered * centered, axis=-1, keepdims=True))
    return centered * lax.rsqrt(variance + EPS) * gain_vec

def softmax_rows(scores):
    largest = lax.optimization_barrier(jnp.max(scores, axis=-1, keepdims=True))
    exp_terms = jnp.exp(scores - largest)
    return exp_terms / lax.optimization_barrier(jnp.sum(exp_terms, axis=-1, keepdims=True))

def attention_branch(block_rows, gain_vec, w_qkv, w_attn):
    row_count = block_rows.shape[0]
    images = row_count // SEQ
    normed = low(layer_norm(block_rows, gain_vec))
    qkv_rows = low_back(low(jnp.dot(normed, w_qkv, precision=HIGH, preferred_element_type=jnp.float32)))
    split_rows = qkv_rows.reshape(images, SEQ, 3, HEADS, HD)
    queries = split_rows[:, :, 0]
    key_rows = split_rows[:, :, 1]
    value_rows = split_rows[:, :, 2]
    scores = low_back(jnp.einsum('iqhd,ikhd->ihqk', queries, key_rows, precision=HIGH)) * HD ** (-0.5)
    attn_probs = low(softmax_rows(scores))
    attn_mixed = jnp.einsum('ihqk,ikhd->iqhd', attn_probs, value_rows, precision=HIGH).reshape(row_count, D)
    attn_mixed = low_back(low(attn_mixed))
    return low_back(jnp.dot(attn_mixed, w_attn, precision=HIGH, preferred_element_type=jnp.float32))

def expert_branch(normed, routed, slotted, dropped_rows, w_router, expert_in, expert_out):
    row_count = normed.shape[0]
    logits = low_back(jnp.dot(normed, w_router, precision=HIGH, preferred_element_type=jnp.float32))
    gate_probs = softmax_rows(logits)
    keeping = 1.0 - dropped_rows.astype(jnp.float32)
    blocks = row_count // TOKB
    owner_ids = (jnp.arange(row_count, dtype=jnp.int32) // TOKB)[:, None]
    buffer = jnp.zeros((blocks, EXPERTS, CAP, D), jnp.float32)
    buffer = buffer.at[owner_ids, routed, slotted].add(normed[:, None, :] * keeping[:, :, None])
    buffer = low_back(buffer)
    expert_rows = jnp.transpose(buffer, (1, 0, 2, 3)).reshape(EXPERTS, blocks * CAP, D)
    hidden = low_back(jnp.einsum('erd,edf->erf', expert_rows, expert_in, precision=HIGH))
    activated = low(jax.nn.gelu(hidden))
    produced = low_back(low(jnp.einsum('erf,efd->erd', activated, expert_out, precision=HIGH)))
    returned = jnp.transpose(produced.reshape(EXPERTS, blocks, CAP, D), (1, 0, 2, 3))
    picked = returned[owner_ids, routed, slotted]
    gate_pair = jnp.take_along_axis(gate_probs, routed, axis=1) * keeping
    return lax.optimization_barrier(jnp.sum(gate_pair[:, :, None] * picked, axis=1))

def whole_block(block_rows, routed, slotted, dropped_rows, params):
    first_gain, w_qkv, w_attn, second_gain, w_router, expert_in, expert_out = params
    residual = block_rows + attention_branch(block_rows, first_gain, w_qkv, w_attn)
    normed = low(layer_norm(residual, second_gain))
    return residual + expert_branch(normed, routed, slotted, dropped_rows, w_router, expert_in, expert_out)

def forward_all(inputs_f, params, expert_ids, slot_ids, dropped):
    group_rows = IMG * SEQ * N_EXPERT
    group_count = MB * TOKENS // group_rows
    stacked = (inputs_f.reshape(group_count, group_rows, D), expert_ids.reshape(group_count, group_rows, 2), slot_ids.reshape(group_count, group_rows, 2), dropped.reshape(group_count, group_rows, 2))

    def apply_group(group_items):
        return whole_block(group_items[0], group_items[1], group_items[2], group_items[3], params)
    return lax.map(jax.checkpoint(apply_group), stacked).reshape(MB, TOKENS, D)

def reference(inputs, first_gain, w_qkv, w_attn, second_gain, w_router, expert_in, expert_out, expert_ids, slot_ids, dropped, out_grad):
    params = (first_gain, w_qkv.astype(jnp.float32), w_attn.astype(jnp.float32), second_gain, w_router.astype(jnp.float32), expert_in.astype(jnp.float32), expert_out.astype(jnp.float32))

    def run_all(inputs_f, params_in):
        return forward_all(inputs_f, params_in, expert_ids, slot_ids, dropped)
    block_out, pullback = jax.vjp(run_all, inputs.astype(jnp.float32), params)
    input_grad, param_grads = pullback(out_grad.astype(jnp.float32))
    return (block_out, input_grad, param_grads[0], param_grads[1], param_grads[2], param_grads[3], param_grads[4], param_grads[5], param_grads[6])
```

```python
import functools

import jax
import jax.numpy as jnp
from jax import lax
from jax.experimental import pallas as pl
from jax.experimental.pallas import tpu as pltpu
from jax.sharding import PartitionSpec as P

D = 384
HEADS = 6
HD = 64
SEQ = 197
MB = 2
CAP = 16
EPS = 1e-06
TP = 208
TL = 256
XR = 16
F32 = jnp.float32
BF16 = jnp.bfloat16
MESH = pl.DeviceIdType.MESH


def mm(a, b, ca=1, cb=0):
    return lax.dot_general(
        a, b, (((ca,), (cb,)), ((), ())), preferred_element_type=F32
    )


def normed_of(rows):
    mean = jnp.sum(rows, axis=-1, keepdims=True) * (1.0 / D)
    centered = rows - mean
    var = jnp.sum(centered * centered, axis=-1, keepdims=True) * (1.0 / D)
    rstd = lax.rsqrt(var + EPS)
    return centered * rstd, rstd


def norm_pull(hat, rstd, gain, grad):
    scaled = grad * gain
    m1 = jnp.sum(scaled, axis=-1, keepdims=True) * (1.0 / D)
    m2 = jnp.sum(scaled * hat, axis=-1, keepdims=True) * (1.0 / D)
    return rstd * (scaled - m1 - hat * m2)


def kernel(
    dims,
    x_ref,
    g_ref,
    gain1_ref,
    gain2_ref,
    wqkv_ref,
    wattn_ref,
    wrt_ref,
    ids_ref,
    slot_ref,
    drop_ref,
    win_hbm,
    wout_hbm,
    bo_ref,
    ig_ref,
    eg_ref,
    ag_ref,
    w1,
    w2,
    n1_ref,
    qkv_ref,
    p_ref,
    am_ref,
    res_ref,
    n2_ref,
    rs_ref,
    cols_ref,
    dsend,
    drecv,
    rsend,
    rrecv,
    act_ref,
    hg_ref,
    xr_ref,
    pr_ref,
    xg_ref,
    x1_ref,
    xs_ref,
    dq_ref,
    acc_ref,
    small_ref,
    arb_ref,
    l1_ref,
    l2s_ref,
    l2_ref,
    l3_ref,
    wsem,
    dsem,
    rsem,
    xsem,
    asem,
):
    L, R, Z, G, FF = dims
    S = G * CAP
    FS = FF // (L * R)
    PR = arb_ref.shape[2]
    NR = PR - XR
    dp = lax.axis_index("dp")
    z = lax.axis_index("expert")
    j = dp // R
    r = dp % R
    me = z * L + j

    def group_id(e):
        return ((e % L) * R + r, e // L)

    def plane_id(i):
        return (i * R + r, z)

    def part_id(rr):
        return (j * R + rr, z)

    def remote(src, dst, sems, device):
        return pltpu.make_async_remote_copy(
            src_ref=src,
            dst_ref=dst,
            send_sem=sems.at[0],
            recv_sem=sems.at[1],
            device_id=device,
            device_id_type=MESH,
        )

    def wait_bytes(ref, sem):
        pltpu.make_async_copy(ref, ref, sem).wait()

    barrier = pltpu.get_barrier_semaphore()

    @pl.loop(1, G)
    def _(o):
        pl.semaphore_signal(
            barrier, inc=1, device_id=group_id((me + o) % G), device_id_type=MESH
        )

    for o in range(1, R):
        pl.semaphore_signal(
            barrier, inc=1, device_id=part_id((r + o) % R), device_id_type=MESH
        )

    load1 = pltpu.make_async_copy(win_hbm.at[j], w1, wsem.at[0])
    load2 = pltpu.make_async_copy(wout_hbm.at[j], w2, wsem.at[1])
    load1.start()
    load2.start()
    pl.semaphore_wait(barrier, G - 1 + R - 1)

    lane128 = lax.broadcasted_iota(jnp.int32, (TP, 128), 1)
    low_half = lane128 < HD
    key_ok = lax.broadcasted_iota(jnp.int32, (TP, TP), 1) < SEQ

    def exchange(send, recv, sems):
        pltpu.make_async_copy(send.at[me], recv.at[me], sems.at[1]).start()

        @pl.loop(1, G)
        def _(o):
            e = (me + o) % G
            remote(send.at[e], recv.at[me], sems, group_id(e)).start()

    def forward(mb, carry):
        x = x_ref[mb].astype(F32)
        hat, _ = normed_of(x)
        n1 = (hat * gain1_ref[...]).astype(BF16)
        n1_ref[mb] = n1
        qkv_ref[mb] = mm(n1, wqkv_ref[...]).astype(BF16)
        for pair in range(HEADS // 2):
            c = pair * 128
            q = qkv_ref[mb, :, c : c + 128] * jnp.asarray(HD**-0.5, BF16)
            k = qkv_ref[mb, :, D + c : D + c + 128]
            v = qkv_ref[mb, :, 2 * D + c : 2 * D + c + 128]
            mixed = []
            for half in range(2):
                mine = low_half if half == 0 else jnp.logical_not(low_half)
                qh = jnp.where(mine, q, jnp.zeros_like(q))
                s = mm(qh, k, 1, 1)
                s = jnp.where(key_ok, s, -1e30)
                e = jnp.exp(s - jnp.max(s, axis=-1, keepdims=True))
                p = e / jnp.sum(e, axis=-1, keepdims=True)
                p_ref[mb, 2 * pair + half] = p
                mixed.append(mm(p.astype(BF16), v))
            am_ref[mb, :, c : c + 128] = jnp.where(
                low_half, mixed[0], mixed[1]
            ).astype(BF16)
        res = x + mm(am_ref[mb], wattn_ref[...])
        res_ref[mb] = res
        hat2, _ = normed_of(res)
        n2 = (hat2 * gain2_ref[...]).astype(BF16)
        n2_ref[mb] = n2
        logits = mm(wrt_ref[...], n2, 1, 1)
        ex = jnp.exp(logits - jnp.max(logits, axis=0, keepdims=True))
        gp = ex / jnp.sum(ex, axis=0, keepdims=True)
        ids = ids_ref[mb]
        drop = drop_ref[mb]
        flat = jnp.where(drop == 0, ids * CAP + slot_ref[mb], S)
        rs_ref[...] = jnp.zeros_like(rs_ref)
        rs_ref[0:G, 0:TP] = gp
        rs_ref[G : G + 2, 0:TP] = jnp.full((2, TP), S, F32)
        rs_ref[G : G + 2, 0:SEQ] = flat.astype(F32)
        rs_ref[G + 2 : G + 4, 0:SEQ] = 1.0 - drop.astype(F32)
        rs_ref[G + 4 : G + 6, 0:SEQ] = ids.astype(F32)
        expert_of = lax.broadcasted_iota(jnp.int32, (G, TP), 0).astype(F32)
        slot_of = lax.broadcasted_iota(jnp.int32, (S, TP), 0).astype(F32)
        picks = []
        gcol = jnp.zeros((S, 1), F32)
        for kk in range(2):
            idr = rs_ref[G + 4 + kk : G + 5 + kk, 0:TP]
            keep = rs_ref[G + 2 + kk : G + 3 + kk, 0:TP]
            flr = rs_ref[G + kk : G + kk + 1, 0:TP]
            gate = (
                jnp.sum(jnp.where(expert_of == idr, gp, 0.0), axis=0, keepdims=True)
                * keep
            )
            rs_ref[G + 6 + kk : G + 7 + kk, 0:TP] = gate
            hit = slot_of == flr
            picks.append(jnp.where(hit, 1.0, 0.0))
            gcol = gcol + jnp.sum(
                jnp.where(hit, gate, 0.0), axis=-1, keepdims=True
            )
        cols_ref[mb] = rs_ref[...].T
        pick = (picks[0] + picks[1]).astype(BF16)
        rows = mm(pick, n2).astype(BF16)
        dsend[mb, :, 0:CAP, :] = rows.reshape(G, CAP, D)
        grows = (mm(pick, g_ref[mb]) * gcol).astype(BF16)
        dsend[mb, :, CAP : 2 * CAP, :] = grows.reshape(G, CAP, D)
        exchange(dsend.at[mb], drecv.at[mb], dsem.at[mb])
        return carry

    lax.fori_loop(0, MB, forward, 0)
    load1.wait()
    load2.wait()

    def experts(mb, carry):
        wait_bytes(drecv.at[mb], dsem.at[mb, 1])
        xs = drecv[mb, :, 0:CAP, :].reshape(S, D)
        pg = drecv[mb, :, CAP : 2 * CAP, :].reshape(S, D)
        base = pl.multiple_of(mb * S, S)
        xr_ref[pl.ds(base, S), :] = xs
        pr_ref[pl.ds(base, S), :] = pg
        step = 384
        produced = jnp.zeros((S, D), F32)
        back = jnp.zeros((S, D), F32)
        for c in range(0, FF, step):
            h = mm(xs, w1[:, c : c + step])
            sq = h * h
            t = jnp.tanh(0.7978845608028654 * (h + 0.044715 * (h * sq)))
            half = 0.5 * (1.0 + t)
            act = (h * half).astype(BF16)
            slope = half + 0.5 * h * (1.0 - t * t) * (
                0.7978845608028654 * (1.0 + 0.134145 * sq)
            )
            ag = mm(pg, w2[c : c + step, :], 1, 1)
            hg = (ag * slope).astype(BF16)
            act_ref[pl.ds(base, S), c : c + step] = act
            hg_ref[pl.ds(base, S), c : c + step] = hg
            produced = produced + mm(act, w2[c : c + step, :])
            back = back + mm(hg, w1[:, c : c + step], 1, 1)
        rsend[mb, :, 0:CAP, :] = produced.astype(BF16).reshape(G, CAP, D)
        rsend[mb, :, CAP : 2 * CAP, :] = back.astype(BF16).reshape(G, CAP, D)
        exchange(rsend.at[mb], rrecv.at[mb], rsem.at[mb])
        return carry

    lax.fori_loop(0, MB, experts, 0)

    span = FF // L

    def weight_grads(i, carry):
        at = pl.ds(pl.multiple_of(i * span, 128), span)
        g1 = mm(hg_ref[:, at], xr_ref[...], 0, 0).astype(BF16)
        g2 = mm(act_ref[:, at], pr_ref[...], 0, 0).astype(BF16)
        for rr in range(R):
            xg_ref[rr, i, 0] = g1[rr * FS : (rr + 1) * FS]
            xg_ref[rr, i, 1] = g2[rr * FS : (rr + 1) * FS]
        return carry

    lax.fori_loop(0, L, weight_grads, 0)
    for o in range(1, R):
        rr = (r + o) % R
        remote(xg_ref.at[rr], x1_ref.at[R - o - 1], xsem.at[0], part_id(rr)).start()

    acc_ref[...] = jnp.zeros_like(acc_ref)
    small_ref[...] = jnp.zeros_like(small_ref)

    def backward(mb, carry):
        wait_bytes(rrecv.at[mb], rsem.at[mb, 1])
        cols = cols_ref[mb][0:TP]
        prod = rrecv[mb, :, 0:CAP, :].reshape(S, D)
        bgr = rrecv[mb, :, CAP : 2 * CAP, :].reshape(S, D)
        g = g_ref[mb].astype(F32)
        res = res_ref[mb]
        slot_lane = lax.broadcasted_iota(jnp.int32, (TP, S), 1).astype(F32)
        expert_lane = lax.broadcasted_iota(jnp.int32, (TP, G), 1).astype(F32)
        gp = cols[:, 0:G]
        out = res
        gates_grad = jnp.zeros((TP, G), F32)
        picks = []
        for kk in range(2):
            flc = cols[:, G + kk : G + kk + 1]
            keep = cols[:, G + 2 + kk : G + 3 + kk]
            idc = cols[:, G + 4 + kk : G + 5 + kk]
            gate = cols[:, G + 6 + kk : G + 7 + kk]
            pick = jnp.where(slot_lane == flc, 1.0, 0.0)
            picks.append(pick)
            rows = mm(pick.astype(BF16), prod)
            out = out + gate * rows
            gate_grad = jnp.sum(rows * g, axis=-1, keepdims=True) * keep
            gates_grad = gates_grad + jnp.where(expert_lane == idc, gate_grad, 0.0)
        bo_ref[mb] = out
        inner = jnp.sum(gp * gates_grad, axis=-1, keepdims=True)
        logit_grad = (gp * (gates_grad - inner)).astype(BF16)
        ngrad = mm((picks[0] + picks[1]).astype(BF16), bgr) + mm(
            logit_grad, wrt_ref[...]
        )
        small_ref[0:G, :] += mm(logit_grad, n2_ref[mb], 0, 0)
        hat2, rstd2 = normed_of(res)
        small_ref[G + 1 : G + 2, :] += jnp.sum(ngrad * hat2, axis=0, keepdims=True)
        rgrad = g + norm_pull(hat2, rstd2, gain2_ref[...], ngrad)
        branch = rgrad.astype(BF16)
        acc_ref[3 * D : 4 * D, :] += mm(am_ref[mb], branch, 0, 0)
        mgrad = mm(branch, wattn_ref[...], 1, 1).astype(BF16)
        for pair in range(HEADS // 2):
            c = pair * 128
            q = qkv_ref[mb, :, c : c + 128]
            k = qkv_ref[mb, :, D + c : D + c + 128]
            v = qkv_ref[mb, :, 2 * D + c : 2 * D + c + 128]
            mg = mgrad[:, c : c + 128]
            dqs, dks, dvs = [], [], []
            for half in range(2):
                mine = low_half if half == 0 else jnp.logical_not(low_half)
                mgh = jnp.where(mine, mg, jnp.zeros_like(mg))
                p = p_ref[mb, 2 * pair + half]
                dp_ = mm(mgh, v, 1, 1)
                delta = jnp.sum(p * dp_, axis=-1, keepdims=True)
                ds = (p * (dp_ - delta) * HD**-0.5).astype(BF16)
                dqs.append(mm(ds, k))
                dks.append(mm(ds, q, 0, 0))
                dvs.append(mm(p.astype(BF16), mg, 0, 0))
            for n, parts in enumerate((dqs, dks, dvs)):
                dq_ref[:, n * D + c : n * D + c + 128] = jnp.where(
                    low_half, parts[0], parts[1]
                ).astype(BF16)
        n1 = n1_ref[mb]
        for n in range(3):
            acc_ref[n * D : (n + 1) * D, :] += mm(
                n1, dq_ref[:, n * D : (n + 1) * D], 0, 0
            )
        fgrad = mm(dq_ref[...], wqkv_ref[...], 1, 1)
        hat, rstd = normed_of(x_ref[mb].astype(F32))
        small_ref[G : G + 1, :] += jnp.sum(fgrad * hat, axis=0, keepdims=True)
        ig_ref[mb] = rgrad + norm_pull(hat, rstd, gain1_ref[...], fgrad)
        return carry

    lax.fori_loop(0, MB, backward, 0)

    for o in range(1, R):
        wait_bytes(x1_ref.at[o - 1], xsem.at[0, 1])

    def add_slices(i, carry):
        total = xg_ref[r, i].astype(F32)
        for o in range(R - 1):
            total = total + x1_ref[o, i].astype(F32)
        xs_ref[i] = total.astype(BF16)
        return carry

    lax.fori_loop(0, L, add_slices, 0)
    for o in range(1, L):
        i = (j + o) % L
        remote(xs_ref.at[i], eg_ref.at[j], xsem.at[1], plane_id(i)).start()
    pltpu.make_async_copy(xs_ref.at[j], eg_ref.at[j], xsem.at[1, 1]).start()

    for rr in range(R):
        for i in range(L):
            at = (rr * L + i) * NR
            arb_ref[rr, i, 0:NR, :] = acc_ref[at : at + NR, :].astype(BF16)
            if (rr * L + i) * XR < small_ref.shape[0]:
                sat = (rr * L + i) * XR
                arb_ref[rr, i, NR:PR, :] = small_ref[sat : sat + XR, :].astype(BF16)
            else:
                arb_ref[rr, i, NR:PR, :] = jnp.zeros((XR, D), BF16)
    for o in range(1, R):
        rr = (r + o) % R
        remote(arb_ref.at[rr], l1_ref.at[R - o - 1], asem.at[0], part_id(rr)).start()
    for o in range(1, R):
        wait_bytes(l1_ref.at[o - 1], asem.at[0, 1])
    for i in range(L):
        total = arb_ref[r, i].astype(F32)
        for o in range(R - 1):
            total = total + l1_ref[o, i].astype(F32)
        l2s_ref[i] = total.astype(BF16)
    for o in range(1, L):
        i = (j + o) % L
        remote(l2s_ref.at[i], l2_ref.at[L - o - 1], asem.at[1], plane_id(i)).start()
    wait_bytes(l2_ref, asem.at[1, 1])
    total = l2s_ref[j].astype(F32)
    for o in range(L - 1):
        total = total + l2_ref[o].astype(F32)
    l3_ref[z] = total.astype(BF16)
    for o in range(1, Z):
        zz = (z + o) % Z
        remote(l3_ref.at[z], l3_ref.at[z], asem.at[2], (dp, zz)).start()
    wait_bytes(l3_ref.at[pl.ds(0, Z - 1)], asem.at[2, 1])
    total = l3_ref[0].astype(F32)
    for zz in range(1, Z):
        total = total + l3_ref[zz].astype(F32)
    ag_ref[r, j] = total.astype(BF16)
    for o in range(1, L):
        i = (j + o) % L
        remote(ag_ref.at[r, j], ag_ref.at[r, j], asem.at[3], plane_id(i)).start()
    wait_bytes(l2_ref, asem.at[3, 1])
    for o in range(1, R):
        rr = (r + o) % R
        remote(ag_ref.at[r], ag_ref.at[r], asem.at[4], part_id(rr)).start()
    for o in range(1, R):
        wait_bytes(l1_ref.at[o - 1], asem.at[4, 1])
    wait_bytes(eg_ref, xsem.at[1, 1])

    for mb in range(MB):
        wait_bytes(dsend.at[mb, pl.ds(0, G - 1)], dsem.at[mb, 0])
        wait_bytes(rsend.at[mb, pl.ds(0, G - 1)], rsem.at[mb, 0])
    for o in range(1, R):
        wait_bytes(x1_ref.at[o - 1], xsem.at[0, 0])
        wait_bytes(l1_ref.at[o - 1], asem.at[0, 0])
        wait_bytes(l1_ref.at[o - 1], asem.at[4, 0])
    wait_bytes(xs_ref.at[pl.ds(0, L - 1)], xsem.at[1, 0])
    wait_bytes(l2_ref, asem.at[1, 0])
    wait_bytes(l3_ref.at[pl.ds(0, Z - 1)], asem.at[2, 0])
    wait_bytes(l2_ref, asem.at[3, 0])


def on_device(
    groups,
    replicas,
    inputs,
    first_gain,
    w_qkv,
    w_attn,
    second_gain,
    w_router,
    expert_in,
    expert_out,
    expert_ids,
    slot_ids,
    dropped,
    out_grad,
):
    L, _, FF = expert_in.shape
    Z = groups
    R = replicas // L
    G = L * Z
    S = G * CAP
    FS = FF // replicas
    NR = 4 * D // replicas
    PR = NR + XR
    small_rows = -(-(G + 2) // XR) * XR
    rs_rows = -(-(G + 8) // 8) * 8
    pad = ((0, 0), (0, TP - SEQ), (0, 0))
    x = jnp.pad(inputs, pad)
    g = jnp.pad(out_grad, pad)
    swap = lambda a: jnp.transpose(a, (0, 2, 1))
    vmem = pl.BlockSpec(memory_space=pltpu.VMEM)
    hbm = pl.BlockSpec(memory_space=pl.ANY)
    sds = jax.ShapeDtypeStruct
    bo, ig, eg, ag = pl.pallas_call(
        functools.partial(kernel, (L, R, Z, G, FF)),
        out_shape=(
            sds((MB, TP, D), F32),
            sds((MB, TP, D), F32),
            sds((L, 2, FS, D), BF16),
            sds((R, L, PR, D), BF16),
        ),
        in_specs=[vmem] * 10 + [hbm] * 2,
        out_specs=(vmem, vmem, vmem, vmem),
        scratch_shapes=[
            pltpu.VMEM((D, FF), BF16),
            pltpu.VMEM((FF, D), BF16),
            pltpu.VMEM((MB, TP, D), BF16),
            pltpu.VMEM((MB, TP, 3 * D), BF16),
            pltpu.VMEM((MB, HEADS, TP, TP), F32),
            pltpu.VMEM((MB, TP, D), BF16),
            pltpu.VMEM((MB, TP, D), F32),
            pltpu.VMEM((MB, TP, D), BF16),
            pltpu.VMEM((rs_rows, TL), F32),
            pltpu.VMEM((MB, TL, rs_rows), F32),
            pltpu.VMEM((MB, G, 2 * CAP, D), BF16),
            pltpu.VMEM((MB, G, 2 * CAP, D), BF16),
            pltpu.VMEM((MB, G, 2 * CAP, D), BF16),
            pltpu.VMEM((MB, G, 2 * CAP, D), BF16),
            pltpu.VMEM((MB * S, FF), BF16),
            pltpu.VMEM((MB * S, FF), BF16),
            pltpu.VMEM((MB * S, D), BF16),
            pltpu.VMEM((MB * S, D), BF16),
            pltpu.VMEM((R, L, 2, FS, D), BF16),
            pltpu.VMEM((R - 1, L, 2, FS, D), BF16),
            pltpu.VMEM((L, 2, FS, D), BF16),
            pltpu.VMEM((TP, 3 * D), BF16),
            pltpu.VMEM((4 * D, D), F32),
            pltpu.VMEM((small_rows, D), F32),
            pltpu.VMEM((R, L, PR, D), BF16),
            pltpu.VMEM((R - 1, L, PR, D), BF16),
            pltpu.VMEM((L, PR, D), BF16),
            pltpu.VMEM((L - 1, PR, D), BF16),
            pltpu.VMEM((Z, PR, D), BF16),
            pltpu.SemaphoreType.DMA((2,)),
            pltpu.SemaphoreType.DMA((MB, 2)),
            pltpu.SemaphoreType.DMA((MB, 2)),
            pltpu.SemaphoreType.DMA((2, 2)),
            pltpu.SemaphoreType.DMA((5, 2)),
        ],
        compiler_params=pltpu.CompilerParams(
            collective_id=0, has_side_effects=True, vmem_limit_bytes=60 << 20
        ),
        name="block",
    )(
        x,
        g,
        first_gain.reshape(1, D),
        second_gain.reshape(1, D),
        w_qkv,
        w_attn,
        w_router.T,
        swap(expert_ids),
        swap(slot_ids),
        swap(dropped),
        expert_in,
        expert_out,
    )
    parts = ag.reshape(replicas, PR, D)
    dense = parts[:, :NR].reshape(4, D, D).astype(F32)
    small = parts[: small_rows // XR, NR:].reshape(small_rows, D).astype(F32)
    return (
        bo[:, :SEQ],
        ig[:, :SEQ],
        small[G],
        jnp.transpose(dense[:3], (1, 0, 2)).reshape(D, 3 * D),
        dense[3],
        small[G + 1],
        small[:G].T,
        jnp.transpose(eg[:, 0].astype(F32), (0, 2, 1)),
        eg[:, 1].astype(F32),
    )


def solution(mesh):
    rows = P(None, ("dp", "expert"), None)
    split = P("expert", None, None)
    return jax.shard_map(
        functools.partial(on_device, mesh.shape["expert"], mesh.shape["dp"]),
        mesh=mesh,
        in_specs=(
            rows,
            P(),
            P(),
            P(),
            P(),
            P(),
            split,
            split,
            rows,
            rows,
            rows,
            rows,
        ),
        out_specs=(
            rows,
            rows,
            P(),
            P(),
            P(),
            P(),
            P(),
            P("expert", None, "dp"),
            P("expert", "dp", None),
        ),
        check_vma=False,
    )
```

```python
import functools
import math

import jax
import jax.numpy as jnp
from jax import lax
from jax.experimental import pallas as pl
from jax.experimental.pallas import tpu as pltpu
from jax.sharding import PartitionSpec as P

D = 384
HEADS = 6
HD = 64
SEQ = 197
MB = 2
CAP = 16
EPS = 1e-06
TP = 208
TL = 256
SM = 32
F32 = jnp.float32
BF16 = jnp.bfloat16
MESH = pl.DeviceIdType.MESH
KINDS = ("rows", "gate", "pull", "ggrad", "back", "made")


def mm(a, b, ca=1, cb=0):
    return lax.dot_general(
        a, b, (((ca,), (cb,)), ((), ())), preferred_element_type=F32
    )


def mm_exact(a, b):
    return lax.dot_general(
        a,
        b,
        (((1,), (0,)), ((), ())),
        preferred_element_type=F32,
        precision=lax.Precision.HIGHEST,
    )


def normed_of(rows):
    mean = jnp.sum(rows, axis=-1, keepdims=True) * (1.0 / D)
    centered = rows - mean
    var = jnp.sum(centered * centered, axis=-1, keepdims=True) * (1.0 / D)
    rstd = lax.rsqrt(var + EPS)
    return centered * rstd, rstd


def norm_pull(hat, rstd, gain, grad):
    scaled = grad * gain
    m1 = jnp.sum(scaled, axis=-1, keepdims=True) * (1.0 / D)
    m2 = jnp.sum(scaled * hat, axis=-1, keepdims=True) * (1.0 / D)
    return rstd * (scaled - m1 - hat * m2)


def kernel(dims, ins, outs, scratch):
    L, R, Z, G, FF = dims
    S = G * CAP
    FS = FF // (L * R)
    (
        x_hbm,
        g_hbm,
        gain1_hbm,
        gain2_hbm,
        wqkv_hbm,
        wattn_hbm,
        wrt_hbm,
        ids_hbm,
        slot_hbm,
        drop_hbm,
        win_hbm,
        wout_hbm,
    ) = ins
    bo_ref, ig_ref, eg_ref, *dense_refs, small_out = outs
    x_ref, g_ref, gain1_ref, gain2_ref = scratch["loads"][:4]
    wqkv_ref, wattn_ref, wrt_ref = scratch["loads"][4:7]
    ids_ref, slot_ref, drop_ref, w1, w2 = scratch["loads"][7:]
    n1_ref, qkv_ref, p_ref, am_ref, res_ref, n2_ref = scratch["saved"]
    rs_ref, cols_ref, slope_ref = scratch["work"]
    act_ref, hg_ref, xg_ref, x1_ref, xs_ref, gacc_ref = scratch["expert"]
    dq_ref, acc_ref, small_ref, t1_ref, t2_ref, t3_ref = scratch["grads"]
    lsem, esem, xsem, tsem = scratch["sems"]
    chunks = scratch["chunks"]
    dp = lax.axis_index("dp")
    z = lax.axis_index("expert")
    j = dp // R
    r = dp % R
    me = z * L + j

    def group_id(e):
        return ((e % L) * R + r, e // L)

    def plane_id(i):
        return (i * R + r, z)

    def part_id(rr):
        return (j * R + rr, z)

    def remote(src, dst, send_sem, recv_sem, device):
        pltpu.make_async_remote_copy(
            src_ref=src,
            dst_ref=dst,
            send_sem=send_sem,
            recv_sem=recv_sem,
            device_id=device,
            device_id_type=MESH,
        ).start()

    def wait_bytes(ref, sem):
        pltpu.make_async_copy(ref, ref, sem).wait()

    barrier = pltpu.get_barrier_semaphore()

    @pl.loop(1, G)
    def _(o):
        pl.semaphore_signal(
            barrier, inc=1, device_id=group_id((me + o) % G), device_id_type=MESH
        )

    for o in range(1, R):
        pl.semaphore_signal(
            barrier, inc=1, device_id=part_id((r + o) % R), device_id_type=MESH
        )

    loads = []
    sources = [
        x_hbm,
        g_hbm,
        gain1_hbm,
        gain2_hbm,
        wqkv_hbm,
        wattn_hbm,
        wrt_hbm,
        ids_hbm,
        slot_hbm,
        drop_hbm,
        win_hbm.at[j],
        wout_hbm.at[j],
    ]
    for n, (src, dst) in enumerate(zip(sources, scratch["loads"])):
        loads.append(pltpu.make_async_copy(src, dst, lsem.at[n]))
    for n in (0, 2, 4, 5, 3, 6, 7, 8, 9, 1, 10, 11):
        loads[n].start()

    def ready(*which):
        for n in which:
            loads[n].wait()

    low_half = lax.broadcasted_iota(jnp.int32, (TP, 128), 1) < HD
    key_ok = lax.broadcasted_iota(jnp.int32, (TP, TP), 1) < SEQ
    slot_lane = lax.broadcasted_iota(
        jnp.int32, (G, CAP, 128), 2
    ) == lax.broadcasted_iota(jnp.int32, (G, CAP, 128), 1)

    def exchange(kind, mb):
        send, recv = scratch[kind]
        send, recv = send.at[mb], recv.at[mb]
        n = KINDS.index(kind)
        pltpu.make_async_copy(send.at[me], recv.at[me], esem.at[n, mb, 1]).start()

        @pl.loop(1, G)
        def _(o):
            e = (me + o) % G
            remote(
                send.at[e],
                recv.at[me],
                esem.at[n, mb, 0],
                esem.at[n, mb, 1],
                group_id(e),
            )

    def arrived(kind, mb):
        recv = scratch[kind][1].at[mb]
        wait_bytes(recv, esem.at[KINDS.index(kind), mb, 1])
        return recv

    def row_of_slots(col):
        spread = jnp.where(slot_lane, col.reshape(G, CAP, 1), 0.0)
        return jnp.sum(spread, axis=1, keepdims=True)

    def slots_of_row(row):
        spread = jnp.where(slot_lane, row, 0.0)
        return jnp.sum(spread, axis=-1, keepdims=True).reshape(S, 1)

    def forward(mb):
        if mb == 0:
            ready(0, 2, 4)
        x = x_ref[mb].astype(F32)
        hat, _ = normed_of(x)
        n1 = (hat * gain1_ref[...].reshape(1, D)).astype(BF16)
        n1_ref[mb] = n1
        qkv_ref[mb] = mm(n1, wqkv_ref[...]).astype(BF16)
        for pair in range(HEADS // 2):
            c = pair * 128
            q = qkv_ref[mb, :, c : c + 128] * jnp.asarray(HD**-0.5, BF16)
            k = qkv_ref[mb, :, D + c : D + c + 128]
            v = qkv_ref[mb, :, 2 * D + c : 2 * D + c + 128]
            mixed = []
            for half in range(2):
                mine = low_half if half == 0 else jnp.logical_not(low_half)
                qh = jnp.where(mine, q, jnp.zeros_like(q))
                s = mm(qh, k, 1, 1)
                s = jnp.where(key_ok, s, -1e30)
                e = jnp.exp(s - jnp.max(s, axis=-1, keepdims=True))
                p = e / jnp.sum(e, axis=-1, keepdims=True)
                p_ref[mb, 2 * pair + half] = p
                mixed.append(mm(p.astype(BF16), v))
            am_ref[mb, :, c : c + 128] = jnp.where(
                low_half, mixed[0], mixed[1]
            ).astype(BF16)
        if mb == 0:
            ready(5, 3, 6, 7, 8, 9, 1)
        res = x + mm(am_ref[mb], wattn_ref[...])
        res_ref[mb] = res
        hat2, _ = normed_of(res)
        n2 = (hat2 * gain2_ref[...].reshape(1, D)).astype(BF16)
        n2_ref[mb] = n2
        logits = mm(wrt_ref[...], n2, 1, 1)
        ex = jnp.exp(logits - jnp.max(logits, axis=0, keepdims=True))
        gp = ex / jnp.sum(ex, axis=0, keepdims=True)
        ids = ids_ref[mb]
        drop = drop_ref[mb]
        slot = slot_ref[mb]
        flat = jnp.where(drop == 0, ids * CAP + slot, S)
        rs_ref[...] = jnp.zeros_like(rs_ref)
        rs_ref[0:G, 0:TP] = gp
        rs_ref[G : G + 2, 0:TP] = jnp.full((2, TP), S, F32)
        rs_ref[G : G + 2, 0:SEQ] = flat.astype(F32)
        rs_ref[G + 2 : G + 4, 0:SEQ] = 1.0 - drop.astype(F32)
        rs_ref[G + 4 : G + 6, 0:SEQ] = ids.astype(F32)
        rs_ref[G + 8 : G + 10, 0:SEQ] = slot.astype(F32)
        expert_of = lax.broadcasted_iota(jnp.int32, (G, TP), 0).astype(F32)
        slot_of = lax.broadcasted_iota(jnp.int32, (S, TP), 0).astype(F32)
        pick = jnp.zeros((S, TP), F32)
        gcol = jnp.zeros((S, 1), F32)
        for kk in range(2):
            flr = rs_ref[G + kk : G + kk + 1, 0:TP]
            keep = rs_ref[G + 2 + kk : G + 3 + kk, 0:TP]
            idr = rs_ref[G + 4 + kk : G + 5 + kk, 0:TP]
            mine = jnp.where(expert_of == idr, gp, 0.0)
            gate = jnp.sum(mine, axis=0, keepdims=True) * keep
            rs_ref[G + 6 + kk : G + 7 + kk, 0:TP] = gate
            hit = slot_of == flr
            pick = pick + jnp.where(hit, 1.0, 0.0)
            gcol = gcol + jnp.sum(jnp.where(hit, gate, 0.0), axis=-1, keepdims=True)
        cols_ref[mb] = rs_ref[...].T
        pick = pick.astype(BF16)
        scratch["rows"][0][mb] = mm(pick, n2).astype(BF16).reshape(G, CAP, D)
        scratch["gate"][0][mb] = row_of_slots(gcol)
        scratch["pull"][0][mb] = mm(pick, g_ref[mb]).astype(BF16).reshape(G, CAP, D)

    def experts(mb):
        xs = arrived("rows", mb)[...].reshape(S, D)
        step = 384
        produced = jnp.zeros((S, D), F32)
        for c in range(0, FF, step):
            h = mm(xs, w1[:, c : c + step])
            sq = h * h
            t = jnp.tanh(0.7978845608028654 * (h + 0.044715 * (h * sq)))
            half = 0.5 * (1.0 + t)
            act = (h * half).astype(BF16)
            slope_ref[:, c : c + step] = half + 0.5 * h * (1.0 - t * t) * (
                0.7978845608028654 * (1.0 + 0.134145 * sq)
            )
            act_ref[mb, :, c : c + step] = act
            produced = produced + mm(act, w2[c : c + step, :])
        produced = produced.astype(BF16)
        scratch["made"][0][mb] = produced.reshape(G, CAP, D)
        gates = slots_of_row(arrived("gate", mb)[...])
        grow = arrived("pull", mb)[...].reshape(S, D).astype(F32)
        pg = (gates * grow).astype(BF16)
        scratch["gated"][mb] = pg
        gg = jnp.sum(grow * produced.astype(F32), axis=-1, keepdims=True)
        scratch["ggrad"][0][mb] = row_of_slots(gg)
        back = jnp.zeros((S, D), F32)
        for c in range(0, FF, step):
            ag = mm(pg, w2[c : c + step, :], 1, 1)
            hg = (ag * slope_ref[:, c : c + step]).astype(BF16)
            hg_ref[mb, :, c : c + step] = hg
            back = back + mm(hg, w1[:, c : c + step], 1, 1)
        scratch["back"][0][mb] = back.astype(BF16).reshape(G, CAP, D)
        exchange("ggrad", mb)
        exchange("back", mb)

    span = FF // L

    def weight_grads(mb):
        xs = scratch["rows"][1][mb].reshape(S, D)
        pg = scratch["gated"][mb]

        def part(i, carry):
            at = pl.ds(pl.multiple_of(i * span, 128), span)
            g1 = mm(hg_ref[mb, :, at], xs, 0, 0)
            g2 = mm(act_ref[mb, :, at], pg, 0, 0)
            if mb < MB - 1:
                if mb > 0:
                    g1 = g1 + gacc_ref[0, i]
                    g2 = g2 + gacc_ref[1, i]
                gacc_ref[0, i] = g1
                gacc_ref[1, i] = g2
            else:
                g1 = (g1 + gacc_ref[0, i]).astype(BF16)
                g2 = (g2 + gacc_ref[1, i]).astype(BF16)
                for rr in range(R):
                    xg_ref[rr, i, 0] = g1[rr * FS : (rr + 1) * FS]
                    xg_ref[rr, i, 1] = g2[rr * FS : (rr + 1) * FS]
            return carry

        lax.fori_loop(0, L, part, 0)

    def swap_slices():
        for o in range(1, R):
            rr = (r + o) % R
            remote(
                xg_ref.at[rr],
                x1_ref.at[R - o - 1],
                xsem.at[0, 0],
                xsem.at[0, 1],
                part_id(rr),
            )

    def add_slices():
        if R > 1:
            wait_bytes(x1_ref, xsem.at[0, 1])

        def part(i, carry):
            total = xg_ref[r, i].astype(F32)
            for o in range(R - 1):
                total = total + x1_ref[o, i].astype(F32)
            xs_ref[i] = total.astype(BF16)
            return carry

        lax.fori_loop(0, L, part, 0)

    def hand_out(mat):
        for o in range(1, L):
            i = (j + o) % L
            remote(
                xs_ref.at[i, mat],
                eg_ref.at[j, mat],
                xsem.at[1 + mat, 0],
                xsem.at[1 + mat, 1],
                plane_id(i),
            )
        pltpu.make_async_copy(
            xs_ref.at[j, mat], eg_ref.at[j, mat], xsem.at[1 + mat, 1]
        ).start()

    def add_block(block, value):
        for ck in chunks:
            if block in ck["blocks"]:
                src, pr = ck["src"], ck["pr"]
                at = ck["blocks"].index(block) * (D // pr)
        if pr % 8 == 0:
            value = value.reshape(D // pr, pr, D)
            src[at : at + D // pr] = value.astype(BF16)
        else:
            acc_ref[block * D : (block + 1) * D] = value
            rows = math.lcm(pr, 8)

            @pl.loop(0, D // rows)
            def _(n):
                first = pl.multiple_of(block * D + n * rows, 8)
                piece = acc_ref[pl.ds(first, rows)].astype(BF16)
                for m in range(rows // pr):
                    src[at + n * (rows // pr) + m] = piece[m * pr : (m + 1) * pr]

    def sum_start(ck):
        for n in range(1, L + 1):
            i = (j + n) % L
            for o in range(1, R):
                rr = (r + o) % R
                remote(
                    ck["src"].at[pl.ds((rr * L + i) * Z, Z)],
                    ck["l1"].at[R - o - 1, i],
                    ck["send"].at[0],
                    ck["s1"].at[R - o - 1, i],
                    part_id(rr),
                )

    def sum_pairs(ck):
        for n in range(1, L + 1):
            i = (j + n) % L
            total = ck["src"][pl.ds((r * L + i) * Z, Z)].astype(F32)
            for o in range(R - 1):
                wait_bytes(ck["l1"].at[o, i], ck["s1"].at[o, i])
                total = total + ck["l1"][o, i].astype(F32)
            ck["l2s"][i] = total.astype(BF16)
            if n < L:
                remote(
                    ck["l2s"].at[i],
                    ck["l2"].at[L - n - 1],
                    ck["send"].at[1],
                    ck["recv"].at[1],
                    plane_id(i),
                )

    def sum_plane(ck):
        if L > 1:
            wait_bytes(ck["l2"], ck["recv"].at[1])
        for n in range(Z - 1, -1, -1):
            zz = (z + n) % Z
            total = ck["l2s"][j, zz].astype(F32)
            for o in range(L - 1):
                total = total + ck["l2"][o, zz].astype(F32)
            ck["l3s"][zz] = total.astype(BF16)
            if n > 0:
                remote(
                    ck["l3s"].at[zz],
                    ck["l3"].at[Z - n - 1],
                    ck["send"].at[2],
                    ck["recv"].at[2],
                    (dp, zz),
                )

    def sum_z(ck):
        out = ck["out"]
        if Z > 1:
            wait_bytes(ck["l3"], ck["recv"].at[2])
        total = ck["l3s"][z].astype(F32)
        for o in range(Z - 1):
            total = total + ck["l3"][o].astype(F32)
        mine = (r * L + j) * Z + z
        out[mine] = total.astype(BF16)
        for n in range(Z - 1, 0, -1):
            remote(
                out.at[mine],
                out.at[mine],
                ck["send"].at[3],
                ck["recv"].at[3],
                (dp, (z + n) % Z),
            )

    def spread_plane(ck):
        out = ck["out"]
        if Z > 1:
            wait_bytes(ck["l3"], ck["recv"].at[3])
        mine = pl.ds((r * L + j) * Z, Z)
        for n in range(1, L):
            remote(
                out.at[mine],
                out.at[mine],
                ck["send"].at[4],
                ck["s2"].at[L - n - 1],
                plane_id((j + n) % L),
            )
        spread_part(ck, j)

    def spread_part(ck, i):
        out = ck["out"]
        at = pl.ds((r * L + i) * Z, Z)
        for o in range(1, R):
            remote(
                out.at[at],
                out.at[at],
                ck["send"].at[5],
                ck["recv"].at[5],
                part_id((r + o) % R),
            )

    def spread_parts(ck):
        for n in range(1, L):
            wait_bytes(ck["l2"].at[n - 1], ck["s2"].at[n - 1])
            spread_part(ck, (j + n) % L)

    def sum_end(ck):
        if R > 1:
            wait_bytes(ck["l1"], ck["recv"].at[5])
            wait_bytes(ck["l1"], ck["send"].at[0])
            wait_bytes(ck["l1"], ck["send"].at[5])
        if L > 1:
            wait_bytes(ck["l2"], ck["send"].at[1])
            wait_bytes(ck["l2"], ck["send"].at[4])
        if Z > 1:
            wait_bytes(ck["l3"], ck["send"].at[2])
            wait_bytes(ck["l3"], ck["send"].at[3])

    levels = ((t1_ref, r, R, part_id), (t2_ref, j, L, plane_id), (t3_ref, z, Z, None))

    def small_start(level):
        buf, at, count, ident = levels[level]
        for o in range(1, count):
            to = (at + o) % count
            remote(
                buf.at[at],
                buf.at[at],
                tsem.at[level, 0],
                tsem.at[level, 1],
                (dp, to) if ident is None else ident(to),
            )

    def small_sum(level):
        buf, _, count, _ = levels[level]
        if count > 1:
            wait_bytes(buf.at[pl.ds(0, count - 1)], tsem.at[level, 1])
        total = buf[0].astype(F32)
        for n in range(1, count):
            total = total + buf[n].astype(F32)
        return total

    def small_next(level):
        total = small_sum(level)
        buf, at, _, _ = levels[level + 1]
        buf[at] = total.astype(BF16)
        small_start(level + 1)

    def small_end():
        small_out[...] = small_sum(2)
        for level in range(3):
            buf, _, count, _ = levels[level]
            if count > 1:
                wait_bytes(buf.at[pl.ds(0, count - 1)], tsem.at[level, 0])

    last = MB - 1

    def add_grad(mb, block, value):
        at = slice(block * D, (block + 1) * D)
        if mb > 0:
            value = value + acc_ref[at]
        if mb < last:
            acc_ref[at] = value
        else:
            add_block(block, value)

    def add_small(mb, at, value):
        small_ref[at] = value if mb == 0 else small_ref[at] + value

    def cols_of(mb):
        cols = cols_ref[mb][0:TP]
        col = lambda n: cols[:, n : n + 1]
        return cols, col

    def backward(mb):
        cols, col = cols_of(mb)
        ggr = arrived("ggrad", mb)[...].reshape(G, 128)
        g = g_ref[mb].astype(F32)
        res = res_ref[mb]
        slot_at = lax.broadcasted_iota(jnp.int32, (TP, S), 1).astype(F32)
        lane_at = lax.broadcasted_iota(jnp.int32, (TP, 128), 1).astype(F32)
        expert_at = lax.broadcasted_iota(jnp.int32, (TP, G), 1).astype(F32)
        gp = cols[:, 0:G]
        gates_grad = jnp.zeros((TP, G), F32)
        pick = jnp.zeros((TP, S), F32)
        for kk in range(2):
            keep = col(G + 2 + kk)
            named = jnp.where(expert_at == col(G + 4 + kk), 1.0, 0.0)
            of_slot = jnp.where(
                lane_at == col(G + 8 + kk), mm_exact(named, ggr), 0.0
            )
            gate_grad = jnp.sum(of_slot, axis=-1, keepdims=True) * keep
            gates_grad = gates_grad + named * gate_grad
            pick = pick + jnp.where(slot_at == col(G + kk), 1.0, 0.0)
        inner = jnp.sum(gp * gates_grad, axis=-1, keepdims=True)
        logit_grad = (gp * (gates_grad - inner)).astype(BF16)
        add_small(mb, slice(0, G), mm(logit_grad, n2_ref[mb], 0, 0))
        bgr = arrived("back", mb)[...].reshape(S, D)
        ngrad = mm(pick.astype(BF16), bgr) + mm(logit_grad, wrt_ref[...])
        hat2, rstd2 = normed_of(res)
        add_small(
            mb, slice(G, G + 1), jnp.sum(ngrad * hat2, axis=0, keepdims=True)
        )
        gain2 = gain2_ref[...].reshape(1, D)
        rgrad = g + norm_pull(hat2, rstd2, gain2, ngrad)
        branch = rgrad.astype(BF16)
        add_grad(mb, 3, mm(am_ref[mb], branch, 0, 0))
        mgrad = mm(branch, wattn_ref[...], 1, 1).astype(BF16)
        for pair in range(HEADS // 2):
            c = pair * 128
            mg = mgrad[:, c : c + 128]
            dvs = [
                mm(p_ref[mb, 2 * pair + half].astype(BF16), mg, 0, 0)
                for half in range(2)
            ]
            dq_ref[:, 2 * D + c : 2 * D + c + 128] = jnp.where(
                low_half, dvs[0], dvs[1]
            ).astype(BF16)
        n1 = n1_ref[mb]
        add_grad(mb, 2, mm(n1, dq_ref[:, 2 * D : 3 * D], 0, 0))
        if mb == last and len(chunks) > 1:
            sum_start(chunks[0])
        for pair in range(HEADS // 2):
            c = pair * 128
            q = qkv_ref[mb, :, c : c + 128]
            k = qkv_ref[mb, :, D + c : D + c + 128]
            v = qkv_ref[mb, :, 2 * D + c : 2 * D + c + 128]
            mg = mgrad[:, c : c + 128]
            dqs, dks = [], []
            for half in range(2):
                mine = low_half if half == 0 else jnp.logical_not(low_half)
                mgh = jnp.where(mine, mg, jnp.zeros_like(mg))
                p = p_ref[mb, 2 * pair + half]
                dp_ = mm(mgh, v, 1, 1)
                delta = jnp.sum(p * dp_, axis=-1, keepdims=True)
                ds = (p * (dp_ - delta) * HD**-0.5).astype(BF16)
                dqs.append(mm(ds, k))
                dks.append(mm(ds, q, 0, 0))
            for n, parts in enumerate((dqs, dks)):
                dq_ref[:, n * D + c : n * D + c + 128] = jnp.where(
                    low_half, parts[0], parts[1]
                ).astype(BF16)
        for n in range(2):
            add_grad(mb, n, mm(n1, dq_ref[:, n * D : (n + 1) * D], 0, 0))
        if mb == last:
            sum_start(chunks[-1])
            if len(chunks) > 1:
                sum_pairs(chunks[0])
        fgrad = mm(dq_ref[...], wqkv_ref[...], 1, 1)
        hat, rstd = normed_of(x_ref[mb].astype(F32))
        add_small(
            mb, slice(G + 1, G + 2), jnp.sum(fgrad * hat, axis=0, keepdims=True)
        )
        gain1 = gain1_ref[...].reshape(1, D)
        ig_ref[mb] = rgrad + norm_pull(hat, rstd, gain1, fgrad)

    def combine(mb):
        _, col = cols_of(mb)
        made = arrived("made", mb)[...].reshape(S, D)
        slot_at = lax.broadcasted_iota(jnp.int32, (TP, S), 1).astype(F32)
        out = res_ref[mb]
        for kk in range(2):
            pick = jnp.where(slot_at == col(G + kk), 1.0, 0.0).astype(BF16)
            out = out + col(G + 6 + kk) * mm(pick, made)
        bo_ref[mb] = out

    forward(0)
    pl.semaphore_wait(barrier, G - 1 + R - 1)
    for kind in ("rows", "gate", "pull"):
        exchange(kind, 0)
    for mb in range(1, MB):
        forward(mb)
        for kind in ("rows", "gate", "pull"):
            exchange(kind, mb)
    ready(10, 11)
    for mb in range(MB):
        experts(mb)
        if mb == last:
            for m in range(MB):
                exchange("made", m)
        weight_grads(mb)
    swap_slices()
    small_ref[...] = jnp.zeros_like(small_ref)
    for mb in range(MB):
        backward(mb)
        if mb == 0:
            add_slices()
            hand_out(0)
    t1_ref[r] = small_ref[...].astype(BF16)
    small_start(0)
    if len(chunks) > 1:
        sum_plane(chunks[0])
    sum_pairs(chunks[-1])
    small_next(0)
    if len(chunks) > 1:
        sum_z(chunks[0])
    combine(0)
    sum_plane(chunks[-1])
    small_next(1)
    hand_out(1)
    if len(chunks) > 1:
        spread_plane(chunks[0])
    for mb in range(1, MB):
        combine(mb)
    sum_z(chunks[-1])
    if len(chunks) > 1:
        spread_parts(chunks[0])
    spread_plane(chunks[-1])
    spread_parts(chunks[-1])
    small_end()
    for ck in chunks:
        sum_end(ck)

    for mat in range(2):
        wait_bytes(xs_ref.at[pl.ds(0, L), 0], xsem.at[1 + mat, 1])
        if L > 1:
            wait_bytes(xs_ref.at[pl.ds(0, L - 1), 0], xsem.at[1 + mat, 0])
    if R > 1:
        wait_bytes(x1_ref, xsem.at[0, 0])
    for n, kind in enumerate(KINDS):
        for mb in range(MB):
            sent = scratch[kind][0].at[mb, pl.ds(0, G - 1)]
            wait_bytes(sent, esem.at[n, mb, 0])


def on_device(
    groups,
    replicas,
    inputs,
    first_gain,
    w_qkv,
    w_attn,
    second_gain,
    w_router,
    expert_in,
    expert_out,
    expert_ids,
    slot_ids,
    dropped,
    out_grad,
):
    L, _, FF = expert_in.shape
    Z = groups
    R = replicas // L
    G = L * Z
    S = G * CAP
    FS = FF // replicas
    parts = R * L * Z
    groups_of_blocks = [(2, 3), (0, 1)]
    if 2 * D % parts or (2 * D // parts) % 8:
        groups_of_blocks = [(0, 1, 2, 3)]
    small_rows = -(-(G + 2) // SM) * SM
    rs_rows = -(-(G + 10) // 8) * 8
    pad = ((0, 0), (0, TP - SEQ), (0, 0))
    swap = lambda a: jnp.transpose(a, (0, 2, 1))
    operands = (
        jnp.pad(inputs, pad),
        jnp.pad(out_grad, pad),
        first_gain,
        second_gain,
        w_qkv,
        w_attn,
        w_router.T,
        swap(expert_ids),
        swap(slot_ids),
        swap(dropped),
        expert_in,
        expert_out,
    )
    vmem = pl.BlockSpec(memory_space=pltpu.VMEM)
    hbm = pl.BlockSpec(memory_space=pl.ANY)
    sds = jax.ShapeDtypeStruct
    V = pltpu.VMEM
    dma = pltpu.SemaphoreType.DMA
    scratch = {
        "loads": [V(a.shape, a.dtype) for a in operands[:10]]
        + [V((D, FF), BF16), V((FF, D), BF16)],
        "saved": [
            V((MB, TP, D), BF16),
            V((MB, TP, 3 * D), BF16),
            V((MB, HEADS, TP, TP), F32),
            V((MB, TP, D), BF16),
            V((MB, TP, D), F32),
            V((MB, TP, D), BF16),
        ],
        "work": [
            V((rs_rows, TL), F32),
            V((MB, TL, rs_rows), F32),
            V((S, FF), F32),
        ],
        "expert": [
            V((MB, S, FF), BF16),
            V((MB, S, FF), BF16),
            V((R, L, 2, FS, D), BF16),
            V((max(R - 1, 1), L, 2, FS, D), BF16),
            V((L, 2, FS, D), BF16),
            V((2, L, FF // L, D), F32),
        ],
        "grads": [
            V((TP, 3 * D), BF16),
            V((4 * D, D), F32),
            V((small_rows, D), F32),
            V((R, small_rows, D), BF16),
            V((L, small_rows, D), BF16),
            V((Z, small_rows, D), BF16),
        ],
        "gated": V((MB, S, D), BF16),
        "sems": [dma((12,)), dma((len(KINDS), MB, 2)), dma((3, 2)), dma((3, 2))],
    }
    for kind in KINDS:
        slim = kind in ("gate", "ggrad")
        shape = (MB, G, 1, 128) if slim else (MB, G, CAP, D)
        scratch[kind] = [V(shape, F32 if slim else BF16)] * 2
    scratch["chunks"] = []
    for blocks in groups_of_blocks:
        pr = len(blocks) * D // parts
        scratch["chunks"].append(
            {
                "src": V((parts, pr, D), BF16),
                "l1": V((max(R - 1, 1), L, Z, pr, D), BF16),
                "l2s": V((L, Z, pr, D), BF16),
                "l2": V((max(L - 1, 1), Z, pr, D), BF16),
                "l3s": V((Z, pr, D), BF16),
                "l3": V((max(Z - 1, 1), pr, D), BF16),
                "s1": dma((max(R - 1, 1), L)),
                "s2": dma((max(L - 1, 1),)),
                "send": dma((6,)),
                "recv": dma((6,)),
            }
        )
    leaves, tree = jax.tree.flatten(scratch)
    n_in, n_out = len(operands), 4 + len(groups_of_blocks)

    def body(*refs):
        ins, outs = refs[:n_in], refs[n_in : n_in + n_out]
        held = jax.tree.unflatten(tree, refs[n_in + n_out :])
        for n, blocks in enumerate(groups_of_blocks):
            ck = held["chunks"][n]
            ck["blocks"] = list(blocks)
            ck["out"] = outs[3 + n]
            ck["pr"] = len(blocks) * D // parts
        kernel((L, R, Z, G, FF), ins, outs, held)

    bo, ig, eg, *dense, small = pl.pallas_call(
        body,
        out_shape=(
            sds((MB, TP, D), F32),
            sds((MB, TP, D), F32),
            sds((L, 2, FS, D), BF16),
            *(
                sds((parts, len(blocks) * D // parts, D), BF16)
                for blocks in groups_of_blocks
            ),
            sds((small_rows, D), F32),
        ),
        in_specs=[hbm] * n_in,
        out_specs=[vmem] * n_out,
        scratch_shapes=leaves,
        compiler_params=pltpu.CompilerParams(
            collective_id=0, has_side_effects=True, vmem_limit_bytes=63 << 20
        ),
        name="block",
    )(*operands)
    blocks = {}
    for names, got in zip(groups_of_blocks, dense):
        got = got.reshape(len(names), D, D).astype(F32)
        for n, name in enumerate(names):
            blocks[name] = got[n]
    return (
        bo[:, :SEQ],
        ig[:, :SEQ],
        small[G + 1],
        jnp.concatenate([blocks[n] for n in range(3)], axis=1),
        blocks[3],
        small[G],
        small[:G].T,
        jnp.transpose(eg[:, 0].astype(F32), (0, 2, 1)),
        eg[:, 1].astype(F32),
    )


def solution(mesh):
    rows = P(None, ("dp", "expert"), None)
    split = P("expert", None, None)
    return jax.shard_map(
        functools.partial(on_device, mesh.shape["expert"], mesh.shape["dp"]),
        mesh=mesh,
        in_specs=(
            rows,
            P(),
            P(),
            P(),
            P(),
            P(),
            split,
            split,
            rows,
            rows,
            rows,
            rows,
        ),
        out_specs=(
            rows,
            rows,
            P(),
            P(),
            P(),
            P(),
            P(),
            P("expert", None, "dp"),
            P("expert", "dp", None),
        ),
        check_vma=False,
    )
```

```python
import functools
import math

import jax
import jax.numpy as jnp
from jax import lax
from jax.experimental import pallas as pl
from jax.experimental.pallas import tpu as pltpu
from jax.sharding import PartitionSpec as P

D = 384
HEADS = 6
HD = 64
SEQ = 197
MB = 2
CAP = 16
EPS = 1e-06
TP = 208
TL = 256
SM = 32
ROWS = (D, D, 256, 256, 256)
START = (0, D, 2 * D, 2 * D + 256, 2 * D + 512)
F32 = jnp.float32
BF16 = jnp.bfloat16
MESH = pl.DeviceIdType.MESH
KINDS = ("rows", "gate", "pull", "ggrad", "back", "made")


def mm(a, b, ca=1, cb=0):
    return lax.dot_general(
        a, b, (((ca,), (cb,)), ((), ())), preferred_element_type=F32
    )


def mm_exact(a, b):
    return lax.dot_general(
        a,
        b,
        (((1,), (0,)), ((), ())),
        preferred_element_type=F32,
        precision=lax.Precision.HIGHEST,
    )


def normed_of(rows):
    mean = jnp.sum(rows, axis=-1, keepdims=True) * (1.0 / D)
    centered = rows - mean
    var = jnp.sum(centered * centered, axis=-1, keepdims=True) * (1.0 / D)
    rstd = lax.rsqrt(var + EPS)
    return centered * rstd, rstd


def norm_pull(hat, rstd, gain, grad):
    scaled = grad * gain
    m1 = jnp.sum(scaled, axis=-1, keepdims=True) * (1.0 / D)
    m2 = jnp.sum(scaled * hat, axis=-1, keepdims=True) * (1.0 / D)
    return rstd * (scaled - m1 - hat * m2)


def kernel(dims, ins, outs, scratch):
    L, R, Z, G, FF = dims
    S = G * CAP
    FS = FF // (L * R)
    (
        x_hbm,
        g_hbm,
        gain1_hbm,
        gain2_hbm,
        wqkv_hbm,
        wattn_hbm,
        wrt_hbm,
        ids_hbm,
        slot_hbm,
        drop_hbm,
        win_hbm,
        wout_hbm,
    ) = ins
    bo_ref, ig_ref, gain1_out, wqkv_out, wattn_out, gain2_out, router_out = outs[:7]
    ein_out, eout_out = outs[7:]
    xin_ref, gin_ref, gain1_ref, gain2_ref = scratch["loads"][:4]
    wqkv_ref, wattn_ref, wrt_ref = scratch["loads"][4:7]
    ids_ref, slot_ref, drop_ref, w1, w2 = scratch["loads"][7:]
    x_ref, g_ref, n1_ref, qkv_ref, p_ref, am_ref, res_ref, n2_ref = scratch["saved"]
    rs_ref, cols_ref, slope_ref, pick_ref = scratch["work"]
    act_ref, hg_ref, xg_ref, x1_ref, xs_ref, eg_ref, gacc_ref = scratch["expert"]
    dq_ref, acc_ref, small_ref, t1_ref, t2_ref, t3_ref = scratch["grads"]
    lsem, esem, xsem, tsem = scratch["sems"]
    chunks = scratch["chunks"]
    dp = lax.axis_index("dp")
    z = lax.axis_index("expert")
    j = dp // R
    r = dp % R
    me = z * L + j

    def group_id(e):
        return ((e % L) * R + r, e // L)

    def plane_id(i):
        return (i * R + r, z)

    def part_id(rr):
        return (j * R + rr, z)

    def remote(src, dst, send_sem, recv_sem, device):
        pltpu.make_async_remote_copy(
            src_ref=src,
            dst_ref=dst,
            send_sem=send_sem,
            recv_sem=recv_sem,
            device_id=device,
            device_id_type=MESH,
        ).start()

    def wait_bytes(ref, sem):
        pltpu.make_async_copy(ref, ref, sem).wait()

    barrier = pltpu.get_barrier_semaphore()

    @pl.loop(1, G)
    def _(o):
        pl.semaphore_signal(
            barrier, inc=1, device_id=group_id((me + o) % G), device_id_type=MESH
        )

    for o in range(1, R):
        pl.semaphore_signal(
            barrier, inc=1, device_id=part_id((r + o) % R), device_id_type=MESH
        )

    loads = []
    sources = [
        x_hbm,
        g_hbm,
        gain1_hbm,
        gain2_hbm,
        wqkv_hbm,
        wattn_hbm,
        wrt_hbm,
        ids_hbm,
        slot_hbm,
        drop_hbm,
        win_hbm.at[j],
        wout_hbm.at[j],
    ]
    for n, (src, dst) in enumerate(zip(sources, scratch["loads"])):
        loads.append(pltpu.make_async_copy(src, dst, lsem.at[n]))
    for n in (0, 2, 4, 7, 8, 9, 1, 5, 3, 6, 10, 11):
        loads[n].start()

    def ready(*which):
        for n in which:
            loads[n].wait()

    low_half = lax.broadcasted_iota(jnp.int32, (TP, 128), 1) < HD
    key_ok = lax.broadcasted_iota(jnp.int32, (TP, TP), 1) < SEQ
    slot_lane = lax.broadcasted_iota(
        jnp.int32, (G, CAP, 128), 2
    ) == lax.broadcasted_iota(jnp.int32, (G, CAP, 128), 1)

    def exchange(kind, mb):
        send, recv = scratch[kind]
        send, recv = send.at[mb], recv.at[mb]
        n = KINDS.index(kind)
        pltpu.make_async_copy(send.at[me], recv.at[me], esem.at[n, mb, 1]).start()

        @pl.loop(1, G)
        def _(o):
            e = (me + o) % G
            remote(
                send.at[e],
                recv.at[me],
                esem.at[n, mb, 0],
                esem.at[n, mb, 1],
                group_id(e),
            )

    def arrived(kind, mb):
        recv = scratch[kind][1].at[mb]
        wait_bytes(recv, esem.at[KINDS.index(kind), mb, 1])
        return recv

    def row_of_slots(col):
        spread = jnp.where(slot_lane, col.reshape(G, CAP, 1), 0.0)
        return jnp.sum(spread, axis=1, keepdims=True)

    def slots_of_row(row):
        spread = jnp.where(slot_lane, row, 0.0)
        return jnp.sum(spread, axis=-1, keepdims=True).reshape(S, 1)

    def route(mb):
        if mb == 0:
            ready(7, 8, 9, 1)
        g_ref[mb, TP - 16 : TP] = jnp.zeros((16, D), BF16)
        g_ref[mb, 0:SEQ] = gin_ref[:, mb, :]
        ids = ids_ref[mb]
        drop = drop_ref[mb]
        slot = slot_ref[mb]
        flat = jnp.where(drop == 0, ids * CAP + slot, S)
        rs_ref[mb] = jnp.zeros_like(rs_ref[mb])
        rs_ref[mb, G : G + 2, 0:TP] = jnp.full((2, TP), S, F32)
        rs_ref[mb, G : G + 2, 0:SEQ] = flat.astype(F32)
        rs_ref[mb, G + 2 : G + 4, 0:SEQ] = 1.0 - drop.astype(F32)
        rs_ref[mb, G + 4 : G + 6, 0:SEQ] = ids.astype(F32)
        rs_ref[mb, G + 8 : G + 10, 0:SEQ] = slot.astype(F32)
        slot_of = lax.broadcasted_iota(jnp.int32, (S, TP), 0).astype(F32)
        hit0 = slot_of == rs_ref[mb, G : G + 1, 0:TP]
        hit1 = slot_of == rs_ref[mb, G + 1 : G + 2, 0:TP]
        pick = jnp.where(hit0, 1.0, jnp.where(hit1, 1.0, 0.0)).astype(BF16)
        pick_ref[mb] = pick
        scratch["pull"][0][mb] = mm(pick, g_ref[mb]).astype(BF16).reshape(G, CAP, D)

    def project(mb):
        if mb == 0:
            ready(0, 2, 4)
        x_ref[mb, TP - 16 : TP] = jnp.zeros((16, D), F32)
        x_ref[mb, 0:SEQ] = xin_ref[:, mb, :].astype(F32)
        hat, _ = normed_of(x_ref[mb])
        n1 = (hat * gain1_ref[...].reshape(1, D)).astype(BF16)
        n1_ref[mb] = n1
        qkv_ref[mb] = mm(n1, wqkv_ref[...]).astype(BF16)

    def forward(mb):
        for pair in range(HEADS // 2):
            c = pair * 128
            q = qkv_ref[mb, :, c : c + 128] * jnp.asarray(HD**-0.5, BF16)
            k = qkv_ref[mb, :, D + c : D + c + 128]
            v = qkv_ref[mb, :, 2 * D + c : 2 * D + c + 128]
            mixed = []
            for half in range(2):
                mine = low_half if half == 0 else jnp.logical_not(low_half)
                qh = jnp.where(mine, q, jnp.zeros_like(q))
                s = mm(qh, k, 1, 1)
                s = jnp.where(key_ok, s, -1e30)
                e = jnp.exp(s - jnp.max(s, axis=-1, keepdims=True))
                p = e / jnp.sum(e, axis=-1, keepdims=True)
                p_ref[mb, 2 * pair + half] = p
                mixed.append(mm(p.astype(BF16), v))
            am_ref[mb, :, c : c + 128] = jnp.where(
                low_half, mixed[0], mixed[1]
            ).astype(BF16)
        if mb == 0:
            ready(5, 3, 6)
        res = x_ref[mb] + mm(am_ref[mb], wattn_ref[...])
        res_ref[mb] = res
        hat2, _ = normed_of(res)
        n2 = (hat2 * gain2_ref[...].reshape(1, D)).astype(BF16)
        n2_ref[mb] = n2
        logits = mm(wrt_ref[...], n2, 1, 1)
        ex = jnp.exp(logits - jnp.max(logits, axis=0, keepdims=True))
        gp = ex / jnp.sum(ex, axis=0, keepdims=True)
        rs_ref[mb, 0:G, 0:TP] = gp
        expert_of = lax.broadcasted_iota(jnp.int32, (G, TP), 0).astype(F32)
        slot_of = lax.broadcasted_iota(jnp.int32, (S, TP), 0).astype(F32)
        gcol = jnp.zeros((S, 1), F32)
        for kk in range(2):
            flr = rs_ref[mb, G + kk : G + kk + 1, 0:TP]
            keep = rs_ref[mb, G + 2 + kk : G + 3 + kk, 0:TP]
            idr = rs_ref[mb, G + 4 + kk : G + 5 + kk, 0:TP]
            mine = jnp.where(expert_of == idr, gp, 0.0)
            gate = jnp.sum(mine, axis=0, keepdims=True) * keep
            rs_ref[mb, G + 6 + kk : G + 7 + kk, 0:TP] = gate
            hit = slot_of == flr
            gcol = gcol + jnp.sum(jnp.where(hit, gate, 0.0), axis=-1, keepdims=True)
        scratch["rows"][0][mb] = mm(pick_ref[mb], n2).astype(BF16).reshape(G, CAP, D)
        scratch["gate"][0][mb] = row_of_slots(gcol)
        exchange("rows", mb)
        exchange("gate", mb)
        cols_ref[mb] = rs_ref[mb].T

    def experts(mb):
        xs = arrived("rows", mb)[...].reshape(S, D)
        step = 384
        produced = jnp.zeros((S, D), F32)
        for c in range(0, FF, step):
            h = mm(xs, w1[:, c : c + step])
            sq = h * h
            t = jnp.tanh(0.7978845608028654 * (h + 0.044715 * (h * sq)))
            half = 0.5 * (1.0 + t)
            act = (h * half).astype(BF16)
            slope_ref[:, c : c + step] = half + 0.5 * h * (1.0 - t * t) * (
                0.7978845608028654 * (1.0 + 0.134145 * sq)
            )
            act_ref[mb, :, c : c + step] = act
            produced = produced + mm(act, w2[c : c + step, :])
        produced = produced.astype(BF16)
        scratch["made"][0][mb] = produced.reshape(G, CAP, D)
        gates = slots_of_row(arrived("gate", mb)[...])
        grow = arrived("pull", mb)[...].reshape(S, D).astype(F32)
        pg = (gates * grow).astype(BF16)
        scratch["gated"][mb] = pg
        gg = jnp.sum(grow * produced.astype(F32), axis=-1, keepdims=True)
        scratch["ggrad"][0][mb] = row_of_slots(gg)
        back = jnp.zeros((S, D), F32)
        for c in range(0, FF, step):
            ag = mm(pg, w2[c : c + step, :], 1, 1)
            hg = (ag * slope_ref[:, c : c + step]).astype(BF16)
            hg_ref[mb, :, c : c + step] = hg
            back = back + mm(hg, w1[:, c : c + step], 1, 1)
        scratch["back"][0][mb] = back.astype(BF16).reshape(G, CAP, D)
        exchange("ggrad", mb)
        exchange("back", mb)

    span = FF // L

    def weight_grads(mb):
        xs = scratch["rows"][1][mb].reshape(S, D)
        pg = scratch["gated"][mb]

        def part(i, carry):
            at = pl.ds(pl.multiple_of(i * span, 128), span)
            g1 = mm(hg_ref[mb, :, at], xs, 0, 0)
            g2 = mm(act_ref[mb, :, at], pg, 0, 0)
            if mb < MB - 1:
                if mb > 0:
                    g1 = g1 + gacc_ref[0, i]
                    g2 = g2 + gacc_ref[1, i]
                gacc_ref[0, i] = g1
                gacc_ref[1, i] = g2
            else:
                g1 = (g1 + gacc_ref[0, i]).astype(BF16)
                g2 = (g2 + gacc_ref[1, i]).astype(BF16)
                for rr in range(R):
                    xg_ref[rr, i, 0] = g1[rr * FS : (rr + 1) * FS]
                    xg_ref[rr, i, 1] = g2[rr * FS : (rr + 1) * FS]
            return carry

        lax.fori_loop(0, L, part, 0)

    def swap_slices():
        for o in range(1, R):
            rr = (r + o) % R
            remote(
                xg_ref.at[rr],
                x1_ref.at[R - o - 1],
                xsem.at[0, 0],
                xsem.at[0, 1],
                part_id(rr),
            )

    def add_slices():
        if R > 1:
            wait_bytes(x1_ref, xsem.at[0, 1])

        def part(i, carry):
            total = xg_ref[r, i].astype(F32)
            for o in range(R - 1):
                total = total + x1_ref[o, i].astype(F32)
            xs_ref[i] = total.astype(BF16)
            return carry

        lax.fori_loop(0, L, part, 0)

    def hand_out(mat):
        for o in range(1, L):
            i = (j + o) % L
            remote(
                xs_ref.at[i, mat],
                eg_ref.at[j, mat],
                xsem.at[1 + mat, 0],
                xsem.at[1 + mat, 1],
                plane_id(i),
            )
        pltpu.make_async_copy(
            xs_ref.at[j, mat], eg_ref.at[j, mat], xsem.at[1 + mat, 1]
        ).start()

    def slices_out(mat):
        wait_bytes(xs_ref.at[pl.ds(0, L), 0], xsem.at[1 + mat, 1])
        out = (ein_out, eout_out)[mat]

        def part(i, carry):
            out[i] = eg_ref[i, mat].astype(F32)
            return carry

        lax.fori_loop(0, L, part, 0)

    def chunk_of(block):
        for ck in chunks:
            at = 0
            for name in ck["blocks"]:
                if name == block:
                    return ck, at
                at += ROWS[name]

    def add_block(block, value):
        ck, at = chunk_of(block)
        src, pr = ck["src"], ck["pr"]
        at = at // pr
        count = ROWS[block] // pr
        if pr % 8 == 0:
            src[at : at + count] = value.reshape(count, pr, D).astype(BF16)
        else:
            first = START[block]
            acc_ref[first : first + ROWS[block]] = value
            rows = math.lcm(pr, 8)

            @pl.loop(0, ROWS[block] // rows)
            def _(n):
                piece = acc_ref[pl.ds(pl.multiple_of(first + n * rows, 8), rows)]
                piece = piece.astype(BF16)
                for m in range(rows // pr):
                    src[at + n * (rows // pr) + m] = piece[m * pr : (m + 1) * pr]

    def total_of(block):
        ck, at = chunk_of(block)
        out, pr = ck["out"], ck["pr"]
        at = at // pr
        count = ROWS[block] // pr
        if pr % 8 == 0:
            return out[at : at + count].astype(F32).reshape(ROWS[block], D)
        first = START[block]
        rows = math.lcm(pr, 8)

        @pl.loop(0, ROWS[block] // rows)
        def _(n):
            pieces = [out[at + n * (rows // pr) + m] for m in range(rows // pr)]
            spot = pl.ds(pl.multiple_of(first + n * rows, 8), rows)
            acc_ref[spot] = jnp.concatenate(
                [piece.astype(F32) for piece in pieces], axis=0
            )

        return acc_ref[first : first + ROWS[block]]

    def store_totals(ck):
        for block in ck["blocks"]:
            total = total_of(block)
            if block == 0:
                wattn_out[...] = total
            elif block == 1:
                wqkv_out[:, 2 * D : 3 * D] = total
            else:
                for n in range(2):
                    c = n * D + (block - 2) * 128
                    for m in range(3):
                        wqkv_out[m * 128 : (m + 1) * 128, c : c + 128] = total[
                            n * 128 : (n + 1) * 128, m * 128 : (m + 1) * 128
                        ]

    def sum_start(ck):
        for n in range(1, L + 1):
            i = (j + n) % L
            for o in range(1, R):
                rr = (r + o) % R
                remote(
                    ck["src"].at[pl.ds((rr * L + i) * Z, Z)],
                    ck["l1"].at[R - o - 1, i],
                    ck["send"].at[0],
                    ck["s1"].at[R - o - 1, i],
                    part_id(rr),
                )

    def sum_pairs(ck):
        for n in range(1, L + 1):
            i = (j + n) % L
            total = ck["src"][pl.ds((r * L + i) * Z, Z)].astype(F32)
            for o in range(R - 1):
                wait_bytes(ck["l1"].at[o, i], ck["s1"].at[o, i])
                total = total + ck["l1"][o, i].astype(F32)
            ck["l2s"][i] = total.astype(BF16)
            if n < L:
                remote(
                    ck["l2s"].at[i],
                    ck["l2"].at[L - n - 1],
                    ck["send"].at[1],
                    ck["recv"].at[1],
                    plane_id(i),
                )

    def sum_plane(ck):
        if L > 1:
            wait_bytes(ck["l2"], ck["recv"].at[1])
        for n in range(Z - 1, -1, -1):
            zz = (z + n) % Z
            total = ck["l2s"][j, zz].astype(F32)
            for o in range(L - 1):
                total = total + ck["l2"][o, zz].astype(F32)
            ck["l3s"][zz] = total.astype(BF16)
            if n > 0:
                remote(
                    ck["l3s"].at[zz],
                    ck["l3"].at[Z - n - 1],
                    ck["send"].at[2],
                    ck["recv"].at[2],
                    (dp, zz),
                )

    def sum_z(ck):
        out = ck["out"]
        if Z > 1:
            wait_bytes(ck["l3"], ck["recv"].at[2])
        total = ck["l3s"][z].astype(F32)
        for o in range(Z - 1):
            total = total + ck["l3"][o].astype(F32)
        mine = (r * L + j) * Z + z
        out[mine] = total.astype(BF16)
        for n in range(Z - 1, 0, -1):
            remote(
                out.at[mine],
                out.at[mine],
                ck["send"].at[3],
                ck["recv"].at[3],
                (dp, (z + n) % Z),
            )

    def spread_plane(ck):
        out = ck["out"]
        if Z > 1:
            wait_bytes(ck["l3"], ck["recv"].at[3])
        mine = pl.ds((r * L + j) * Z, Z)
        for n in range(1, L):
            remote(
                out.at[mine],
                out.at[mine],
                ck["send"].at[4],
                ck["s2"].at[L - n - 1],
                plane_id((j + n) % L),
            )
        spread_part(ck, j)

    def spread_part(ck, i):
        out = ck["out"]
        at = pl.ds((r * L + i) * Z, Z)
        for o in range(1, R):
            remote(
                out.at[at],
                out.at[at],
                ck["send"].at[5],
                ck["recv"].at[5],
                part_id((r + o) % R),
            )

    def spread_parts(ck):
        for n in range(1, L):
            wait_bytes(ck["l2"].at[n - 1], ck["s2"].at[n - 1])
            spread_part(ck, (j + n) % L)

    def sum_end(ck):
        if R > 1:
            wait_bytes(ck["l1"], ck["recv"].at[5])
            wait_bytes(ck["l1"], ck["send"].at[0])
            wait_bytes(ck["l1"], ck["send"].at[5])
        if L > 1:
            wait_bytes(ck["l2"], ck["send"].at[1])
            wait_bytes(ck["l2"], ck["send"].at[4])
        if Z > 1:
            wait_bytes(ck["l3"], ck["send"].at[2])
            wait_bytes(ck["l3"], ck["send"].at[3])

    levels = ((t1_ref, r, R, part_id), (t2_ref, j, L, plane_id), (t3_ref, z, Z, None))

    def small_start(level):
        buf, at, count, ident = levels[level]
        for o in range(1, count):
            to = (at + o) % count
            remote(
                buf.at[at],
                buf.at[at],
                tsem.at[level, 0],
                tsem.at[level, 1],
                (dp, to) if ident is None else ident(to),
            )

    def small_sum(level):
        buf, _, count, _ = levels[level]
        if count > 1:
            wait_bytes(buf.at[pl.ds(0, count - 1)], tsem.at[level, 1])
        total = buf[0].astype(F32)
        for n in range(1, count):
            total = total + buf[n].astype(F32)
        return total

    def small_next(level):
        total = small_sum(level)
        buf, at, _, _ = levels[level + 1]
        buf[at] = total.astype(BF16)
        small_start(level + 1)

    def small_end():
        total = small_sum(2)
        router_out[...] = total[0:G]
        gain2_out[...] = total[G]
        gain1_out[...] = total[G + 1]
        for level in range(3):
            buf, _, count, _ = levels[level]
            if count > 1:
                wait_bytes(buf.at[pl.ds(0, count - 1)], tsem.at[level, 0])

    last = MB - 1

    def add_grad(mb, block, value):
        at = slice(START[block], START[block] + ROWS[block])
        if mb > 0:
            value = value + acc_ref[at]
        if mb < last:
            acc_ref[at] = value
        else:
            add_block(block, value)

    def add_small(mb, at, value):
        small_ref[at] = value if mb == 0 else small_ref[at] + value

    def cols_of(mb):
        cols = cols_ref[mb][0:TP]
        col = lambda n: cols[:, n : n + 1]
        return cols, col

    def backward(mb):
        cols, col = cols_of(mb)
        ggr = arrived("ggrad", mb)[...].reshape(G, 128)
        g = g_ref[mb].astype(F32)
        res = res_ref[mb]
        slot_at = lax.broadcasted_iota(jnp.int32, (TP, S), 1).astype(F32)
        lane_at = lax.broadcasted_iota(jnp.int32, (TP, 128), 1).astype(F32)
        expert_at = lax.broadcasted_iota(jnp.int32, (TP, G), 1).astype(F32)
        gp = cols[:, 0:G]
        gates_grad = jnp.zeros((TP, G), F32)
        pick = jnp.zeros((TP, S), F32)
        for kk in range(2):
            keep = col(G + 2 + kk)
            named = jnp.where(expert_at == col(G + 4 + kk), 1.0, 0.0)
            of_slot = jnp.where(
                lane_at == col(G + 8 + kk), mm_exact(named, ggr), 0.0
            )
            gate_grad = jnp.sum(of_slot, axis=-1, keepdims=True) * keep
            gates_grad = gates_grad + named * gate_grad
            pick = pick + jnp.where(slot_at == col(G + kk), 1.0, 0.0)
        inner = jnp.sum(gp * gates_grad, axis=-1, keepdims=True)
        logit_grad = (gp * (gates_grad - inner)).astype(BF16)
        add_small(mb, slice(0, G), mm(logit_grad, n2_ref[mb], 0, 0))
        bgr = arrived("back", mb)[...].reshape(S, D)
        ngrad = mm(pick.astype(BF16), bgr) + mm(logit_grad, wrt_ref[...])
        hat2, rstd2 = normed_of(res)
        add_small(
            mb, slice(G, G + 1), jnp.sum(ngrad * hat2, axis=0, keepdims=True)
        )
        gain2 = gain2_ref[...].reshape(1, D)
        rgrad = g + norm_pull(hat2, rstd2, gain2, ngrad)
        branch = rgrad.astype(BF16)
        add_grad(mb, 0, mm(am_ref[mb], branch, 0, 0))
        mgrad = mm(branch, wattn_ref[...], 1, 1).astype(BF16)
        for pair in range(HEADS // 2):
            c = pair * 128
            mg = mgrad[:, c : c + 128]
            dvs = [
                mm(p_ref[mb, 2 * pair + half].astype(BF16), mg, 0, 0)
                for half in range(2)
            ]
            dq_ref[:, 2 * D + c : 2 * D + c + 128] = jnp.where(
                low_half, dvs[0], dvs[1]
            ).astype(BF16)
        n1 = n1_ref[mb]
        add_grad(mb, 1, mm(n1, dq_ref[:, 2 * D : 3 * D], 0, 0))
        piped = mb == last and len(chunks) > 1
        if piped:
            sum_start(chunks[0])
        for pair in range(HEADS // 2):
            c = pair * 128
            q = qkv_ref[mb, :, c : c + 128]
            k = qkv_ref[mb, :, D + c : D + c + 128]
            v = qkv_ref[mb, :, 2 * D + c : 2 * D + c + 128]
            mg = mgrad[:, c : c + 128]
            dqs, dks = [], []
            for half in range(2):
                mine = low_half if half == 0 else jnp.logical_not(low_half)
                mgh = jnp.where(mine, mg, jnp.zeros_like(mg))
                p = p_ref[mb, 2 * pair + half]
                dp_ = mm(mgh, v, 1, 1)
                delta = jnp.sum(p * dp_, axis=-1, keepdims=True)
                ds = (p * (dp_ - delta) * HD**-0.5).astype(BF16)
                dqs.append(mm(ds, k))
                dks.append(mm(ds, q, 0, 0))
            grads = [
                jnp.where(low_half, parts[0], parts[1]).astype(BF16)
                for parts in (dqs, dks)
            ]
            for n in range(2):
                dq_ref[:, n * D + c : n * D + c + 128] = grads[n]
            wgrad = mm(n1, jnp.concatenate(grads, axis=1), 0, 0)
            packed = jnp.concatenate(
                [
                    jnp.concatenate(
                        [
                            wgrad[m * 128 : (m + 1) * 128, n * 128 : (n + 1) * 128]
                            for m in range(3)
                        ],
                        axis=1,
                    )
                    for n in range(2)
                ],
                axis=0,
            )
            add_grad(mb, 2 + pair, packed)
            if piped:
                sum_start(chunks[1 + pair])
                sum_pairs(chunks[pair])
        if mb == last and not piped:
            sum_start(chunks[0])
        fgrad = mm(dq_ref[...], wqkv_ref[...], 1, 1)
        hat, rstd = normed_of(x_ref[mb])
        add_small(
            mb, slice(G + 1, G + 2), jnp.sum(fgrad * hat, axis=0, keepdims=True)
        )
        gain1 = gain1_ref[...].reshape(1, D)
        grad = rgrad + norm_pull(hat, rstd, gain1, fgrad)
        ig_ref[:, mb, :] = grad[0:SEQ]

    def combine(mb):
        _, col = cols_of(mb)
        made = arrived("made", mb)[...].reshape(S, D)
        slot_at = lax.broadcasted_iota(jnp.int32, (TP, S), 1).astype(F32)
        out = res_ref[mb]
        for kk in range(2):
            pick = jnp.where(slot_at == col(G + kk), 1.0, 0.0).astype(BF16)
            out = out + col(G + 6 + kk) * mm(pick, made)
        bo_ref[:, mb, :] = out[0:SEQ]

    project(0)
    route(0)
    pl.semaphore_wait(barrier, G - 1 + R - 1)
    exchange("pull", 0)
    forward(0)
    for mb in range(1, MB):
        project(mb)
        route(mb)
        forward(mb)
        exchange("pull", mb)
    ready(10, 11)
    for mb in range(MB):
        experts(mb)
        if mb == last:
            for m in range(MB):
                exchange("made", m)
        weight_grads(mb)
    swap_slices()
    small_ref[...] = jnp.zeros_like(small_ref)
    for mb in range(MB):
        backward(mb)
        if mb == 0:
            add_slices()
            hand_out(0)
    t1_ref[r] = small_ref[...].astype(BF16)
    small_start(0)
    sum_pairs(chunks[-1])
    combine(0)
    small_next(0)
    for ck in chunks:
        sum_plane(ck)
    hand_out(1)
    for mb in range(1, MB):
        combine(mb)
    small_next(1)
    for ck in chunks:
        sum_z(ck)
    slices_out(0)
    for ck in chunks:
        spread_plane(ck)
    slices_out(1)
    small_end()
    for ck in chunks:
        spread_parts(ck)
    for ck in chunks:
        sum_end(ck)
        store_totals(ck)

    for mat in range(2):
        if L > 1:
            wait_bytes(xs_ref.at[pl.ds(0, L - 1), 0], xsem.at[1 + mat, 0])
    if R > 1:
        wait_bytes(x1_ref, xsem.at[0, 0])
    for n, kind in enumerate(KINDS):
        for mb in range(MB):
            sent = scratch[kind][0].at[mb, pl.ds(0, G - 1)]
            wait_bytes(sent, esem.at[n, mb, 0])


def on_device(
    groups,
    replicas,
    inputs,
    first_gain,
    w_qkv,
    w_attn,
    second_gain,
    w_router,
    expert_in,
    expert_out,
    expert_ids,
    slot_ids,
    dropped,
    out_grad,
):
    L, _, FF = expert_in.shape
    Z = groups
    R = replicas // L
    G = L * Z
    S = G * CAP
    FS = FF // replicas
    parts = R * L * Z
    groups_of_blocks = [(0, 1), (2,), (3,), (4,)]
    if any(n % (8 * parts) for n in ROWS[2:]):
        groups_of_blocks = [(0, 1, 2, 3, 4)]
    rows_of = [sum(ROWS[n] for n in blocks) for blocks in groups_of_blocks]
    small_rows = -(-(G + 2) // SM) * SM
    rs_rows = -(-(G + 10) // 8) * 8
    swap = lambda a: jnp.transpose(a, (0, 2, 1))
    turn = lambda a: jnp.transpose(a, (1, 0, 2))
    operands = (
        turn(inputs),
        turn(out_grad),
        first_gain,
        second_gain,
        w_qkv,
        w_attn,
        w_router.T,
        swap(expert_ids),
        swap(slot_ids),
        swap(dropped),
        expert_in,
        expert_out,
    )
    vmem = pl.BlockSpec(memory_space=pltpu.VMEM)
    hbm = pl.BlockSpec(memory_space=pltpu.HBM)
    sds = jax.ShapeDtypeStruct
    V = pltpu.VMEM
    dma = pltpu.SemaphoreType.DMA
    scratch = {
        "loads": [V(a.shape, a.dtype) for a in operands[:10]]
        + [V((D, FF), BF16), V((FF, D), BF16)],
        "saved": [
            V((MB, TP, D), F32),
            V((MB, TP, D), BF16),
            V((MB, TP, D), BF16),
            V((MB, TP, 3 * D), BF16),
            V((MB, HEADS, TP, TP), F32),
            V((MB, TP, D), BF16),
            V((MB, TP, D), F32),
            V((MB, TP, D), BF16),
        ],
        "work": [
            V((MB, rs_rows, TL), F32),
            V((MB, TL, rs_rows), F32),
            V((S, FF), F32),
            V((MB, S, TP), BF16),
        ],
        "expert": [
            V((MB, S, FF), BF16),
            V((MB, S, FF), BF16),
            V((R, L, 2, FS, D), BF16),
            V((max(R - 1, 1), L, 2, FS, D), BF16),
            V((L, 2, FS, D), BF16),
            V((L, 2, FS, D), BF16),
            V((2, L, FF // L, D), F32),
        ],
        "grads": [
            V((TP, 3 * D), BF16),
            V((4 * D, D), F32),
            V((small_rows, D), F32),
            V((R, small_rows, D), BF16),
            V((L, small_rows, D), BF16),
            V((Z, small_rows, D), BF16),
        ],
        "gated": V((MB, S, D), BF16),
        "sems": [dma((12,)), dma((len(KINDS), MB, 2)), dma((3, 2)), dma((3, 2))],
    }
    for kind in KINDS:
        slim = kind in ("gate", "ggrad")
        shape = (MB, G, 1, 128) if slim else (MB, G, CAP, D)
        scratch[kind] = [V(shape, F32 if slim else BF16)] * 2
    scratch["chunks"] = []
    for rows in rows_of:
        pr = rows // parts
        scratch["chunks"].append(
            {
                "src": V((parts, pr, D), BF16),
                "out": V((parts, pr, D), BF16),
                "l1": V((max(R - 1, 1), L, Z, pr, D), BF16),
                "l2s": V((L, Z, pr, D), BF16),
                "l2": V((max(L - 1, 1), Z, pr, D), BF16),
                "l3s": V((Z, pr, D), BF16),
                "l3": V((max(Z - 1, 1), pr, D), BF16),
                "s1": dma((max(R - 1, 1), L)),
                "s2": dma((max(L - 1, 1),)),
                "send": dma((6,)),
                "recv": dma((6,)),
            }
        )
    leaves, tree = jax.tree.flatten(scratch)
    results = (
        sds((SEQ, MB, D), F32),
        sds((SEQ, MB, D), F32),
        sds((D,), F32),
        sds((D, 3 * D), F32),
        sds((D, D), F32),
        sds((D,), F32),
        sds((G, D), F32),
        sds((L, FS, D), F32),
        sds((L, FS, D), F32),
    )
    n_in, n_out = len(operands), len(results)

    def body(*refs):
        ins, outs = refs[:n_in], refs[n_in : n_in + n_out]
        held = jax.tree.unflatten(tree, refs[n_in + n_out :])
        for ck, blocks, rows in zip(held["chunks"], groups_of_blocks, rows_of):
            ck["blocks"] = blocks
            ck["pr"] = rows // parts
        kernel((L, R, Z, G, FF), ins, outs, held)

    held = pl.pallas_call(
        body,
        out_shape=results,
        in_specs=[hbm] * n_in,
        out_specs=[vmem] * n_out,
        scratch_shapes=leaves,
        compiler_params=pltpu.CompilerParams(
            collective_id=0, has_side_effects=True, vmem_limit_bytes=48 << 20
        ),
        name="block",
    )(*(pltpu.with_memory_space_constraint(a, pltpu.HBM) for a in operands))

    def put_out(*refs):
        ins, outs, sem = refs[:n_out], refs[n_out:-1], refs[-1]
        copies = [
            pltpu.make_async_copy(src, dst, sem.at[n])
            for n, (src, dst) in enumerate(zip(ins, outs))
        ]
        for copy in copies:
            copy.start()
        for copy in copies:
            copy.wait()

    bo, ig, gain1, wqkv, wattn, gain2, router, ein, eout = pl.pallas_call(
        put_out,
        out_shape=results,
        in_specs=[vmem] * n_out,
        out_specs=[hbm] * n_out,
        scratch_shapes=[dma((n_out,))],
        compiler_params=pltpu.CompilerParams(vmem_limit_bytes=1 << 20),
        name="put_out",
    )(*held)
    return (
        turn(bo),
        turn(ig),
        gain1,
        wqkv,
        wattn,
        gain2,
        router.T,
        jnp.transpose(ein, (0, 2, 1)),
        eout,
    )


def solution(mesh):
    rows = P(None, ("dp", "expert"), None)
    split = P("expert", None, None)
    return jax.shard_map(
        functools.partial(on_device, mesh.shape["expert"], mesh.shape["dp"]),
        mesh=mesh,
        in_specs=(
            rows,
            P(),
            P(),
            P(),
            P(),
            P(),
            split,
            split,
            rows,
            rows,
            rows,
            rows,
        ),
        out_specs=(
            rows,
            rows,
            P(),
            P(),
            P(),
            P(),
            P(),
            P("expert", None, "dp"),
            P("expert", "dp", None),
        ),
        check_vma=False,
    )
```

```python
import functools
import math

import jax
import jax.numpy as jnp
from jax import lax
from jax.experimental import pallas as pl
from jax.experimental.pallas import tpu as pltpu
from jax.sharding import PartitionSpec as P

D = 384
HEADS = 6
HD = 64
SEQ = 197
MB = 2
CAP = 16
EPS = 1e-06
TP = 208
TL = 256
SM = 32
ROWS = (256, 128, 128, 256, 256, 256, 256)
START = (0, 256, 384, 512, 768, 1024, 1280)
CHUNKS = ((0,), (1, 2), (3,), (4,), (5,), (6,))
F32 = jnp.float32
BF16 = jnp.bfloat16
MESH = pl.DeviceIdType.MESH
EARLY = 2
Z_TIMES = ((3.5, 1.5), (7.5, 1.5), (11.0, 1.5), (15.5, 1.2))
XY_TIMES = ((3.0, 0.9), (8.0, 0.9), (12.0, 0.8), (15.5, 0.8))
X_TIMES = (7.1, 8.2, 9.1, 10.0)
KINDS = ("rows", "gate", "pull", "ggrad", "back", "made")


def mm(a, b, ca=1, cb=0):
    return lax.dot_general(
        a, b, (((ca,), (cb,)), ((), ())), preferred_element_type=F32
    )


def mm_exact(a, b):
    return lax.dot_general(
        a,
        b,
        (((1,), (0,)), ((), ())),
        preferred_element_type=F32,
        precision=lax.Precision.HIGHEST,
    )


def normed_of(rows):
    mean = jnp.sum(rows, axis=-1, keepdims=True) * (1.0 / D)
    centered = rows - mean
    var = jnp.sum(centered * centered, axis=-1, keepdims=True) * (1.0 / D)
    rstd = lax.rsqrt(var + EPS)
    return centered * rstd, rstd


def norm_pull(hat, rstd, gain, grad):
    scaled = grad * gain
    m1 = jnp.sum(scaled, axis=-1, keepdims=True) * (1.0 / D)
    m2 = jnp.sum(scaled * hat, axis=-1, keepdims=True) * (1.0 / D)
    return rstd * (scaled - m1 - hat * m2)


def kernel(dims, ins, outs, scratch):
    L, R, Z, G, FF = dims
    S = G * CAP
    FS = FF // (L * R)
    (
        x_hbm,
        g_hbm,
        gain1_hbm,
        gain2_hbm,
        wqkv_hbm,
        wattn_hbm,
        wrt_hbm,
        ids_hbm,
        slot_hbm,
        drop_hbm,
        win_hbm,
        wout_hbm,
    ) = ins
    bo_ref, ig_ref, gain1_out, wqkv_out, wattn_out, gain2_out, router_out = outs[:7]
    ein_out, eout_out = outs[7:]
    xin_ref, gin_ref, gain1_ref, gain2_ref = scratch["loads"][:4]
    wqkv_ref, wattn_ref, wrt_ref = scratch["loads"][4:7]
    ids_ref, slot_ref, drop_ref, w1, w2 = scratch["loads"][7:]
    x_ref, g_ref, n1_ref, qkv_ref, p_ref, am_ref, res_ref, n2_ref = scratch["saved"]
    rs_ref, cols_ref, slope_ref, pick_ref = scratch["work"]
    act_ref, hg_ref, xg_ref, x1_ref, xs_ref, eg_ref, gacc_ref = scratch["expert"]
    dq_ref, held_rgrad, acc_ref, small_ref, t1_ref, t2_ref, t3_ref = scratch["grads"]
    lsem, esem, xsem, tsem, ssem, x1sem = scratch["sems"]
    sums_ref = scratch["sums"]
    chunks = scratch["chunks"]
    last = MB - 1
    dp = lax.axis_index("dp")
    z = lax.axis_index("expert")
    j = dp // R
    r = dp % R
    me = z * L + j

    def group_id(e):
        return ((e % L) * R + r, e // L)

    def plane_id(i):
        return (i * R + r, z)

    def part_id(rr):
        return (j * R + rr, z)

    def remote(src, dst, send_sem, recv_sem, device):
        pltpu.make_async_remote_copy(
            src_ref=src,
            dst_ref=dst,
            send_sem=send_sem,
            recv_sem=recv_sem,
            device_id=device,
            device_id_type=MESH,
        ).start()

    def wait_bytes(ref, sem):
        pltpu.make_async_copy(ref, ref, sem).wait()

    for n, ck in enumerate(chunks):
        ck["src"] = sums_ref.at[pl.ds(n * G * R, G * R)]
        plane = (j, L, plane_id)
        along = (z, Z, lambda i: (dp, i))
        ck["dims"] = (along, plane) if ck["z_first"] else (plane, along)

    barrier = pltpu.get_barrier_semaphore()

    @pl.loop(1, G)
    def _(o):
        pl.semaphore_signal(
            barrier, inc=1, device_id=group_id((me + o) % G), device_id_type=MESH
        )

    for o in range(1, R):
        pl.semaphore_signal(
            barrier, inc=1, device_id=part_id((r + o) % R), device_id_type=MESH
        )

    loads = []
    sources = [
        x_hbm,
        g_hbm,
        gain1_hbm,
        gain2_hbm,
        wqkv_hbm,
        wattn_hbm,
        wrt_hbm,
        ids_hbm,
        slot_hbm,
        drop_hbm,
        win_hbm.at[j],
        wout_hbm.at[j],
    ]
    for n, (src, dst) in enumerate(zip(sources, scratch["loads"])):
        loads.append(pltpu.make_async_copy(src, dst, lsem.at[n]))
    for n in (0, 2, 4, 7, 8, 9, 1, 5, 3, 6, 10, 11):
        loads[n].start()

    def ready(*which):
        for n in which:
            loads[n].wait()

    low_half = lax.broadcasted_iota(jnp.int32, (TP, 128), 1) < HD
    key_ok = lax.broadcasted_iota(jnp.int32, (TP, TP), 1) < SEQ
    slot_lane = lax.broadcasted_iota(
        jnp.int32, (G, CAP, 128), 2
    ) == lax.broadcasted_iota(jnp.int32, (G, CAP, 128), 1)

    def exchange(*which):
        legs = []
        for kind, mb in which:
            send, recv = scratch[kind]
            sems = esem.at[KINDS.index(kind), mb]
            legs.append((send.at[mb], recv.at[mb], sems))
        for send, recv, sems in legs:
            pltpu.make_async_copy(send.at[me], recv.at[me], sems.at[1]).start()

        @pl.loop(1, G)
        def _(o):
            e = (me + o) % G
            to = group_id(e)
            for send, recv, sems in legs:
                remote(send.at[e], recv.at[me], sems.at[0], sems.at[1], to)

    def for_core(core, what):
        pl.when(dp % 2 == core)(what)

    def left(*which):
        for kind, mb in which:
            sent = scratch[kind][0].at[mb, pl.ds(0, G - 1)]
            wait_bytes(sent, esem.at[KINDS.index(kind), mb, 0])

    def arrived(kind, mb):
        recv = scratch[kind][1].at[mb]
        wait_bytes(recv, esem.at[KINDS.index(kind), mb, 1])
        return recv

    def row_of_slots(col):
        spread = jnp.where(slot_lane, col.reshape(G, CAP, 1), 0.0)
        return jnp.sum(spread, axis=1, keepdims=True)

    def slots_of_row(row):
        spread = jnp.where(slot_lane, row, 0.0)
        return jnp.sum(spread, axis=-1, keepdims=True).reshape(S, 1)

    def route(mb):
        if mb == 0:
            ready(7, 8, 9, 1)
        g_ref[mb, TP - 16 : TP] = jnp.zeros((16, D), BF16)
        g_ref[mb, 0:SEQ] = gin_ref[:, mb, :]
        ids = ids_ref[mb]
        drop = drop_ref[mb]
        slot = slot_ref[mb]
        flat = jnp.where(drop == 0, ids * CAP + slot, S)
        rs_ref[mb] = jnp.zeros_like(rs_ref[mb])
        rs_ref[mb, G : G + 2, 0:TP] = jnp.full((2, TP), S, F32)
        rs_ref[mb, G : G + 2, 0:SEQ] = flat.astype(F32)
        rs_ref[mb, G + 2 : G + 4, 0:SEQ] = 1.0 - drop.astype(F32)
        rs_ref[mb, G + 4 : G + 6, 0:SEQ] = ids.astype(F32)
        rs_ref[mb, G + 8 : G + 10, 0:SEQ] = slot.astype(F32)
        slot_of = lax.broadcasted_iota(jnp.int32, (S, TP), 0).astype(F32)
        hit0 = slot_of == rs_ref[mb, G : G + 1, 0:TP]
        hit1 = slot_of == rs_ref[mb, G + 1 : G + 2, 0:TP]
        pick = jnp.where(hit0, 1.0, jnp.where(hit1, 1.0, 0.0)).astype(BF16)
        pick_ref[mb] = pick
        scratch["pull"][0][mb] = mm(pick, g_ref[mb]).astype(BF16).reshape(G, CAP, D)

    def project(mb):
        if mb == 0:
            ready(0, 2, 4)
        x_ref[mb, TP - 16 : TP] = jnp.zeros((16, D), F32)
        x_ref[mb, 0:SEQ] = xin_ref[:, mb, :].astype(F32)
        hat, _ = normed_of(x_ref[mb])
        n1 = (hat * gain1_ref[...].reshape(1, D)).astype(BF16)
        n1_ref[mb] = n1
        qkv_ref[mb] = mm(n1, wqkv_ref[...]).astype(BF16)

    def forward(mb):
        for pair in range(HEADS // 2):
            c = pair * 128
            q = qkv_ref[mb, :, c : c + 128] * jnp.asarray(HD**-0.5, BF16)
            k = qkv_ref[mb, :, D + c : D + c + 128]
            v = qkv_ref[mb, :, 2 * D + c : 2 * D + c + 128]
            mixed = []
            for half in range(2):
                mine = low_half if half == 0 else jnp.logical_not(low_half)
                qh = jnp.where(mine, q, jnp.zeros_like(q))
                s = mm(qh, k, 1, 1)
                s = jnp.where(key_ok, s, -1e30)
                e = jnp.exp(s - jnp.max(s, axis=-1, keepdims=True))
                p = e / jnp.sum(e, axis=-1, keepdims=True)
                p_ref[mb, 2 * pair + half] = p
                mixed.append(mm(p.astype(BF16), v))
            am_ref[mb, :, c : c + 128] = jnp.where(
                low_half, mixed[0], mixed[1]
            ).astype(BF16)
        if mb == 0:
            ready(5, 3, 6)
        res = x_ref[mb] + mm(am_ref[mb], wattn_ref[...])
        res_ref[mb] = res
        hat2, _ = normed_of(res)
        n2 = (hat2 * gain2_ref[...].reshape(1, D)).astype(BF16)
        n2_ref[mb] = n2
        logits = mm(wrt_ref[...], n2, 1, 1)
        ex = jnp.exp(logits - jnp.max(logits, axis=0, keepdims=True))
        gp = ex / jnp.sum(ex, axis=0, keepdims=True)
        rs_ref[mb, 0:G, 0:TP] = gp
        expert_of = lax.broadcasted_iota(jnp.int32, (G, TP), 0).astype(F32)
        slot_of = lax.broadcasted_iota(jnp.int32, (S, TP), 0).astype(F32)
        gcol = jnp.zeros((S, 1), F32)
        for kk in range(2):
            flr = rs_ref[mb, G + kk : G + kk + 1, 0:TP]
            keep = rs_ref[mb, G + 2 + kk : G + 3 + kk, 0:TP]
            idr = rs_ref[mb, G + 4 + kk : G + 5 + kk, 0:TP]
            mine = jnp.where(expert_of == idr, gp, 0.0)
            gate = jnp.sum(mine, axis=0, keepdims=True) * keep
            rs_ref[mb, G + 6 + kk : G + 7 + kk, 0:TP] = gate
            hit = slot_of == flr
            gcol = gcol + jnp.sum(jnp.where(hit, gate, 0.0), axis=-1, keepdims=True)
        scratch["rows"][0][mb] = mm(pick_ref[mb], n2).astype(BF16).reshape(G, CAP, D)
        scratch["gate"][0][mb] = row_of_slots(gcol)
        cols_ref[mb] = rs_ref[mb].T

    def experts(mb, halfway=None):
        if mb == last:
            arrived("rows", mb)
        xs = scratch["rows"][1][mb].reshape(S, D)
        step = 384
        produced = jnp.zeros((S, D), F32)
        for c in range(0, FF, step):
            h = mm(xs, w1[:, c : c + step])
            sq = h * h
            t = jnp.tanh(0.7978845608028654 * (h + 0.044715 * (h * sq)))
            half = 0.5 * (1.0 + t)
            act = (h * half).astype(BF16)
            slope_ref[:, c : c + step] = half + 0.5 * h * (1.0 - t * t) * (
                0.7978845608028654 * (1.0 + 0.134145 * sq)
            )
            act_ref[mb, :, c : c + step] = act
            produced = produced + mm(act, w2[c : c + step, :])
        produced = produced.astype(BF16)
        scratch["made"][0][mb] = produced.reshape(G, CAP, D)
        if halfway is not None:
            halfway()
        gates = slots_of_row(arrived("gate", mb)[...])
        grow = arrived("pull", mb)[...].reshape(S, D).astype(F32)
        pg = (gates * grow).astype(BF16)
        scratch["gated"][mb] = pg
        gg = jnp.sum(grow * produced.astype(F32), axis=-1, keepdims=True)
        scratch["ggrad"][0][mb] = row_of_slots(gg)
        back = jnp.zeros((S, D), F32)
        for c in range(0, FF, step):
            ag = mm(pg, w2[c : c + step, :], 1, 1)
            hg = (ag * slope_ref[:, c : c + step]).astype(BF16)
            hg_ref[mb, :, c : c + step] = hg
            back = back + mm(hg, w1[:, c : c + step], 1, 1)
        scratch["back"][0][mb] = back.astype(BF16).reshape(G, CAP, D)

    span = FF // L

    def weight_grads(mb, mats):
        xs = scratch["rows"][1][mb].reshape(S, D)
        pg = scratch["gated"][mb]

        def part(i, carry):
            at = pl.ds(pl.multiple_of(i * span, 128), span)
            for mat in mats:
                left_rows = (hg_ref, act_ref)[mat][mb, :, at]
                grad = mm(left_rows, (xs, pg)[mat], 0, 0)
                if mb > 0:
                    grad = grad + gacc_ref[mat, i]
                if mb < last:
                    gacc_ref[mat, i] = grad
                else:
                    grad = grad.astype(BF16)
                    for rr in range(R):
                        xg_ref[mat, rr, i] = grad[rr * FS : (rr + 1) * FS]
            return carry

        lax.fori_loop(0, L, part, 0)

    def swap_slices(mat):
        for o in range(1, R):
            rr = (r + o) % R
            remote(
                xg_ref.at[mat, rr],
                x1_ref.at[mat, R - o - 1],
                x1sem.at[mat, 0],
                x1sem.at[mat, 1],
                part_id(rr),
            )

    def add_slices(mat):
        if R > 1:
            wait_bytes(x1_ref.at[mat], x1sem.at[mat, 1])

        def part(i, carry):
            total = xg_ref[mat, r, i].astype(F32)
            for o in range(R - 1):
                total = total + x1_ref[mat, o, i].astype(F32)
            xs_ref[i, mat] = total.astype(BF16)
            return carry

        lax.fori_loop(0, L, part, 0)

    pieces = max(1, FS // 48)

    def hand_out(which):
        mat, piece = which
        rows = pl.ds(piece * (FS // pieces), FS // pieces)
        for o in range(1, L):
            i = (j + o) % L
            remote(
                xs_ref.at[i, mat, rows],
                eg_ref.at[j, mat, rows],
                xsem.at[1 + mat, 0],
                xsem.at[1 + mat, 1],
                plane_id(i),
            )
        pltpu.make_async_copy(
            xs_ref.at[j, mat, rows], eg_ref.at[j, mat, rows], xsem.at[1 + mat, 1]
        ).start()

    def slices_out(mat):
        wait_bytes(xs_ref.at[pl.ds(0, L), 0], xsem.at[1 + mat, 1])
        out = (ein_out, eout_out)[mat]

        def part(i, carry):
            out[i] = eg_ref[i, mat].astype(F32)
            return carry

        lax.fori_loop(0, L, part, 0)

    def chunk_of(block):
        for ck in chunks:
            at = 0
            for name in ck["blocks"]:
                if name == block:
                    return ck, at
                at += ROWS[name]

    def add_block(block, value):
        ck, at = chunk_of(block)
        src, pr = ck["src"], ck["pr"]
        at = at // pr
        count = ROWS[block] // pr
        if pr % 8 == 0:
            src[at : at + count] = value.reshape(count, pr, D).astype(BF16)
        else:
            first = START[block]
            acc_ref[first : first + ROWS[block]] = value
            rows = math.lcm(pr, 8)

            @pl.loop(0, ROWS[block] // rows)
            def _(n):
                piece = acc_ref[pl.ds(pl.multiple_of(first + n * rows, 8), rows)]
                piece = piece.astype(BF16)
                for m in range(rows // pr):
                    src[at + n * (rows // pr) + m] = piece[m * pr : (m + 1) * pr]

    def total_of(block):
        ck, at = chunk_of(block)
        out, pr = ck["out"], ck["pr"]
        at = at // pr
        count = ROWS[block] // pr
        if pr % 8 == 0:
            return out[at : at + count].astype(F32).reshape(ROWS[block], D)
        first = START[block]
        rows = math.lcm(pr, 8)

        @pl.loop(0, ROWS[block] // rows)
        def _(n):
            pieces = [out[at + n * (rows // pr) + m] for m in range(rows // pr)]
            spot = pl.ds(pl.multiple_of(first + n * rows, 8), rows)
            acc_ref[spot] = jnp.concatenate(
                [piece.astype(F32) for piece in pieces], axis=0
            )

        return acc_ref[first : first + ROWS[block]]

    def store_totals(ck):
        if R > 1:
            wait_bytes(ck["l1"], ck["recv"].at[5])
        for block in ck["blocks"]:
            total = total_of(block)
            if block < 2:
                wattn_out[START[block] : START[block] + ROWS[block]] = total
            elif block < 4:
                first = START[block] - D
                wqkv_out[first : first + ROWS[block], 2 * D : 3 * D] = total
            else:
                for n in range(2):
                    c = n * D + (block - 4) * 128
                    for m in range(3):
                        wqkv_out[m * 128 : (m + 1) * 128, c : c + 128] = total[
                            n * 128 : (n + 1) * 128, m * 128 : (m + 1) * 128
                        ]

    def sum_start(ck):
        (_, A, _), (_, B, _) = ck["dims"]
        for o in range(1, R):
            rr = (r + o) % R
            remote(
                ck["src"].at[pl.ds(rr * A * B, A * B)],
                ck["l1"].at[R - o - 1],
                ssem.at[0],
                ck["recv"].at[0],
                part_id(rr),
            )

    def sum_pairs(ck):
        (a, A, ident), (_, B, _) = ck["dims"]
        if R > 1:
            wait_bytes(ck["l1"], ck["recv"].at[0])
        for n in range(1, A + 1):
            i = (a + n) % A
            total = ck["src"][pl.ds((r * A + i) * B, B)].astype(F32)
            for o in range(R - 1):
                total = total + ck["l1"][o, pl.ds(i * B, B)].astype(F32)
            ck["l2s"][i] = total.astype(BF16)
            if n < A:
                remote(
                    ck["l2s"].at[i],
                    ck["l2"].at[A - n - 1],
                    ssem.at[0],
                    ck["recv"].at[1],
                    ident(i),
                )

    def sum_first(ck):
        (a, A, _), (b, B, ident) = ck["dims"]
        if A > 1:
            wait_bytes(ck["l2"], ck["recv"].at[1])
        for n in range(B - 1, -1, -1):
            i = (b + n) % B
            total = ck["l2s"][a, i].astype(F32)
            for o in range(A - 1):
                total = total + ck["l2"][o, i].astype(F32)
            ck["l3s"][i] = total.astype(BF16)
            if n > 0:
                remote(
                    ck["l3s"].at[i],
                    ck["l3"].at[B - n - 1],
                    ssem.at[1],
                    ck["recv"].at[2],
                    ident(i),
                )

    def sum_second(ck):
        (a, A, _), (b, B, ident) = ck["dims"]
        out = ck["out"]
        if B > 1:
            wait_bytes(ck["l3"], ck["recv"].at[2])
        total = ck["l3s"][b].astype(F32)
        for o in range(B - 1):
            total = total + ck["l3"][o].astype(F32)
        mine = (r * A + a) * B + b
        out[mine] = total.astype(BF16)
        for n in range(B - 1, 0, -1):
            remote(
                out.at[mine],
                out.at[mine],
                ssem.at[1],
                ck["recv"].at[3],
                ident((b + n) % B),
            )

    def spread_first(ck):
        (a, A, ident), (_, B, _) = ck["dims"]
        out = ck["out"]
        if B > 1:
            wait_bytes(ck["l3"], ck["recv"].at[3])
        mine = pl.ds((r * A + a) * B, B)
        for n in range(1, A):
            remote(
                out.at[mine],
                out.at[mine],
                ssem.at[1],
                ck["recv"].at[4],
                ident((a + n) % A),
            )

    def spread_parts(ck):
        (_, A, _), (_, B, _) = ck["dims"]
        out = ck["out"]
        if A > 1:
            wait_bytes(ck["l2"], ck["recv"].at[4])
        mine = pl.ds(r * A * B, A * B)
        for o in range(1, R):
            remote(
                out.at[mine],
                out.at[mine],
                ssem.at[2],
                ck["recv"].at[5],
                part_id((r + o) % R),
            )

    def sums_left():
        counts = [0, 0, 0]
        for ck in chunks:
            (_, A, _), (_, B, _) = ck["dims"]
            counts[0] += (R - 1) * A * B + (A - 1) * B
            counts[1] += 2 * (B - 1) + (A - 1) * B
            counts[2] += (R - 1) * A * B
        for n, total in enumerate(counts):
            if total:
                wait_bytes(sums_ref.at[pl.ds(0, total)], ssem.at[n])

    levels = ((t1_ref, r, R, part_id), (t2_ref, j, L, plane_id), (t3_ref, z, Z, None))

    def small_start(level):
        buf, at, count, ident = levels[level]
        for o in range(1, count):
            to = (at + o) % count
            remote(
                buf.at[at],
                buf.at[at],
                tsem.at[level, 0],
                tsem.at[level, 1],
                (dp, to) if ident is None else ident(to),
            )

    def small_sum(level):
        buf, _, count, _ = levels[level]
        if count > 1:
            wait_bytes(buf.at[pl.ds(0, count - 1)], tsem.at[level, 1])
        total = buf[0].astype(F32)
        for n in range(1, count):
            total = total + buf[n].astype(F32)
        return total

    def small_next(level):
        total = small_sum(level)
        buf, at, _, _ = levels[level + 1]
        buf[at] = total.astype(BF16)
        small_start(level + 1)

    def small_end():
        total = small_sum(2)
        router_out[...] = total[0:G]
        gain2_out[...] = total[G]
        gain1_out[...] = total[G + 1]
        for level in range(3):
            buf, _, count, _ = levels[level]
            if count > 1:
                wait_bytes(buf.at[pl.ds(0, count - 1)], tsem.at[level, 0])

    def add_grad(mb, block, value):
        at = slice(START[block], START[block] + ROWS[block])
        if mb > 0:
            value = value + acc_ref[at]
        if mb < last:
            acc_ref[at] = value
        else:
            add_block(block, value)

    def add_small(mb, at, value):
        small_ref[at] += value

    def cols_of(mb):
        cols = cols_ref[mb][0:TP]
        col = lambda n: cols[:, n : n + 1]
        return cols, col

    def backward(mb):
        cols, col = cols_of(mb)
        ggr = arrived("ggrad", mb)[...].reshape(G, 128)
        g = g_ref[mb].astype(F32)
        res = res_ref[mb]
        slot_at = lax.broadcasted_iota(jnp.int32, (TP, S), 1).astype(F32)
        lane_at = lax.broadcasted_iota(jnp.int32, (TP, 128), 1).astype(F32)
        expert_at = lax.broadcasted_iota(jnp.int32, (TP, G), 1).astype(F32)
        gp = cols[:, 0:G]
        gates_grad = jnp.zeros((TP, G), F32)
        pick = jnp.zeros((TP, S), F32)
        for kk in range(2):
            keep = col(G + 2 + kk)
            named = jnp.where(expert_at == col(G + 4 + kk), 1.0, 0.0)
            of_slot = jnp.where(
                lane_at == col(G + 8 + kk), mm_exact(named, ggr), 0.0
            )
            gate_grad = jnp.sum(of_slot, axis=-1, keepdims=True) * keep
            gates_grad = gates_grad + named * gate_grad
            pick = pick + jnp.where(slot_at == col(G + kk), 1.0, 0.0)
        inner = jnp.sum(gp * gates_grad, axis=-1, keepdims=True)
        logit_grad = (gp * (gates_grad - inner)).astype(BF16)
        add_small(mb, slice(0, G), mm(logit_grad, n2_ref[mb], 0, 0))
        bgr = arrived("back", mb)[...].reshape(S, D)
        ngrad = mm(pick.astype(BF16), bgr) + mm(logit_grad, wrt_ref[...])
        hat2, rstd2 = normed_of(res)
        add_small(
            mb, slice(G, G + 1), jnp.sum(ngrad * hat2, axis=0, keepdims=True)
        )
        gain2 = gain2_ref[...].reshape(1, D)
        rgrad = g + norm_pull(hat2, rstd2, gain2, ngrad)
        branch = rgrad.astype(BF16)
        piped = mb == last and len(chunks) > 1
        wgrad = mm(am_ref[mb], branch, 0, 0)
        add_grad(mb, 0, wgrad[0:256])
        add_grad(mb, 1, wgrad[256:D])
        if piped:
            sum_start(chunks[0])
        if mb == last - 1:
            add_slices(0)
            for piece in range(pieces):
                hand_out((0, piece))
        mgrad = mm(branch, wattn_ref[...], 1, 1).astype(BF16)
        for pair in range(HEADS // 2):
            c = pair * 128
            mg = mgrad[:, c : c + 128]
            dvs = [
                mm(p_ref[mb, 2 * pair + half].astype(BF16), mg, 0, 0)
                for half in range(2)
            ]
            dq_ref[mb, :, 2 * D + c : 2 * D + c + 128] = jnp.where(
                low_half, dvs[0], dvs[1]
            ).astype(BF16)
        n1 = n1_ref[mb]
        wgrad = mm(n1, dq_ref[mb, :, 2 * D : 3 * D], 0, 0)
        add_grad(mb, 2, wgrad[0:128])
        add_grad(mb, 3, wgrad[128:D])
        if piped:
            sum_start(chunks[1])
            sum_start(chunks[2])
            sum_pairs(chunks[0])
        for pair in range(HEADS // 2):
            c = pair * 128
            q = qkv_ref[mb, :, c : c + 128]
            k = qkv_ref[mb, :, D + c : D + c + 128]
            v = qkv_ref[mb, :, 2 * D + c : 2 * D + c + 128]
            mg = mgrad[:, c : c + 128]
            dqs, dks = [], []
            for half in range(2):
                mine = low_half if half == 0 else jnp.logical_not(low_half)
                mgh = jnp.where(mine, mg, jnp.zeros_like(mg))
                p = p_ref[mb, 2 * pair + half]
                dp_ = mm(mgh, v, 1, 1)
                delta = jnp.sum(p * dp_, axis=-1, keepdims=True)
                ds = (p * (dp_ - delta) * HD**-0.5).astype(BF16)
                dqs.append(mm(ds, k))
                dks.append(mm(ds, q, 0, 0))
            grads = [
                jnp.where(low_half, parts[0], parts[1]).astype(BF16)
                for parts in (dqs, dks)
            ]
            for n in range(2):
                dq_ref[mb, :, n * D + c : n * D + c + 128] = grads[n]
            wgrad = mm(n1, jnp.concatenate(grads, axis=1), 0, 0)
            packed = jnp.concatenate(
                [
                    jnp.concatenate(
                        [
                            wgrad[m * 128 : (m + 1) * 128, n * 128 : (n + 1) * 128]
                            for m in range(3)
                        ],
                        axis=1,
                    )
                    for n in range(2)
                ],
                axis=0,
            )
            add_grad(mb, 4 + pair, packed)
            if piped:
                sum_start(chunks[3 + pair])
                sum_pairs(chunks[1 + pair])
        if mb == last and not piped:
            sum_start(chunks[0])
        held_rgrad[mb] = rgrad

    def finish(mb):
        fgrad = mm(dq_ref[mb], wqkv_ref[...], 1, 1)
        hat, rstd = normed_of(x_ref[mb])
        add_small(
            mb, slice(G + 1, G + 2), jnp.sum(fgrad * hat, axis=0, keepdims=True)
        )
        gain1 = gain1_ref[...].reshape(1, D)
        grad = held_rgrad[mb] + norm_pull(hat, rstd, gain1, fgrad)
        ig_ref[:, mb, :] = grad[0:SEQ]

    def combine(mb):
        _, col = cols_of(mb)
        made = arrived("made", mb)[...].reshape(S, D)
        slot_at = lax.broadcasted_iota(jnp.int32, (TP, S), 1).astype(F32)
        out = res_ref[mb]
        for kk in range(2):
            pick = jnp.where(slot_at == col(G + kk), 1.0, 0.0).astype(BF16)
            out = out + col(G + 6 + kk) * mm(pick, made)
        bo_ref[:, mb, :] = out[0:SEQ]

    project(0)
    route(0)
    pl.semaphore_wait(barrier, G - 1 + R - 1)
    exchange(("pull", 0))
    forward(0)
    exchange(("rows", 0), ("gate", 0))
    for mb in range(1, MB):
        project(mb)
        route(mb)
        forward(mb)
        for_core(0, lambda: exchange(("rows", mb), ("gate", mb)))
        arrived("rows", mb - 1)
        for_core(1, lambda: exchange(("rows", mb), ("gate", mb)))
        for_core(0, lambda: exchange(("pull", mb)))
    ready(10, 11)
    experts(0)
    for_core(1, lambda: exchange(("pull", last)))
    exchange(("ggrad", 0))
    weight_grads(0, (0, 1))
    for_core(0, lambda: exchange(("back", 0)))
    for mb in range(1, MB):
        experts(mb, lambda: for_core(1, lambda: exchange(("back", mb - 1))))
        exchange(("ggrad", mb))
        exchange(("back", mb))
        weight_grads(mb, (0,))
    swap_slices(0)
    exchange(*(("made", mb) for mb in range(last)))
    small_ref[...] = jnp.zeros_like(small_ref)
    for mb in range(MB):
        backward(mb)

    def late_slices():
        weight_grads(last, (1,))
        swap_slices(1)

    def small_begin():
        t1_ref[r] = small_ref[...].astype(BF16)
        small_start(0)

    plan = []
    count = len(chunks)
    early = sum(ck["z_first"] for ck in chunks)
    for n, ck in enumerate(chunks):
        if n >= count - 2 or count == 1:
            plan.append((0.1 * (n - count), sum_pairs, ck))
        if ck["z_first"]:
            times = [t + s * n for t, s in Z_TIMES]
        else:
            times = [t + s * (n - early) for t, s in XY_TIMES]
        steps = (sum_first, sum_second, spread_first, spread_parts)
        plan.extend((when, step, ck) for when, step in zip(times, steps))
        plan.append((times[3] + 1.2, store_totals, ck))
    for piece in range(pieces):
        plan.append((X_TIMES[piece % 4], hand_out, (1, piece)))
    plan.append((-0.15, finish, last))
    plan.append((0.2, lambda _: late_slices(), 0))
    for mb in range(last):
        plan.append((0.5, finish, mb))
    plan.append((0.6, lambda _: small_begin(), 0))
    plan.append((0.5, lambda _: exchange(("made", last)), 0))
    plan.append((4.9, add_slices, 1))
    plan.append((3.0, combine, 0))
    plan.append((2.7, small_next, 0))
    for mb in range(1, MB):
        plan.append((10.0, combine, mb))
    plan.append((6.0, small_next, 1))
    plan.append((9.2, slices_out, 0))
    plan.append((17.0, slices_out, 1))
    plan.append((17.1, lambda _: small_end(), 0))
    for when, what, which in sorted(plan, key=lambda step: step[0]):
        what(which)
    sums_left()

    for mat in range(2):
        if L > 1:
            wait_bytes(xs_ref.at[pl.ds(0, L - 1), 0], xsem.at[1 + mat, 0])
        if R > 1:
            wait_bytes(x1_ref.at[mat], x1sem.at[mat, 0])
    for mb in range(MB):
        left(("rows", mb), ("gate", mb), ("ggrad", mb), ("made", mb))
        left(("back", mb))
    left(*(("pull", mb) for mb in range(MB)))


def on_device(
    groups,
    replicas,
    inputs,
    first_gain,
    w_qkv,
    w_attn,
    second_gain,
    w_router,
    expert_in,
    expert_out,
    expert_ids,
    slot_ids,
    dropped,
    out_grad,
):
    L, _, FF = expert_in.shape
    Z = groups
    R = replicas // L
    G = L * Z
    S = G * CAP
    FS = FF // replicas
    parts = R * L * Z
    groups_of_blocks = CHUNKS
    if any(sum(ROWS[n] for n in blocks) % (8 * parts) for blocks in CHUNKS):
        groups_of_blocks = [tuple(range(len(ROWS)))]
    rows_of = [sum(ROWS[n] for n in blocks) for blocks in groups_of_blocks]
    small_rows = -(-(G + 2) // SM) * SM
    rs_rows = -(-(G + 10) // 8) * 8
    swap = lambda a: jnp.transpose(a, (0, 2, 1))
    stored = lambda a: jnp.transpose(a, (1, 0, 2))
    operands = (
        stored(inputs),
        stored(out_grad),
        first_gain,
        second_gain,
        w_qkv,
        w_attn,
        w_router.T,
        swap(expert_ids),
        swap(slot_ids),
        swap(dropped),
        expert_in,
        expert_out,
    )
    vmem = pl.BlockSpec(memory_space=pltpu.VMEM)
    hbm = pl.BlockSpec(memory_space=pltpu.HBM)
    sds = jax.ShapeDtypeStruct
    V = pltpu.VMEM
    dma = pltpu.SemaphoreType.DMA
    scratch = {
        "loads": [V(a.shape, a.dtype) for a in operands[:10]]
        + [V((D, FF), BF16), V((FF, D), BF16)],
        "saved": [
            V((MB, TP, D), F32),
            V((MB, TP, D), BF16),
            V((MB, TP, D), BF16),
            V((MB, TP, 3 * D), BF16),
            V((MB, HEADS, TP, TP), F32),
            V((MB, TP, D), BF16),
            V((MB, TP, D), F32),
            V((MB, TP, D), BF16),
        ],
        "work": [
            V((MB, rs_rows, TL), F32),
            V((MB, TL, rs_rows), F32),
            V((S, FF), F32),
            V((MB, S, TP), BF16),
        ],
        "expert": [
            V((MB, S, FF), BF16),
            V((MB, S, FF), BF16),
            V((2, R, L, FS, D), BF16),
            V((2, max(R - 1, 1), L, FS, D), BF16),
            V((L, 2, FS, D), BF16),
            V((L, 2, FS, D), BF16),
            V((2, L, FF // L, D), F32),
        ],
        "grads": [
            V((MB, TP, 3 * D), BF16),
            V((MB, TP, D), F32),
            V((4 * D, D), F32),
            V((small_rows, D), F32),
            V((R, small_rows, D), BF16),
            V((L, small_rows, D), BF16),
            V((Z, small_rows, D), BF16),
        ],
        "gated": V((MB, S, D), BF16),
        "sums": V((2 * parts * len(rows_of), rows_of[0] // parts, D), BF16),
        "sems": [dma((12,)), dma((len(KINDS), MB, 2)), dma((3, 2)), dma((3, 2)), dma((3,)), dma((2, 2))],
    }
    for kind in KINDS:
        slim = kind in ("gate", "ggrad")
        shape = (MB, G, 1, 128) if slim else (MB, G, CAP, D)
        scratch[kind] = [V(shape, F32 if slim else BF16)] * 2
    scratch["chunks"] = []
    early = EARLY if len(rows_of) > 1 else 0
    for n, rows in enumerate(rows_of):
        pr = rows // parts
        A, B = (Z, L) if n < early else (L, Z)
        scratch["chunks"].append(
            {
                "out": V((parts, pr, D), BF16),
                "l1": V((max(R - 1, 1), A * B, pr, D), BF16),
                "l2s": V((A, B, pr, D), BF16),
                "l2": V((max(A - 1, 1), B, pr, D), BF16),
                "l3s": V((B, pr, D), BF16),
                "l3": V((max(B - 1, 1), pr, D), BF16),
                "recv": dma((6,)),
            }
        )
    leaves, tree = jax.tree.flatten(scratch)
    results = (
        sds((SEQ, MB, D), F32),
        sds((SEQ, MB, D), F32),
        sds((D,), F32),
        sds((D, 3 * D), F32),
        sds((D, D), F32),
        sds((D,), F32),
        sds((G, D), F32),
        sds((L, FS, D), F32),
        sds((L, FS, D), F32),
    )
    n_in, n_out = len(operands), len(results)

    def body(*refs):
        ins, outs = refs[:n_in], refs[n_in : n_in + n_out]
        held = jax.tree.unflatten(tree, refs[n_in + n_out :])
        for ck, blocks, rows in zip(held["chunks"], groups_of_blocks, rows_of):
            ck["blocks"] = blocks
            ck["pr"] = rows // parts
            ck["z_first"] = len(rows_of) > 1 and blocks in groups_of_blocks[:early]
        kernel((L, R, Z, G, FF), ins, outs, held)

    held = pl.pallas_call(
        body,
        out_shape=results,
        in_specs=[hbm] * n_in,
        out_specs=[vmem] * n_out,
        scratch_shapes=leaves,
        compiler_params=pltpu.CompilerParams(
            collective_id=0, has_side_effects=True, vmem_limit_bytes=53 << 20
        ),
        name="block",
    )(*(pltpu.with_memory_space_constraint(a, pltpu.HBM) for a in operands))

    def put_out(*refs):
        ins, outs, sem = refs[:n_out], refs[n_out:-1], refs[-1]
        copies = [
            pltpu.make_async_copy(src, dst, sem.at[n])
            for n, (src, dst) in enumerate(zip(ins, outs))
        ]
        for copy in copies:
            copy.start()
        for copy in copies:
            copy.wait()

    bo, ig, gain1, wqkv, wattn, gain2, router, ein, eout = pl.pallas_call(
        put_out,
        out_shape=results,
        in_specs=[vmem] * n_out,
        out_specs=[hbm] * n_out,
        scratch_shapes=[dma((n_out,))],
        compiler_params=pltpu.CompilerParams(vmem_limit_bytes=1 << 20),
        name="put_out",
    )(*held)
    return (
        stored(bo),
        stored(ig),
        gain1,
        wqkv,
        wattn,
        gain2,
        router.T,
        jnp.transpose(ein, (0, 2, 1)),
        eout,
    )


def solution(mesh):
    rows = P(None, ("dp", "expert"), None)
    split = P("expert", None, None)
    return jax.shard_map(
        functools.partial(on_device, mesh.shape["expert"], mesh.shape["dp"]),
        mesh=mesh,
        in_specs=(
            rows,
            P(),
            P(),
            P(),
            P(),
            P(),
            split,
            split,
            rows,
            rows,
            rows,
            rows,
        ),
        out_specs=(
            rows,
            rows,
            P(),
            P(),
            P(),
            P(),
            P(),
            P("expert", None, "dp"),
            P("expert", "dp", None),
        ),
        check_vma=False,
    )
```

```python
import functools
import math

import jax
import jax.numpy as jnp
from jax import lax
from jax.experimental import pallas as pl
from jax.experimental.pallas import tpu as pltpu
from jax.sharding import PartitionSpec as P

D = 384
HEADS = 6
HD = 64
SEQ = 197
MB = 2
CAP = 16
EPS = 1e-06
TP = 208
TL = 256
SM = 32
ROWS = (256, 128, 128, 256, 256, 256, 256)
START = (0, 256, 384, 512, 768, 1024, 1280)
CHUNKS = ((0,), (1, 2), (3,), (4,), (5,), (6,))
F32 = jnp.float32
BF16 = jnp.bfloat16
MESH = pl.DeviceIdType.MESH
EARLY = 2
Z_TIMES = ((3.5, 1.5), (7.5, 1.5), (11.0, 1.5), (15.5, 1.2))
XY_TIMES = ((3.0, 0.9), (8.0, 0.9), (12.0, 0.8), (15.5, 0.8))
X_TIMES = (7.1, 8.2, 9.1, 10.0)
KINDS = ("rows", "gate", "pull", "ggrad", "back", "made")


def mm(a, b, ca=1, cb=0):
    return lax.dot_general(
        a, b, (((ca,), (cb,)), ((), ())), preferred_element_type=F32
    )


def mm_exact(a, b):
    return lax.dot_general(
        a,
        b,
        (((1,), (0,)), ((), ())),
        preferred_element_type=F32,
        precision=lax.Precision.HIGHEST,
    )


def normed_of(rows):
    mean = jnp.sum(rows, axis=-1, keepdims=True) * (1.0 / D)
    centered = rows - mean
    var = jnp.sum(centered * centered, axis=-1, keepdims=True) * (1.0 / D)
    rstd = lax.rsqrt(var + EPS)
    return centered * rstd, rstd


def norm_pull(hat, rstd, gain, grad):
    scaled = grad * gain
    m1 = jnp.sum(scaled, axis=-1, keepdims=True) * (1.0 / D)
    m2 = jnp.sum(scaled * hat, axis=-1, keepdims=True) * (1.0 / D)
    return rstd * (scaled - m1 - hat * m2)


def kernel(dims, ins, outs, scratch):
    L, R, Z, G, FF = dims
    S = G * CAP
    FS = FF // (L * R)
    (
        x_hbm,
        g_hbm,
        gain1_hbm,
        gain2_hbm,
        wqkv_hbm,
        wattn_hbm,
        wrt_hbm,
        ids_hbm,
        slot_hbm,
        drop_hbm,
        win_hbm,
        wout_hbm,
    ) = ins
    bo_ref, ig_ref, gain1_out, wqkv_out, wattn_out, gain2_out, router_out = outs[:7]
    ein_out, eout_out = outs[7:]
    xin_ref, gin_ref, gain1_ref, gain2_ref = scratch["loads"][:4]
    wqkv_ref, wattn_ref, wrt_ref = scratch["loads"][4:7]
    ids_ref, slot_ref, drop_ref, w1, w2 = scratch["loads"][7:]
    x_ref, g_ref, n1_ref, qkv_ref, p_ref, am_ref, res_ref, n2_ref = scratch["saved"]
    rs_ref, cols_ref, slope_ref, pick_ref = scratch["work"]
    act_ref, hg_ref, xg_ref, x1_ref, xs_ref, eg_ref, gacc_ref = scratch["expert"]
    dq_ref, held_rgrad, acc_ref, small_ref, t1_ref, t2_ref, t3_ref = scratch["grads"]
    lsem, esem, xsem, tsem, ssem, x1sem = scratch["sems"]
    sums_ref = scratch["sums"]
    chunks = scratch["chunks"]
    last = MB - 1
    dp = lax.axis_index("dp")
    z = lax.axis_index("expert")
    j = dp // R
    r = dp % R
    me = z * L + j

    def group_id(e):
        return ((e % L) * R + r, e // L)

    def plane_id(i):
        return (i * R + r, z)

    def part_id(rr):
        return (j * R + rr, z)

    def remote(src, dst, send_sem, recv_sem, device):
        pltpu.make_async_remote_copy(
            src_ref=src,
            dst_ref=dst,
            send_sem=send_sem,
            recv_sem=recv_sem,
            device_id=device,
            device_id_type=MESH,
        ).start()

    def wait_bytes(ref, sem):
        pltpu.make_async_copy(ref, ref, sem).wait()

    for n, ck in enumerate(chunks):
        ck["src"] = sums_ref.at[pl.ds(n * G * R, G * R)]
        plane = (j, L, plane_id)
        along = (z, Z, lambda i: (dp, i))
        ck["dims"] = (along, plane) if ck["z_first"] else (plane, along)

    barrier = pltpu.get_barrier_semaphore()

    @pl.loop(1, G)
    def _(o):
        pl.semaphore_signal(
            barrier, inc=1, device_id=group_id((me + o) % G), device_id_type=MESH
        )

    for o in range(1, R):
        pl.semaphore_signal(
            barrier, inc=1, device_id=part_id((r + o) % R), device_id_type=MESH
        )

    loads = []
    sources = [
        x_hbm,
        g_hbm,
        gain1_hbm,
        gain2_hbm,
        wqkv_hbm,
        wattn_hbm,
        wrt_hbm,
        ids_hbm,
        slot_hbm,
        drop_hbm,
        win_hbm.at[j],
        wout_hbm.at[j],
    ]
    for n, (src, dst) in enumerate(zip(sources, scratch["loads"])):
        loads.append(pltpu.make_async_copy(src, dst, lsem.at[n]))
    for n in (0, 2, 4, 7, 8, 9, 1, 5, 3, 6, 10, 11):
        loads[n].start()

    def ready(*which):
        for n in which:
            loads[n].wait()

    low_half = lax.broadcasted_iota(jnp.int32, (TP, 128), 1) < HD
    key_ok = lax.broadcasted_iota(jnp.int32, (TP, TP), 1) < SEQ
    slot_lane = lax.broadcasted_iota(
        jnp.int32, (G, CAP, 128), 2
    ) == lax.broadcasted_iota(jnp.int32, (G, CAP, 128), 1)

    def exchange(*which):
        legs = []
        for kind, mb in which:
            send, recv = scratch[kind]
            sems = esem.at[KINDS.index(kind), mb]
            legs.append((send.at[mb], recv.at[mb], sems))
        for send, recv, sems in legs:
            pltpu.make_async_copy(send.at[me], recv.at[me], sems.at[1]).start()

        @pl.loop(1, G)
        def _(o):
            e = (me + o) % G
            to = group_id(e)
            for send, recv, sems in legs:
                remote(send.at[e], recv.at[me], sems.at[0], sems.at[1], to)

    def for_core(core, what):
        pl.when(dp % 2 == core)(what)

    def left(*which):
        for kind, mb in which:
            sent = scratch[kind][0].at[mb, pl.ds(0, G - 1)]
            wait_bytes(sent, esem.at[KINDS.index(kind), mb, 0])

    def arrived(kind, mb):
        recv = scratch[kind][1].at[mb]
        wait_bytes(recv, esem.at[KINDS.index(kind), mb, 1])
        return recv

    def row_of_slots(col):
        spread = jnp.where(slot_lane, col.reshape(G, CAP, 1), 0.0)
        return jnp.sum(spread, axis=1, keepdims=True)

    def slots_of_row(row):
        spread = jnp.where(slot_lane, row, 0.0)
        return jnp.sum(spread, axis=-1, keepdims=True).reshape(S, 1)

    def route(mb):
        if mb == 0:
            ready(7, 8, 9, 1)
        g_ref[mb, TP - 16 : TP] = jnp.zeros((16, D), BF16)
        g_ref[mb, 0:SEQ] = gin_ref[:, mb, :]
        ids = ids_ref[mb]
        drop = drop_ref[mb]
        slot = slot_ref[mb]
        flat = jnp.where(drop == 0, ids * CAP + slot, S)
        rs_ref[mb] = jnp.zeros_like(rs_ref[mb])
        rs_ref[mb, G : G + 2, 0:TP] = jnp.full((2, TP), S, F32)
        rs_ref[mb, G : G + 2, 0:SEQ] = flat.astype(F32)
        rs_ref[mb, G + 2 : G + 4, 0:SEQ] = 1.0 - drop.astype(F32)
        rs_ref[mb, G + 4 : G + 6, 0:SEQ] = ids.astype(F32)
        rs_ref[mb, G + 8 : G + 10, 0:SEQ] = slot.astype(F32)
        slot_of = lax.broadcasted_iota(jnp.int32, (S, TP), 0).astype(F32)
        hit0 = slot_of == rs_ref[mb, G : G + 1, 0:TP]
        hit1 = slot_of == rs_ref[mb, G + 1 : G + 2, 0:TP]
        pick = jnp.where(hit0, 1.0, jnp.where(hit1, 1.0, 0.0)).astype(BF16)
        pick_ref[mb] = pick
        scratch["pull"][0][mb] = mm(pick, g_ref[mb]).astype(BF16).reshape(G, CAP, D)

    def project(mb):
        if mb == 0:
            ready(0, 2, 4)
        x_ref[mb, TP - 16 : TP] = jnp.zeros((16, D), F32)
        x_ref[mb, 0:SEQ] = xin_ref[:, mb, :].astype(F32)
        hat, _ = normed_of(x_ref[mb])
        n1 = (hat * gain1_ref[...].reshape(1, D)).astype(BF16)
        n1_ref[mb] = n1
        qkv_ref[mb] = mm(n1, wqkv_ref[...]).astype(BF16)

    def forward(mb):
        for pair in range(HEADS // 2):
            c = pair * 128
            q = qkv_ref[mb, :, c : c + 128] * jnp.asarray(HD**-0.5, BF16)
            k = qkv_ref[mb, :, D + c : D + c + 128]
            v = qkv_ref[mb, :, 2 * D + c : 2 * D + c + 128]
            mixed = []
            for half in range(2):
                mine = low_half if half == 0 else jnp.logical_not(low_half)
                qh = jnp.where(mine, q, jnp.zeros_like(q))
                s = mm(qh, k, 1, 1)
                s = jnp.where(key_ok, s, -1e30)
                e = jnp.exp(s - jnp.max(s, axis=-1, keepdims=True))
                p = e / jnp.sum(e, axis=-1, keepdims=True)
                p_ref[mb, 2 * pair + half] = p
                mixed.append(mm(p.astype(BF16), v))
            am_ref[mb, :, c : c + 128] = jnp.where(
                low_half, mixed[0], mixed[1]
            ).astype(BF16)
        if mb == 0:
            ready(5, 3, 6)
        res = x_ref[mb] + mm(am_ref[mb], wattn_ref[...])
        res_ref[mb] = res
        hat2, _ = normed_of(res)
        n2 = (hat2 * gain2_ref[...].reshape(1, D)).astype(BF16)
        n2_ref[mb] = n2
        logits = mm(wrt_ref[...], n2, 1, 1)
        ex = jnp.exp(logits - jnp.max(logits, axis=0, keepdims=True))
        gp = ex / jnp.sum(ex, axis=0, keepdims=True)
        rs_ref[mb, 0:G, 0:TP] = gp
        expert_of = lax.broadcasted_iota(jnp.int32, (G, TP), 0).astype(F32)
        slot_of = lax.broadcasted_iota(jnp.int32, (S, TP), 0).astype(F32)
        gcol = jnp.zeros((S, 1), F32)
        for kk in range(2):
            flr = rs_ref[mb, G + kk : G + kk + 1, 0:TP]
            keep = rs_ref[mb, G + 2 + kk : G + 3 + kk, 0:TP]
            idr = rs_ref[mb, G + 4 + kk : G + 5 + kk, 0:TP]
            mine = jnp.where(expert_of == idr, gp, 0.0)
            gate = jnp.sum(mine, axis=0, keepdims=True) * keep
            rs_ref[mb, G + 6 + kk : G + 7 + kk, 0:TP] = gate
            hit = slot_of == flr
            gcol = gcol + jnp.sum(jnp.where(hit, gate, 0.0), axis=-1, keepdims=True)
        scratch["rows"][0][mb] = mm(pick_ref[mb], n2).astype(BF16).reshape(G, CAP, D)
        scratch["gate"][0][mb] = row_of_slots(gcol)
        cols_ref[mb] = rs_ref[mb].T

    def experts(mb, halfway=None):
        if mb == last:
            arrived("rows", mb)
        xs = scratch["rows"][1][mb].reshape(S, D)
        step = 384
        produced = jnp.zeros((S, D), F32)
        for c in range(0, FF, step):
            h = mm(xs, w1[:, c : c + step])
            sq = h * h
            t = jnp.tanh(0.7978845608028654 * (h + 0.044715 * (h * sq)))
            half = 0.5 * (1.0 + t)
            act = (h * half).astype(BF16)
            slope_ref[:, c : c + step] = half + 0.5 * h * (1.0 - t * t) * (
                0.7978845608028654 * (1.0 + 0.134145 * sq)
            )
            act_ref[mb, :, c : c + step] = act
            produced = produced + mm(act, w2[c : c + step, :])
        produced = produced.astype(BF16)
        scratch["made"][0][mb] = produced.reshape(G, CAP, D)
        if halfway is not None:
            halfway()
        gates = slots_of_row(arrived("gate", mb)[...])
        grow = arrived("pull", mb)[...].reshape(S, D).astype(F32)
        pg = (gates * grow).astype(BF16)
        scratch["gated"][mb] = pg
        gg = jnp.sum(grow * produced.astype(F32), axis=-1, keepdims=True)
        scratch["ggrad"][0][mb] = row_of_slots(gg)
        back = jnp.zeros((S, D), F32)
        for c in range(0, FF, step):
            ag = mm(pg, w2[c : c + step, :], 1, 1)
            hg = (ag * slope_ref[:, c : c + step]).astype(BF16)
            hg_ref[mb, :, c : c + step] = hg
            back = back + mm(hg, w1[:, c : c + step], 1, 1)
        scratch["back"][0][mb] = back.astype(BF16).reshape(G, CAP, D)

    span = FF // L

    def weight_grads(mb, mats):
        xs = scratch["rows"][1][mb].reshape(S, D)
        pg = scratch["gated"][mb]

        def part(i, carry):
            at = pl.ds(pl.multiple_of(i * span, 128), span)
            for mat in mats:
                left_rows = (hg_ref, act_ref)[mat][mb, :, at]
                grad = mm(left_rows, (xs, pg)[mat], 0, 0)
                if mb > 0:
                    grad = grad + gacc_ref[mat, i]
                if mb < last:
                    gacc_ref[mat, i] = grad
                else:
                    grad = grad.astype(BF16)
                    for rr in range(R):
                        xg_ref[mat, rr, i] = grad[rr * FS : (rr + 1) * FS]
            return carry

        lax.fori_loop(0, L, part, 0)

    def swap_slices(mat):
        for o in range(1, R):
            rr = (r + o) % R
            remote(
                xg_ref.at[mat, rr],
                x1_ref.at[mat, R - o - 1],
                x1sem.at[mat, 0],
                x1sem.at[mat, 1],
                part_id(rr),
            )

    def add_slices(mat):
        if R > 1:
            wait_bytes(x1_ref.at[mat], x1sem.at[mat, 1])

        def part(i, carry):
            total = xg_ref[mat, r, i].astype(F32)
            for o in range(R - 1):
                total = total + x1_ref[mat, o, i].astype(F32)
            xs_ref[i, mat] = total.astype(BF16)
            return carry

        lax.fori_loop(0, L, part, 0)

    pieces = max(1, FS // 48)

    def hand_out(which):
        mat, piece = which
        rows = pl.ds(piece * (FS // pieces), FS // pieces)
        for o in range(1, L):
            i = (j + o) % L
            remote(
                xs_ref.at[i, mat, rows],
                eg_ref.at[j, mat, rows],
                xsem.at[1 + mat, 0],
                xsem.at[1 + mat, 1],
                plane_id(i),
            )
        pltpu.make_async_copy(
            xs_ref.at[j, mat, rows], eg_ref.at[j, mat, rows], xsem.at[1 + mat, 1]
        ).start()

    def slices_out(mat):
        wait_bytes(xs_ref.at[pl.ds(0, L), 0], xsem.at[1 + mat, 1])
        out = (ein_out, eout_out)[mat]

        def part(i, carry):
            out[i] = eg_ref[i, mat].astype(F32)
            return carry

        lax.fori_loop(0, L, part, 0)

    def chunk_of(block):
        for ck in chunks:
            at = 0
            for name in ck["blocks"]:
                if name == block:
                    return ck, at
                at += ROWS[name]

    def add_block(block, value):
        ck, at = chunk_of(block)
        src, pr = ck["src"], ck["pr"]
        at = at // pr
        count = ROWS[block] // pr
        if pr % 8 == 0:
            src[at : at + count] = value.reshape(count, pr, D).astype(BF16)
        else:
            first = START[block]
            acc_ref[first : first + ROWS[block]] = value
            rows = math.lcm(pr, 8)

            @pl.loop(0, ROWS[block] // rows)
            def _(n):
                piece = acc_ref[pl.ds(pl.multiple_of(first + n * rows, 8), rows)]
                piece = piece.astype(BF16)
                for m in range(rows // pr):
                    src[at + n * (rows // pr) + m] = piece[m * pr : (m + 1) * pr]

    def total_of(block):
        ck, at = chunk_of(block)
        out, pr = ck["out"], ck["pr"]
        at = at // pr
        count = ROWS[block] // pr
        if pr % 8 == 0:
            return out[at : at + count].astype(F32).reshape(ROWS[block], D)
        first = START[block]
        rows = math.lcm(pr, 8)

        @pl.loop(0, ROWS[block] // rows)
        def _(n):
            pieces = [out[at + n * (rows // pr) + m] for m in range(rows // pr)]
            spot = pl.ds(pl.multiple_of(first + n * rows, 8), rows)
            acc_ref[spot] = jnp.concatenate(
                [piece.astype(F32) for piece in pieces], axis=0
            )

        return acc_ref[first : first + ROWS[block]]

    def store_totals(ck):
        if R > 1:
            wait_bytes(ck["l1"], ck["recv"].at[5])
        for block in ck["blocks"]:
            total = total_of(block)
            if block < 2:
                wattn_out[START[block] : START[block] + ROWS[block]] = total
            elif block < 4:
                first = START[block] - D
                wqkv_out[first : first + ROWS[block], 2 * D : 3 * D] = total
            else:
                for n in range(2):
                    c = n * D + (block - 4) * 128
                    for m in range(3):
                        wqkv_out[m * 128 : (m + 1) * 128, c : c + 128] = total[
                            n * 128 : (n + 1) * 128, m * 128 : (m + 1) * 128
                        ]

    def sum_start(ck):
        (_, A, _), (_, B, _) = ck["dims"]
        for o in range(1, R):
            rr = (r + o) % R
            remote(
                ck["src"].at[pl.ds(rr * A * B, A * B)],
                ck["l1"].at[R - o - 1],
                ssem.at[0],
                ck["recv"].at[0],
                part_id(rr),
            )

    def sum_pairs(ck):
        (a, A, ident), (_, B, _) = ck["dims"]
        if R > 1:
            wait_bytes(ck["l1"], ck["recv"].at[0])
        for n in range(1, A + 1):
            i = (a + n) % A
            total = ck["src"][pl.ds((r * A + i) * B, B)].astype(F32)
            for o in range(R - 1):
                total = total + ck["l1"][o, pl.ds(i * B, B)].astype(F32)
            ck["l2s"][i] = total.astype(BF16)
            if n < A:
                remote(
                    ck["l2s"].at[i],
                    ck["l2"].at[A - n - 1],
                    ssem.at[0],
                    ck["recv"].at[1],
                    ident(i),
                )

    def sum_first(ck):
        (a, A, _), (b, B, ident) = ck["dims"]
        if A > 1:
            wait_bytes(ck["l2"], ck["recv"].at[1])
        for n in range(B - 1, -1, -1):
            i = (b + n) % B
            total = ck["l2s"][a, i].astype(F32)
            for o in range(A - 1):
                total = total + ck["l2"][o, i].astype(F32)
            ck["l3s"][i] = total.astype(BF16)
            if n > 0:
                remote(
                    ck["l3s"].at[i],
                    ck["l3"].at[B - n - 1],
                    ssem.at[1],
                    ck["recv"].at[2],
                    ident(i),
                )

    def sum_second(ck):
        (a, A, _), (b, B, ident) = ck["dims"]
        out = ck["out"]
        if B > 1:
            wait_bytes(ck["l3"], ck["recv"].at[2])
        total = ck["l3s"][b].astype(F32)
        for o in range(B - 1):
            total = total + ck["l3"][o].astype(F32)
        mine = (r * A + a) * B + b
        out[mine] = total.astype(BF16)
        for n in range(B - 1, 0, -1):
            remote(
                out.at[mine],
                out.at[mine],
                ssem.at[1],
                ck["recv"].at[3],
                ident((b + n) % B),
            )

    def spread_first(ck):
        (a, A, ident), (_, B, _) = ck["dims"]
        out = ck["out"]
        if B > 1:
            wait_bytes(ck["l3"], ck["recv"].at[3])
        mine = pl.ds((r * A + a) * B, B)
        for n in range(1, A):
            remote(
                out.at[mine],
                out.at[mine],
                ssem.at[1],
                ck["recv"].at[4],
                ident((a + n) % A),
            )

    def spread_parts(ck):
        (_, A, _), (_, B, _) = ck["dims"]
        out = ck["out"]
        if A > 1:
            wait_bytes(ck["l2"], ck["recv"].at[4])
        mine = pl.ds(r * A * B, A * B)
        for o in range(1, R):
            remote(
                out.at[mine],
                out.at[mine],
                ssem.at[2],
                ck["recv"].at[5],
                part_id((r + o) % R),
            )

    def sums_left():
        counts = [0, 0, 0]
        for ck in chunks:
            (_, A, _), (_, B, _) = ck["dims"]
            counts[0] += (R - 1) * A * B + (A - 1) * B
            counts[1] += 2 * (B - 1) + (A - 1) * B
            counts[2] += (R - 1) * A * B
        for n, total in enumerate(counts):
            if total:
                wait_bytes(sums_ref.at[pl.ds(0, total)], ssem.at[n])

    levels = ((t1_ref, r, R, part_id), (t2_ref, j, L, plane_id), (t3_ref, z, Z, None))

    def small_start(level):
        buf, at, count, ident = levels[level]
        for o in range(1, count):
            to = (at + o) % count
            remote(
                buf.at[at],
                buf.at[at],
                tsem.at[level, 0],
                tsem.at[level, 1],
                (dp, to) if ident is None else ident(to),
            )

    def small_sum(level):
        buf, _, count, _ = levels[level]
        if count > 1:
            wait_bytes(buf.at[pl.ds(0, count - 1)], tsem.at[level, 1])
        total = buf[0].astype(F32)
        for n in range(1, count):
            total = total + buf[n].astype(F32)
        return total

    def small_next(level):
        total = small_sum(level)
        buf, at, _, _ = levels[level + 1]
        buf[at] = total.astype(BF16)
        small_start(level + 1)

    def small_end():
        total = small_sum(2)
        router_out[...] = total[0:G]
        gain2_out[...] = total[G]
        gain1_out[...] = total[G + 1]
        for level in range(3):
            buf, _, count, _ = levels[level]
            if count > 1:
                wait_bytes(buf.at[pl.ds(0, count - 1)], tsem.at[level, 0])

    def add_grad(mb, block, value):
        at = slice(START[block], START[block] + ROWS[block])
        if mb > 0:
            value = value + acc_ref[at]
        if mb < last:
            acc_ref[at] = value
        else:
            add_block(block, value)

    def add_small(mb, at, value):
        small_ref[at] += value

    def cols_of(mb):
        cols = cols_ref[mb][0:TP]
        col = lambda n: cols[:, n : n + 1]
        return cols, col

    def backward(mb):
        cols, col = cols_of(mb)
        ggr = arrived("ggrad", mb)[...].reshape(G, 128)
        g = g_ref[mb].astype(F32)
        res = res_ref[mb]
        slot_at = lax.broadcasted_iota(jnp.int32, (TP, S), 1).astype(F32)
        lane_at = lax.broadcasted_iota(jnp.int32, (TP, 128), 1).astype(F32)
        expert_at = lax.broadcasted_iota(jnp.int32, (TP, G), 1).astype(F32)
        gp = cols[:, 0:G]
        gates_grad = jnp.zeros((TP, G), F32)
        pick = jnp.zeros((TP, S), F32)
        for kk in range(2):
            keep = col(G + 2 + kk)
            named = jnp.where(expert_at == col(G + 4 + kk), 1.0, 0.0)
            of_slot = jnp.where(
                lane_at == col(G + 8 + kk), mm_exact(named, ggr), 0.0
            )
            gate_grad = jnp.sum(of_slot, axis=-1, keepdims=True) * keep
            gates_grad = gates_grad + named * gate_grad
            pick = pick + jnp.where(slot_at == col(G + kk), 1.0, 0.0)
        inner = jnp.sum(gp * gates_grad, axis=-1, keepdims=True)
        logit_grad = (gp * (gates_grad - inner)).astype(BF16)
        add_small(mb, slice(0, G), mm(logit_grad, n2_ref[mb], 0, 0))
        bgr = arrived("back", mb)[...].reshape(S, D)
        ngrad = mm(pick.astype(BF16), bgr) + mm(logit_grad, wrt_ref[...])
        hat2, rstd2 = normed_of(res)
        add_small(
            mb, slice(G, G + 1), jnp.sum(ngrad * hat2, axis=0, keepdims=True)
        )
        gain2 = gain2_ref[...].reshape(1, D)
        rgrad = g + norm_pull(hat2, rstd2, gain2, ngrad)
        branch = rgrad.astype(BF16)
        piped = mb == last and len(chunks) > 1
        wgrad = mm(am_ref[mb], branch, 0, 0)
        add_grad(mb, 0, wgrad[0:256])
        add_grad(mb, 1, wgrad[256:D])
        if piped:
            sum_start(chunks[0])
        if mb == last - 1:
            add_slices(0)
            for piece in range(pieces):
                hand_out((0, piece))
        mgrad = mm(branch, wattn_ref[...], 1, 1).astype(BF16)
        for pair in range(HEADS // 2):
            c = pair * 128
            mg = mgrad[:, c : c + 128]
            dvs = [
                mm(p_ref[mb, 2 * pair + half].astype(BF16), mg, 0, 0)
                for half in range(2)
            ]
            dq_ref[mb, :, 2 * D + c : 2 * D + c + 128] = jnp.where(
                low_half, dvs[0], dvs[1]
            ).astype(BF16)
        n1 = n1_ref[mb]
        wgrad = mm(n1, dq_ref[mb, :, 2 * D : 3 * D], 0, 0)
        add_grad(mb, 2, wgrad[0:128])
        add_grad(mb, 3, wgrad[128:D])
        if piped:
            sum_start(chunks[1])
            sum_start(chunks[2])
            sum_pairs(chunks[0])
        for pair in range(HEADS // 2):
            c = pair * 128
            q = qkv_ref[mb, :, c : c + 128]
            k = qkv_ref[mb, :, D + c : D + c + 128]
            v = qkv_ref[mb, :, 2 * D + c : 2 * D + c + 128]
            mg = mgrad[:, c : c + 128]
            dqs, dks = [], []
            for half in range(2):
                mine = low_half if half == 0 else jnp.logical_not(low_half)
                mgh = jnp.where(mine, mg, jnp.zeros_like(mg))
                p = p_ref[mb, 2 * pair + half]
                dp_ = mm(mgh, v, 1, 1)
                delta = jnp.sum(p * dp_, axis=-1, keepdims=True)
                ds = (p * (dp_ - delta) * HD**-0.5).astype(BF16)
                dqs.append(mm(ds, k))
                dks.append(mm(ds, q, 0, 0))
            grads = [
                jnp.where(low_half, parts[0], parts[1]).astype(BF16)
                for parts in (dqs, dks)
            ]
            for n in range(2):
                dq_ref[mb, :, n * D + c : n * D + c + 128] = grads[n]
            wgrad = mm(n1, jnp.concatenate(grads, axis=1), 0, 0)
            packed = jnp.concatenate(
                [
                    jnp.concatenate(
                        [
                            wgrad[m * 128 : (m + 1) * 128, n * 128 : (n + 1) * 128]
                            for m in range(3)
                        ],
                        axis=1,
                    )
                    for n in range(2)
                ],
                axis=0,
            )
            add_grad(mb, 4 + pair, packed)
            if piped:
                sum_start(chunks[3 + pair])
                sum_pairs(chunks[1 + pair])
        if mb == last and not piped:
            sum_start(chunks[0])
        held_rgrad[mb] = rgrad

    def finish(mb):
        fgrad = mm(dq_ref[mb], wqkv_ref[...], 1, 1)
        hat, rstd = normed_of(x_ref[mb])
        add_small(
            mb, slice(G + 1, G + 2), jnp.sum(fgrad * hat, axis=0, keepdims=True)
        )
        gain1 = gain1_ref[...].reshape(1, D)
        grad = held_rgrad[mb] + norm_pull(hat, rstd, gain1, fgrad)
        ig_ref[:, mb, :] = grad[0:SEQ]

    def combine(mb):
        _, col = cols_of(mb)
        made = arrived("made", mb)[...].reshape(S, D)
        slot_at = lax.broadcasted_iota(jnp.int32, (TP, S), 1).astype(F32)
        out = res_ref[mb]
        for kk in range(2):
            pick = jnp.where(slot_at == col(G + kk), 1.0, 0.0).astype(BF16)
            out = out + col(G + 6 + kk) * mm(pick, made)
        bo_ref[:, mb, :] = out[0:SEQ]

    project(0)
    route(0)
    pl.semaphore_wait(barrier, G - 1 + R - 1)
    exchange(("pull", 0))
    forward(0)
    exchange(("rows", 0), ("gate", 0))
    for mb in range(1, MB):
        project(mb)
        route(mb)
        forward(mb)
        for_core(0, lambda: exchange(("rows", mb), ("gate", mb)))
        arrived("rows", mb - 1)
        for_core(1, lambda: exchange(("rows", mb), ("gate", mb)))
        for_core(0, lambda: exchange(("pull", mb)))
    ready(10, 11)
    experts(0)
    for_core(1, lambda: exchange(("pull", last)))
    exchange(("ggrad", 0))
    weight_grads(0, (0, 1))
    for_core(0, lambda: exchange(("back", 0)))
    for mb in range(1, MB):
        experts(mb, lambda: for_core(1, lambda: exchange(("back", mb - 1))))
        exchange(("ggrad", mb))
        exchange(("back", mb))
        weight_grads(mb, (0,))
    swap_slices(0)
    exchange(*(("made", mb) for mb in range(last)))
    small_ref[...] = jnp.zeros_like(small_ref)
    for mb in range(MB):
        backward(mb)

    def late_slices():
        weight_grads(last, (1,))
        swap_slices(1)

    def small_begin():
        t1_ref[r] = small_ref[...].astype(BF16)
        small_start(0)

    plan = []
    count = len(chunks)
    early = sum(ck["z_first"] for ck in chunks)
    for n, ck in enumerate(chunks):
        if n >= count - 2 or count == 1:
            plan.append((0.1 * (n - count), sum_pairs, ck))
        if ck["z_first"]:
            times = [t + s * n for t, s in Z_TIMES]
        else:
            times = [t + s * (n - early) for t, s in XY_TIMES]
        steps = (sum_first, sum_second, spread_first, spread_parts)
        plan.extend((when, step, ck) for when, step in zip(times, steps))
        plan.append((times[3] + 1.2, store_totals, ck))
    for piece in range(pieces):
        plan.append((X_TIMES[piece % 4], hand_out, (1, piece)))
    plan.append((-0.15, finish, last))
    plan.append((0.2, lambda _: late_slices(), 0))
    for mb in range(last):
        plan.append((0.5, finish, mb))
    plan.append((0.6, lambda _: small_begin(), 0))
    plan.append((0.5, lambda _: exchange(("made", last)), 0))
    plan.append((4.9, add_slices, 1))
    plan.append((3.0, combine, 0))
    plan.append((2.7, small_next, 0))
    for mb in range(1, MB):
        plan.append((10.0, combine, mb))
    plan.append((6.0, small_next, 1))
    plan.append((9.2, slices_out, 0))
    plan.append((17.0, slices_out, 1))
    plan.append((17.1, lambda _: small_end(), 0))
    for when, what, which in sorted(plan, key=lambda step: step[0]):
        what(which)
    sums_left()

    for mat in range(2):
        if L > 1:
            wait_bytes(xs_ref.at[pl.ds(0, L - 1), 0], xsem.at[1 + mat, 0])
        if R > 1:
            wait_bytes(x1_ref.at[mat], x1sem.at[mat, 0])
    for mb in range(MB):
        left(("rows", mb), ("gate", mb), ("ggrad", mb), ("made", mb))
        left(("back", mb))
    left(*(("pull", mb) for mb in range(MB)))


def on_device(
    groups,
    replicas,
    inputs,
    first_gain,
    w_qkv,
    w_attn,
    second_gain,
    w_router,
    expert_in,
    expert_out,
    expert_ids,
    slot_ids,
    dropped,
    out_grad,
):
    L, _, FF = expert_in.shape
    Z = groups
    R = replicas // L
    G = L * Z
    S = G * CAP
    FS = FF // replicas
    parts = R * L * Z
    groups_of_blocks = CHUNKS
    if any(sum(ROWS[n] for n in blocks) % (8 * parts) for blocks in CHUNKS):
        groups_of_blocks = [tuple(range(len(ROWS)))]
    rows_of = [sum(ROWS[n] for n in blocks) for blocks in groups_of_blocks]
    small_rows = -(-(G + 2) // SM) * SM
    rs_rows = -(-(G + 10) // 8) * 8
    swap = lambda a: jnp.transpose(a, (0, 2, 1))
    stored = lambda a: jnp.transpose(a, (1, 0, 2))
    operands = (
        stored(inputs),
        stored(out_grad),
        first_gain,
        second_gain,
        w_qkv,
        w_attn,
        w_router.T,
        swap(expert_ids),
        swap(slot_ids),
        swap(dropped),
        expert_in,
        expert_out,
    )
    vmem = pl.BlockSpec(memory_space=pltpu.VMEM)
    hbm = pl.BlockSpec(memory_space=pltpu.HBM)
    sds = jax.ShapeDtypeStruct
    V = pltpu.VMEM
    dma = pltpu.SemaphoreType.DMA
    scratch = {
        "loads": [V(a.shape, a.dtype) for a in operands[:10]]
        + [V((D, FF), BF16), V((FF, D), BF16)],
        "saved": [
            V((MB, TP, D), F32),
            V((MB, TP, D), BF16),
            V((MB, TP, D), BF16),
            V((MB, TP, 3 * D), BF16),
            V((MB, HEADS, TP, TP), F32),
            V((MB, TP, D), BF16),
            V((MB, TP, D), F32),
            V((MB, TP, D), BF16),
        ],
        "work": [
            V((MB, rs_rows, TL), F32),
            V((MB, TL, rs_rows), F32),
            V((S, FF), F32),
            V((MB, S, TP), BF16),
        ],
        "expert": [
            V((MB, S, FF), BF16),
            V((MB, S, FF), BF16),
            V((2, R, L, FS, D), BF16),
            V((2, max(R - 1, 1), L, FS, D), BF16),
            V((L, 2, FS, D), BF16),
            V((L, 2, FS, D), BF16),
            V((2, L, FF // L, D), F32),
        ],
        "grads": [
            V((MB, TP, 3 * D), BF16),
            V((MB, TP, D), F32),
            V((4 * D, D), F32),
            V((small_rows, D), F32),
            V((R, small_rows, D), BF16),
            V((L, small_rows, D), BF16),
            V((Z, small_rows, D), BF16),
        ],
        "gated": V((MB, S, D), BF16),
        "sums": V((parts * len(rows_of), rows_of[0] // parts, D), BF16),
        "sems": [dma((12,)), dma((len(KINDS), MB, 2)), dma((3, 2)), dma((3, 2)), dma((3,)), dma((2, 2))],
    }
    for kind in KINDS:
        slim = kind in ("gate", "ggrad")
        shape = (MB, G, 1, 128) if slim else (MB, G, CAP, D)
        scratch[kind] = [V(shape, F32 if slim else BF16)] * 2
    scratch["chunks"] = []
    early = EARLY if len(rows_of) > 1 else 0
    for n, rows in enumerate(rows_of):
        pr = rows // parts
        A, B = (Z, L) if n < early else (L, Z)
        scratch["chunks"].append(
            {
                "out": V((parts, pr, D), BF16),
                "l1": V((max(R - 1, 1), A * B, pr, D), BF16),
                "l2s": V((A, B, pr, D), BF16),
                "l2": V((max(A - 1, 1), B, pr, D), BF16),
                "l3s": V((B, pr, D), BF16),
                "l3": V((max(B - 1, 1), pr, D), BF16),
                "recv": dma((6,)),
            }
        )
    leaves, tree = jax.tree.flatten(scratch)
    results = (
        sds((SEQ, MB, D), F32),
        sds((SEQ, MB, D), F32),
        sds((D,), F32),
        sds((D, 3 * D), F32),
        sds((D, D), F32),
        sds((D,), F32),
        sds((G, D), F32),
        sds((L, FS, D), F32),
        sds((L, FS, D), F32),
    )
    n_in, n_out = len(operands), len(results)

    def body(*refs):
        ins, outs = refs[:n_in], refs[n_in : n_in + n_out]
        held = jax.tree.unflatten(tree, refs[n_in + n_out :])
        for ck, blocks, rows in zip(held["chunks"], groups_of_blocks, rows_of):
            ck["blocks"] = blocks
            ck["pr"] = rows // parts
            ck["z_first"] = len(rows_of) > 1 and blocks in groups_of_blocks[:early]
        kernel((L, R, Z, G, FF), ins, outs, held)

    held = pl.pallas_call(
        body,
        out_shape=results,
        in_specs=[hbm] * n_in,
        out_specs=[vmem] * n_out,
        scratch_shapes=leaves,
        compiler_params=pltpu.CompilerParams(
            collective_id=0, has_side_effects=True, vmem_limit_bytes=48 << 20
        ),
        name="block",
    )(*(pltpu.with_memory_space_constraint(a, pltpu.HBM) for a in operands))

    def put_out(*refs):
        ins, outs, sem = refs[:n_out], refs[n_out:-1], refs[-1]
        copies = [
            pltpu.make_async_copy(src, dst, sem.at[n])
            for n, (src, dst) in enumerate(zip(ins, outs))
        ]
        for copy in copies:
            copy.start()
        for copy in copies:
            copy.wait()

    bo, ig, gain1, wqkv, wattn, gain2, router, ein, eout = pl.pallas_call(
        put_out,
        out_shape=results,
        in_specs=[vmem] * n_out,
        out_specs=[hbm] * n_out,
        scratch_shapes=[dma((n_out,))],
        compiler_params=pltpu.CompilerParams(vmem_limit_bytes=1 << 20),
        name="put_out",
    )(*held)
    return (
        stored(bo),
        stored(ig),
        gain1,
        wqkv,
        wattn,
        gain2,
        router.T,
        jnp.transpose(ein, (0, 2, 1)),
        eout,
    )


def solution(mesh):
    rows = P(None, ("dp", "expert"), None)
    split = P("expert", None, None)
    return jax.shard_map(
        functools.partial(on_device, mesh.shape["expert"], mesh.shape["dp"]),
        mesh=mesh,
        in_specs=(
            rows,
            P(),
            P(),
            P(),
            P(),
            P(),
            split,
            split,
            rows,
            rows,
            rows,
            rows,
        ),
        out_specs=(
            rows,
            rows,
            P(),
            P(),
            P(),
            P(),
            P(),
            P("expert", None, "dp"),
            P("expert", "dp", None),
        ),
        check_vma=False,
    )
```

```python
import functools
import math

import jax
import jax.numpy as jnp
from jax import lax
from jax.experimental import pallas as pl
from jax.experimental.pallas import tpu as pltpu
from jax.sharding import PartitionSpec as P

D = 384
HEADS = 6
HD = 64
SEQ = 197
MB = 2
CAP = 16
EPS = 1e-06
TP = 208
TL = 256
SM = 8
ROWS = (256, 128, 128, 256, 256, 256, 256)
START = (0, 256, 384, 512, 768, 1024, 1280)
CHUNKS = ((0,), (1, 2), (3,), (4,), (5,), (6,))
F32 = jnp.float32
BF16 = jnp.bfloat16
MESH = pl.DeviceIdType.MESH
EARLY = 2
Z_TIMES = ((3.5, 1.5), (7.5, 1.5), (11.0, 1.5), (15.5, 1.2))
XY_TIMES = ((3.0, 0.9), (8.0, 0.9), (12.0, 0.8), (15.5, 0.8))
X_TIMES = (7.1, 8.2, 9.1, 10.0)
KINDS = ("rows", "gate", "pull", "ggrad", "back", "made")


def mm(a, b, ca=1, cb=0):
    return lax.dot_general(
        a, b, (((ca,), (cb,)), ((), ())), preferred_element_type=F32
    )


def mm_exact(a, b):
    return lax.dot_general(
        a,
        b,
        (((1,), (0,)), ((), ())),
        preferred_element_type=F32,
        precision=lax.Precision.HIGHEST,
    )


def normed_of(rows):
    mean = jnp.sum(rows, axis=-1, keepdims=True) * (1.0 / D)
    centered = rows - mean
    var = jnp.sum(centered * centered, axis=-1, keepdims=True) * (1.0 / D)
    rstd = lax.rsqrt(var + EPS)
    return centered * rstd, rstd


def norm_pull(hat, rstd, gain, grad):
    scaled = grad * gain
    m1 = jnp.sum(scaled, axis=-1, keepdims=True) * (1.0 / D)
    m2 = jnp.sum(scaled * hat, axis=-1, keepdims=True) * (1.0 / D)
    return rstd * (scaled - m1 - hat * m2)


def kernel(dims, ins, outs, scratch):
    L, R, Z, G, FF = dims
    S = G * CAP
    FS = FF // (L * R)
    (
        x_hbm,
        g_hbm,
        gain1_hbm,
        gain2_hbm,
        wqkv_hbm,
        wattn_hbm,
        wrt_hbm,
        ids_hbm,
        slot_hbm,
        drop_hbm,
        win_hbm,
        wout_hbm,
    ) = ins
    bo_ref, ig_ref, gain1_out, wqkv_out, wattn_out, gain2_out, router_out = outs[:7]
    ein_out, eout_out = outs[7:]
    xin_ref, gin_ref, gain1_ref, gain2_ref = scratch["loads"][:4]
    wqkv_ref, wattn_ref, wrt_ref = scratch["loads"][4:7]
    ids_ref, slot_ref, drop_ref, w1, w2 = scratch["loads"][7:]
    x_ref, g_ref, n1_ref, qkv_ref, p_ref, am_ref, res_ref, n2_ref = scratch["saved"]
    rs_ref, cols_ref, slope_ref, pick_ref = scratch["work"]
    act_ref, hg_ref, xg_ref, x1_ref, xs_ref, eg_ref, gacc_ref = scratch["expert"]
    dq_ref, held_rgrad, acc_ref, small_ref, t1_ref, t2_ref, t3_ref = scratch["grads"]
    lsem, esem, xsem, tsem, ssem, x1sem = scratch["sems"]
    sums_ref = scratch["sums"]
    chunks = scratch["chunks"]
    last = MB - 1
    dp = lax.axis_index("dp")
    z = lax.axis_index("expert")
    j = dp // R
    r = dp % R
    me = z * L + j

    def group_id(e):
        return ((e % L) * R + r, e // L)

    def plane_id(i):
        return (i * R + r, z)

    def part_id(rr):
        return (j * R + rr, z)

    def remote(src, dst, send_sem, recv_sem, device):
        pltpu.make_async_remote_copy(
            src_ref=src,
            dst_ref=dst,
            send_sem=send_sem,
            recv_sem=recv_sem,
            device_id=device,
            device_id_type=MESH,
        ).start()

    def wait_bytes(ref, sem):
        pltpu.make_async_copy(ref, ref, sem).wait()

    for n, ck in enumerate(chunks):
        ck["src"] = sums_ref.at[pl.ds(n * G * R, G * R)]
        plane = (j, L, plane_id)
        along = (z, Z, lambda i: (dp, i))
        ck["dims"] = (along, plane) if ck["z_first"] else (plane, along)

    barrier = pltpu.get_barrier_semaphore()

    @pl.loop(1, G)
    def _(o):
        pl.semaphore_signal(
            barrier, inc=1, device_id=group_id((me + o) % G), device_id_type=MESH
        )

    for o in range(1, R):
        pl.semaphore_signal(
            barrier, inc=1, device_id=part_id((r + o) % R), device_id_type=MESH
        )

    loads = []
    sources = [
        x_hbm,
        g_hbm,
        gain1_hbm,
        gain2_hbm,
        wqkv_hbm,
        wattn_hbm,
        wrt_hbm,
        ids_hbm,
        slot_hbm,
        drop_hbm,
        win_hbm.at[j],
        wout_hbm.at[j],
    ]
    for n, (src, dst) in enumerate(zip(sources, scratch["loads"])):
        loads.append(pltpu.make_async_copy(src, dst, lsem.at[n]))
    for n in (0, 2, 4, 7, 8, 9, 1, 5, 3, 6, 10, 11):
        loads[n].start()

    def ready(*which):
        for n in which:
            loads[n].wait()

    low_half = lax.broadcasted_iota(jnp.int32, (TP, 128), 1) < HD
    key_ok = lax.broadcasted_iota(jnp.int32, (TP, TP), 1) < SEQ
    slot_lane = lax.broadcasted_iota(
        jnp.int32, (G, CAP, 128), 2
    ) == lax.broadcasted_iota(jnp.int32, (G, CAP, 128), 1)

    def exchange(*which):
        legs = []
        for kind, mb in which:
            send, recv = scratch[kind]
            sems = esem.at[KINDS.index(kind), mb]
            legs.append((send.at[mb], recv.at[mb], sems))
        for send, recv, sems in legs:
            pltpu.make_async_copy(send.at[me], recv.at[me], sems.at[1]).start()

        @pl.loop(1, G)
        def _(o):
            e = (me + o) % G
            to = group_id(e)
            for send, recv, sems in legs:
                remote(send.at[e], recv.at[me], sems.at[0], sems.at[1], to)

    def for_core(core, what):
        pl.when(dp % 2 == core)(what)

    def left(*which):
        for kind, mb in which:
            sent = scratch[kind][0].at[mb, pl.ds(0, G - 1)]
            wait_bytes(sent, esem.at[KINDS.index(kind), mb, 0])

    def arrived(kind, mb):
        recv = scratch[kind][1].at[mb]
        wait_bytes(recv, esem.at[KINDS.index(kind), mb, 1])
        return recv

    def row_of_slots(col):
        spread = jnp.where(slot_lane, col.reshape(G, CAP, 1), 0.0)
        return jnp.sum(spread, axis=1, keepdims=True)

    def slots_of_row(row):
        spread = jnp.where(slot_lane, row, 0.0)
        return jnp.sum(spread, axis=-1, keepdims=True).reshape(S, 1)

    def route(mb):
        if mb == 0:
            ready(7, 8, 9, 1)
        g_ref[mb, TP - 16 : TP] = jnp.zeros((16, D), BF16)
        g_ref[mb, 0:SEQ] = gin_ref[:, mb, :]
        ids = ids_ref[mb]
        drop = drop_ref[mb]
        slot = slot_ref[mb]
        flat = jnp.where(drop == 0, ids * CAP + slot, S)
        rs_ref[mb] = jnp.zeros_like(rs_ref[mb])
        rs_ref[mb, G : G + 2, 0:TP] = jnp.full((2, TP), S, F32)
        rs_ref[mb, G : G + 2, 0:SEQ] = flat.astype(F32)
        rs_ref[mb, G + 2 : G + 4, 0:SEQ] = 1.0 - drop.astype(F32)
        rs_ref[mb, G + 4 : G + 6, 0:SEQ] = ids.astype(F32)
        rs_ref[mb, G + 8 : G + 10, 0:SEQ] = slot.astype(F32)
        slot_of = lax.broadcasted_iota(jnp.int32, (S, TP), 0).astype(F32)
        hit0 = slot_of == rs_ref[mb, G : G + 1, 0:TP]
        hit1 = slot_of == rs_ref[mb, G + 1 : G + 2, 0:TP]
        pick = jnp.where(hit0, 1.0, jnp.where(hit1, 1.0, 0.0)).astype(BF16)
        pick_ref[mb] = pick
        scratch["pull"][0][mb] = mm(pick, g_ref[mb]).astype(BF16).reshape(G, CAP, D)

    def project(mb):
        if mb == 0:
            ready(0, 2, 4)
        x_ref[mb, TP - 16 : TP] = jnp.zeros((16, D), F32)
        x_ref[mb, 0:SEQ] = xin_ref[:, mb, :].astype(F32)
        hat, _ = normed_of(x_ref[mb])
        n1 = (hat * gain1_ref[...].reshape(1, D)).astype(BF16)
        n1_ref[mb] = n1
        qkv_ref[mb] = mm(n1, wqkv_ref[...]).astype(BF16)

    def forward(mb):
        for pair in range(HEADS // 2):
            c = pair * 128
            q = qkv_ref[mb, :, c : c + 128] * jnp.asarray(HD**-0.5, BF16)
            k = qkv_ref[mb, :, D + c : D + c + 128]
            v = qkv_ref[mb, :, 2 * D + c : 2 * D + c + 128]
            mixed = []
            for half in range(2):
                mine = low_half if half == 0 else jnp.logical_not(low_half)
                qh = jnp.where(mine, q, jnp.zeros_like(q))
                s = mm(qh, k, 1, 1)
                s = jnp.where(key_ok, s, -1e30)
                e = jnp.exp(s - jnp.max(s, axis=-1, keepdims=True))
                p = e / jnp.sum(e, axis=-1, keepdims=True)
                p_ref[mb, 2 * pair + half] = p
                mixed.append(mm(p.astype(BF16), v))
            am_ref[mb, :, c : c + 128] = jnp.where(
                low_half, mixed[0], mixed[1]
            ).astype(BF16)
        if mb == 0:
            ready(5, 3, 6)
        res = x_ref[mb] + mm(am_ref[mb], wattn_ref[...])
        res_ref[mb] = res
        hat2, _ = normed_of(res)
        n2 = (hat2 * gain2_ref[...].reshape(1, D)).astype(BF16)
        n2_ref[mb] = n2
        logits = mm(wrt_ref[...], n2, 1, 1)
        ex = jnp.exp(logits - jnp.max(logits, axis=0, keepdims=True))
        gp = ex / jnp.sum(ex, axis=0, keepdims=True)
        rs_ref[mb, 0:G, 0:TP] = gp
        expert_of = lax.broadcasted_iota(jnp.int32, (G, TP), 0).astype(F32)
        slot_of = lax.broadcasted_iota(jnp.int32, (S, TP), 0).astype(F32)
        gcol = jnp.zeros((S, 1), F32)
        for kk in range(2):
            flr = rs_ref[mb, G + kk : G + kk + 1, 0:TP]
            keep = rs_ref[mb, G + 2 + kk : G + 3 + kk, 0:TP]
            idr = rs_ref[mb, G + 4 + kk : G + 5 + kk, 0:TP]
            mine = jnp.where(expert_of == idr, gp, 0.0)
            gate = jnp.sum(mine, axis=0, keepdims=True) * keep
            rs_ref[mb, G + 6 + kk : G + 7 + kk, 0:TP] = gate
            hit = slot_of == flr
            gcol = gcol + jnp.sum(jnp.where(hit, gate, 0.0), axis=-1, keepdims=True)
        scratch["rows"][0][mb] = mm(pick_ref[mb], n2).astype(BF16).reshape(G, CAP, D)
        scratch["gate"][0][mb] = row_of_slots(gcol)
        cols_ref[mb] = rs_ref[mb].T

    def experts(mb, halfway=None):
        if mb == last:
            arrived("rows", mb)
        xs = scratch["rows"][1][mb].reshape(S, D)
        step = 384
        produced = jnp.zeros((S, D), F32)
        for c in range(0, FF, step):
            h = mm(xs, w1[:, c : c + step])
            sq = h * h
            t = jnp.tanh(0.7978845608028654 * (h + 0.044715 * (h * sq)))
            half = 0.5 * (1.0 + t)
            act = (h * half).astype(BF16)
            slope_ref[:, c : c + step] = half + 0.5 * h * (1.0 - t * t) * (
                0.7978845608028654 * (1.0 + 0.134145 * sq)
            )
            act_ref[mb, :, c : c + step] = act
            produced = produced + mm(act, w2[c : c + step, :])
        produced = produced.astype(BF16)
        scratch["made"][0][mb] = produced.reshape(G, CAP, D)
        if halfway is not None:
            halfway()
        gates = slots_of_row(arrived("gate", mb)[...])
        grow = arrived("pull", mb)[...].reshape(S, D).astype(F32)
        pg = (gates * grow).astype(BF16)
        scratch["gated"][mb] = pg
        gg = jnp.sum(grow * produced.astype(F32), axis=-1, keepdims=True)
        scratch["ggrad"][0][mb] = row_of_slots(gg)
        back = jnp.zeros((S, D), F32)
        for c in range(0, FF, step):
            ag = mm(pg, w2[c : c + step, :], 1, 1)
            hg = (ag * slope_ref[:, c : c + step]).astype(BF16)
            hg_ref[mb, :, c : c + step] = hg
            back = back + mm(hg, w1[:, c : c + step], 1, 1)
        scratch["back"][0][mb] = back.astype(BF16).reshape(G, CAP, D)

    span = FF // L

    def weight_grads(mb, mats):
        xs = scratch["rows"][1][mb].reshape(S, D)
        pg = scratch["gated"][mb]

        def part(i, carry):
            at = pl.ds(pl.multiple_of(i * span, 128), span)
            for mat in mats:
                left_rows = (hg_ref, act_ref)[mat][mb, :, at]
                grad = mm(left_rows, (xs, pg)[mat], 0, 0)
                if mb > 0:
                    grad = grad + gacc_ref[mat, i]
                if mb < last:
                    gacc_ref[mat, i] = grad
                else:
                    grad = grad.astype(BF16)
                    for rr in range(R):
                        xg_ref[mat, rr, i] = grad[rr * FS : (rr + 1) * FS]
            return carry

        lax.fori_loop(0, L, part, 0)

    def swap_slices(mat):
        for o in range(1, R):
            rr = (r + o) % R
            remote(
                xg_ref.at[mat, rr],
                x1_ref.at[mat, R - o - 1],
                x1sem.at[mat, 0],
                x1sem.at[mat, 1],
                part_id(rr),
            )

    def add_slices(mat):
        if R > 1:
            wait_bytes(x1_ref.at[mat], x1sem.at[mat, 1])

        def part(i, carry):
            total = xg_ref[mat, r, i].astype(F32)
            for o in range(R - 1):
                total = total + x1_ref[mat, o, i].astype(F32)
            xs_ref[i, mat] = total.astype(BF16)
            return carry

        lax.fori_loop(0, L, part, 0)

    pieces = max(1, FS // 48)

    def hand_out(which):
        mat, piece = which
        rows = pl.ds(piece * (FS // pieces), FS // pieces)
        for o in range(1, L):
            i = (j + o) % L
            remote(
                xs_ref.at[i, mat, rows],
                eg_ref.at[j, mat, rows],
                xsem.at[1 + mat, 0],
                xsem.at[1 + mat, 1],
                plane_id(i),
            )
        pltpu.make_async_copy(
            xs_ref.at[j, mat, rows], eg_ref.at[j, mat, rows], xsem.at[1 + mat, 1]
        ).start()

    def slices_out(mat):
        wait_bytes(xs_ref.at[pl.ds(0, L), 0], xsem.at[1 + mat, 1])
        out = (ein_out, eout_out)[mat]

        def part(i, carry):
            out[i] = eg_ref[i, mat].astype(F32)
            return carry

        lax.fori_loop(0, L, part, 0)

    def chunk_of(block):
        for ck in chunks:
            at = 0
            for name in ck["blocks"]:
                if name == block:
                    return ck, at
                at += ROWS[name]

    def add_block(block, value):
        ck, at = chunk_of(block)
        src, pr = ck["src"], ck["pr"]
        at = at // pr
        count = ROWS[block] // pr
        if pr % 8 == 0:
            src[at : at + count] = value.reshape(count, pr, D).astype(BF16)
        else:
            first = START[block]
            acc_ref[first : first + ROWS[block]] = value
            rows = math.lcm(pr, 8)

            @pl.loop(0, ROWS[block] // rows)
            def _(n):
                piece = acc_ref[pl.ds(pl.multiple_of(first + n * rows, 8), rows)]
                piece = piece.astype(BF16)
                for m in range(rows // pr):
                    src[at + n * (rows // pr) + m] = piece[m * pr : (m + 1) * pr]

    def total_of(block):
        ck, at = chunk_of(block)
        out, pr = ck["out"], ck["pr"]
        at = at // pr
        count = ROWS[block] // pr
        if pr % 8 == 0:
            return out[at : at + count].astype(F32).reshape(ROWS[block], D)
        first = START[block]
        rows = math.lcm(pr, 8)

        @pl.loop(0, ROWS[block] // rows)
        def _(n):
            pieces = [out[at + n * (rows // pr) + m] for m in range(rows // pr)]
            spot = pl.ds(pl.multiple_of(first + n * rows, 8), rows)
            acc_ref[spot] = jnp.concatenate(
                [piece.astype(F32) for piece in pieces], axis=0
            )

        return acc_ref[first : first + ROWS[block]]

    def store_totals(ck):
        if R > 1:
            wait_bytes(ck["l1"], ck["recv"].at[5])
        for block in ck["blocks"]:
            total = total_of(block)
            if block < 2:
                wattn_out[START[block] : START[block] + ROWS[block]] = total
            elif block < 4:
                first = START[block] - D
                wqkv_out[first : first + ROWS[block], 2 * D : 3 * D] = total
            else:
                for n in range(2):
                    c = n * D + (block - 4) * 128
                    for m in range(3):
                        wqkv_out[m * 128 : (m + 1) * 128, c : c + 128] = total[
                            n * 128 : (n + 1) * 128, m * 128 : (m + 1) * 128
                        ]

    def sum_start(ck):
        (_, A, _), (_, B, _) = ck["dims"]
        for o in range(1, R):
            rr = (r + o) % R
            remote(
                ck["src"].at[pl.ds(rr * A * B, A * B)],
                ck["l1"].at[R - o - 1],
                ssem.at[0],
                ck["recv"].at[0],
                part_id(rr),
            )

    def sum_pairs(ck):
        (a, A, ident), (_, B, _) = ck["dims"]
        if R > 1:
            wait_bytes(ck["l1"], ck["recv"].at[0])
        for n in range(1, A + 1):
            i = (a + n) % A
            total = ck["src"][pl.ds((r * A + i) * B, B)].astype(F32)
            for o in range(R - 1):
                total = total + ck["l1"][o, pl.ds(i * B, B)].astype(F32)
            ck["l2s"][i] = total.astype(BF16)
            if n < A:
                remote(
                    ck["l2s"].at[i],
                    ck["l2"].at[A - n - 1],
                    ssem.at[0],
                    ck["recv"].at[1],
                    ident(i),
                )

    def sum_first(ck):
        (a, A, _), (b, B, ident) = ck["dims"]
        if A > 1:
            wait_bytes(ck["l2"], ck["recv"].at[1])
        for n in range(B - 1, -1, -1):
            i = (b + n) % B
            total = ck["l2s"][a, i].astype(F32)
            for o in range(A - 1):
                total = total + ck["l2"][o, i].astype(F32)
            ck["l3s"][i] = total.astype(BF16)
            if n > 0:
                remote(
                    ck["l3s"].at[i],
                    ck["l3"].at[B - n - 1],
                    ssem.at[1],
                    ck["recv"].at[2],
                    ident(i),
                )

    def sum_second(ck):
        (a, A, _), (b, B, ident) = ck["dims"]
        out = ck["out"]
        if B > 1:
            wait_bytes(ck["l3"], ck["recv"].at[2])
        total = ck["l3s"][b].astype(F32)
        for o in range(B - 1):
            total = total + ck["l3"][o].astype(F32)
        mine = (r * A + a) * B + b
        out[mine] = total.astype(BF16)
        for n in range(B - 1, 0, -1):
            remote(
                out.at[mine],
                out.at[mine],
                ssem.at[1],
                ck["recv"].at[3],
                ident((b + n) % B),
            )

    def spread_first(ck):
        (a, A, ident), (_, B, _) = ck["dims"]
        out = ck["out"]
        if B > 1:
            wait_bytes(ck["l3"], ck["recv"].at[3])
        mine = pl.ds((r * A + a) * B, B)
        for n in range(1, A):
            remote(
                out.at[mine],
                out.at[mine],
                ssem.at[1],
                ck["recv"].at[4],
                ident((a + n) % A),
            )

    def spread_parts(ck):
        (_, A, _), (_, B, _) = ck["dims"]
        out = ck["out"]
        if A > 1:
            wait_bytes(ck["l2"], ck["recv"].at[4])
        mine = pl.ds(r * A * B, A * B)
        for o in range(1, R):
            remote(
                out.at[mine],
                out.at[mine],
                ssem.at[2],
                ck["recv"].at[5],
                part_id((r + o) % R),
            )

    def sums_left():
        counts = [0, 0, 0]
        for ck in chunks:
            (_, A, _), (_, B, _) = ck["dims"]
            counts[0] += (R - 1) * A * B + (A - 1) * B
            counts[1] += 2 * (B - 1) + (A - 1) * B
            counts[2] += (R - 1) * A * B
        for n, total in enumerate(counts):
            if total:
                wait_bytes(sums_ref.at[pl.ds(0, total)], ssem.at[n])

    levels = ((t1_ref, r, R, part_id), (t2_ref, j, L, plane_id), (t3_ref, z, Z, None))

    def small_start(level):
        buf, at, count, ident = levels[level]
        for o in range(1, count):
            to = (at + o) % count
            remote(
                buf.at[at],
                buf.at[at],
                tsem.at[level, 0],
                tsem.at[level, 1],
                (dp, to) if ident is None else ident(to),
            )

    def small_sum(level):
        buf, _, count, _ = levels[level]
        if count > 1:
            wait_bytes(buf.at[pl.ds(0, count - 1)], tsem.at[level, 1])
        total = buf[0].astype(F32)
        for n in range(1, count):
            total = total + buf[n].astype(F32)
        return total

    def small_next(level):
        total = small_sum(level)
        buf, at, _, _ = levels[level + 1]
        buf[at] = total.astype(BF16)
        small_start(level + 1)

    def small_end():
        total = small_sum(2)
        router_out[...] = total[0:G]
        gain2_out[...] = total[G]
        gain1_out[...] = total[G + 1]
        for level in range(3):
            buf, _, count, _ = levels[level]
            if count > 1:
                wait_bytes(buf.at[pl.ds(0, count - 1)], tsem.at[level, 0])

    def add_grad(mb, block, value):
        at = slice(START[block], START[block] + ROWS[block])
        if mb > 0:
            value = value + acc_ref[at]
        if mb < last:
            acc_ref[at] = value
        else:
            add_block(block, value)

    def add_small(mb, at, value):
        small_ref[at] += value

    def cols_of(mb):
        cols = cols_ref[mb][0:TP]
        col = lambda n: cols[:, n : n + 1]
        return cols, col

    def backward(mb):
        cols, col = cols_of(mb)
        ggr = arrived("ggrad", mb)[...].reshape(G, 128)
        g = g_ref[mb].astype(F32)
        res = res_ref[mb]
        slot_at = lax.broadcasted_iota(jnp.int32, (TP, S), 1).astype(F32)
        lane_at = lax.broadcasted_iota(jnp.int32, (TP, 128), 1).astype(F32)
        expert_at = lax.broadcasted_iota(jnp.int32, (TP, G), 1).astype(F32)
        gp = cols[:, 0:G]
        gates_grad = jnp.zeros((TP, G), F32)
        pick = jnp.zeros((TP, S), F32)
        for kk in range(2):
            keep = col(G + 2 + kk)
            named = jnp.where(expert_at == col(G + 4 + kk), 1.0, 0.0)
            of_slot = jnp.where(
                lane_at == col(G + 8 + kk), mm_exact(named, ggr), 0.0
            )
            gate_grad = jnp.sum(of_slot, axis=-1, keepdims=True) * keep
            gates_grad = gates_grad + named * gate_grad
            pick = pick + jnp.where(slot_at == col(G + kk), 1.0, 0.0)
        inner = jnp.sum(gp * gates_grad, axis=-1, keepdims=True)
        logit_grad = (gp * (gates_grad - inner)).astype(BF16)
        add_small(mb, slice(0, G), mm(logit_grad, n2_ref[mb], 0, 0))
        bgr = arrived("back", mb)[...].reshape(S, D)
        ngrad = mm(pick.astype(BF16), bgr) + mm(logit_grad, wrt_ref[...])
        hat2, rstd2 = normed_of(res)
        add_small(
            mb, slice(G, G + 1), jnp.sum(ngrad * hat2, axis=0, keepdims=True)
        )
        gain2 = gain2_ref[...].reshape(1, D)
        rgrad = g + norm_pull(hat2, rstd2, gain2, ngrad)
        branch = rgrad.astype(BF16)
        piped = mb == last and len(chunks) > 1
        wgrad = mm(am_ref[mb], branch, 0, 0)
        add_grad(mb, 0, wgrad[0:256])
        add_grad(mb, 1, wgrad[256:D])
        if piped:
            sum_start(chunks[0])
        if mb == last - 1:
            add_slices(0)
            for piece in range(pieces):
                hand_out((0, piece))
        mgrad = mm(branch, wattn_ref[...], 1, 1).astype(BF16)
        for pair in range(HEADS // 2):
            c = pair * 128
            mg = mgrad[:, c : c + 128]
            dvs = [
                mm(p_ref[mb, 2 * pair + half].astype(BF16), mg, 0, 0)
                for half in range(2)
            ]
            dq_ref[mb, :, 2 * D + c : 2 * D + c + 128] = jnp.where(
                low_half, dvs[0], dvs[1]
            ).astype(BF16)
        n1 = n1_ref[mb]
        wgrad = mm(n1, dq_ref[mb, :, 2 * D : 3 * D], 0, 0)
        add_grad(mb, 2, wgrad[0:128])
        add_grad(mb, 3, wgrad[128:D])
        if piped:
            sum_start(chunks[1])
            sum_start(chunks[2])
            sum_pairs(chunks[0])
        for pair in range(HEADS // 2):
            c = pair * 128
            q = qkv_ref[mb, :, c : c + 128]
            k = qkv_ref[mb, :, D + c : D + c + 128]
            v = qkv_ref[mb, :, 2 * D + c : 2 * D + c + 128]
            mg = mgrad[:, c : c + 128]
            dqs, dks = [], []
            for half in range(2):
                mine = low_half if half == 0 else jnp.logical_not(low_half)
                mgh = jnp.where(mine, mg, jnp.zeros_like(mg))
                p = p_ref[mb, 2 * pair + half]
                dp_ = mm(mgh, v, 1, 1)
                delta = jnp.sum(p * dp_, axis=-1, keepdims=True)
                ds = (p * (dp_ - delta) * HD**-0.5).astype(BF16)
                dqs.append(mm(ds, k))
                dks.append(mm(ds, q, 0, 0))
            grads = [
                jnp.where(low_half, parts[0], parts[1]).astype(BF16)
                for parts in (dqs, dks)
            ]
            for n in range(2):
                dq_ref[mb, :, n * D + c : n * D + c + 128] = grads[n]
            wgrad = mm(n1, jnp.concatenate(grads, axis=1), 0, 0)
            packed = jnp.concatenate(
                [
                    jnp.concatenate(
                        [
                            wgrad[m * 128 : (m + 1) * 128, n * 128 : (n + 1) * 128]
                            for m in range(3)
                        ],
                        axis=1,
                    )
                    for n in range(2)
                ],
                axis=0,
            )
            add_grad(mb, 4 + pair, packed)
            if piped:
                sum_start(chunks[3 + pair])
                sum_pairs(chunks[1 + pair])
        if mb == last and not piped:
            sum_start(chunks[0])
        held_rgrad[mb] = rgrad

    def finish(mb):
        fgrad = mm(dq_ref[mb], wqkv_ref[...], 1, 1)
        hat, rstd = normed_of(x_ref[mb])
        add_small(
            mb, slice(G + 1, G + 2), jnp.sum(fgrad * hat, axis=0, keepdims=True)
        )
        gain1 = gain1_ref[...].reshape(1, D)
        grad = held_rgrad[mb] + norm_pull(hat, rstd, gain1, fgrad)
        ig_ref[:, mb, :] = grad[0:SEQ]

    def combine(mb):
        _, col = cols_of(mb)
        made = arrived("made", mb)[...].reshape(S, D)
        slot_at = lax.broadcasted_iota(jnp.int32, (TP, S), 1).astype(F32)
        out = res_ref[mb]
        for kk in range(2):
            pick = jnp.where(slot_at == col(G + kk), 1.0, 0.0).astype(BF16)
            out = out + col(G + 6 + kk) * mm(pick, made)
        bo_ref[:, mb, :] = out[0:SEQ]

    project(0)
    route(0)
    pl.semaphore_wait(barrier, G - 1 + R - 1)
    exchange(("pull", 0))
    forward(0)
    exchange(("rows", 0), ("gate", 0))
    for mb in range(1, MB):
        project(mb)
        route(mb)
        forward(mb)
        for_core(0, lambda: exchange(("rows", mb), ("gate", mb)))
        arrived("rows", mb - 1)
        for_core(1, lambda: exchange(("rows", mb), ("gate", mb)))
        for_core(0, lambda: exchange(("pull", mb)))
    ready(10, 11)
    experts(0)
    for_core(1, lambda: exchange(("pull", last)))
    exchange(("ggrad", 0))
    weight_grads(0, (0, 1))
    for_core(0, lambda: exchange(("back", 0)))
    for mb in range(1, MB):
        experts(mb, lambda: for_core(1, lambda: exchange(("back", mb - 1))))
        exchange(("ggrad", mb))
        exchange(("back", mb))
        weight_grads(mb, (0, 1))
    swap_slices(0)
    swap_slices(1)
    exchange(*(("made", mb) for mb in range(last)))
    small_ref[...] = jnp.zeros_like(small_ref)
    sent_early = min(0, pieces)
    for mb in range(MB):
        backward(mb)
        if mb == last - 1:
            add_slices(1)
            for piece in range(sent_early):
                hand_out((1, piece))

    def small_begin():
        t1_ref[r] = small_ref[...].astype(BF16)
        small_start(0)

    plan = []
    count = len(chunks)
    early = sum(ck["z_first"] for ck in chunks)
    for n, ck in enumerate(chunks):
        if n >= count - 2 or count == 1:
            plan.append((0.1 * (n - count), sum_pairs, ck))
        if ck["z_first"]:
            times = [t + s * n for t, s in Z_TIMES]
        else:
            times = [t + s * (n - early) for t, s in XY_TIMES]
        steps = (sum_first, sum_second, spread_first, spread_parts)
        plan.extend((when, step, ck) for when, step in zip(times, steps))
        plan.append((times[3] + 1.2, store_totals, ck))
    for piece in range(sent_early, pieces):
        plan.append((X_TIMES[piece % 4], hand_out, (1, piece)))
    plan.append((-0.15, finish, last))
    for mb in range(last):
        plan.append((0.5, finish, mb))
    plan.append((0.6, lambda _: small_begin(), 0))
    plan.append((0.5, lambda _: exchange(("made", last)), 0))
    plan.append((7.0, combine, 0))
    plan.append((5.8, small_next, 0))
    for mb in range(1, MB):
        plan.append((10.0, combine, mb))
    plan.append((10.7, small_next, 1))
    plan.append((9.2, slices_out, 0))
    plan.append((17.0, slices_out, 1))
    plan.append((17.1, lambda _: small_end(), 0))
    for when, what, which in sorted(plan, key=lambda step: step[0]):
        what(which)
    sums_left()

    for mat in range(2):
        if L > 1:
            wait_bytes(xs_ref.at[pl.ds(0, L - 1), 0], xsem.at[1 + mat, 0])
        if R > 1:
            wait_bytes(x1_ref.at[mat], x1sem.at[mat, 0])
    for mb in range(MB):
        left(("rows", mb), ("gate", mb), ("ggrad", mb), ("made", mb))
        left(("back", mb))
    left(*(("pull", mb) for mb in range(MB)))


def on_device(
    groups,
    replicas,
    inputs,
    first_gain,
    w_qkv,
    w_attn,
    second_gain,
    w_router,
    expert_in,
    expert_out,
    expert_ids,
    slot_ids,
    dropped,
    out_grad,
):
    L, _, FF = expert_in.shape
    Z = groups
    R = replicas // L
    G = L * Z
    S = G * CAP
    FS = FF // replicas
    parts = R * L * Z
    groups_of_blocks = CHUNKS
    if any(sum(ROWS[n] for n in blocks) % (8 * parts) for blocks in CHUNKS):
        groups_of_blocks = [tuple(range(len(ROWS)))]
    rows_of = [sum(ROWS[n] for n in blocks) for blocks in groups_of_blocks]
    small_rows = -(-(G + 2) // SM) * SM
    rs_rows = -(-(G + 10) // 8) * 8
    swap = lambda a: jnp.transpose(a, (0, 2, 1))
    stored = lambda a: jnp.transpose(a, (1, 0, 2))
    operands = (
        stored(inputs),
        stored(out_grad),
        first_gain,
        second_gain,
        w_qkv,
        w_attn,
        w_router.T,
        swap(expert_ids),
        swap(slot_ids),
        swap(dropped),
        expert_in,
        expert_out,
    )
    vmem = pl.BlockSpec(memory_space=pltpu.VMEM)
    hbm = pl.BlockSpec(memory_space=pltpu.HBM)
    sds = jax.ShapeDtypeStruct
    V = pltpu.VMEM
    dma = pltpu.SemaphoreType.DMA
    scratch = {
        "loads": [V(a.shape, a.dtype) for a in operands[:10]]
        + [V((D, FF), BF16), V((FF, D), BF16)],
        "saved": [
            V((MB, TP, D), F32),
            V((MB, TP, D), BF16),
            V((MB, TP, D), BF16),
            V((MB, TP, 3 * D), BF16),
            V((MB, HEADS, TP, TP), F32),
            V((MB, TP, D), BF16),
            V((MB, TP, D), F32),
            V((MB, TP, D), BF16),
        ],
        "work": [
            V((MB, rs_rows, TL), F32),
            V((MB, TL, rs_rows), F32),
            V((S, FF), F32),
            V((MB, S, TP), BF16),
        ],
        "expert": [
            V((MB, S, FF), BF16),
            V((MB, S, FF), BF16),
            V((2, R, L, FS, D), BF16),
            V((2, max(R - 1, 1), L, FS, D), BF16),
            V((L, 2, FS, D), BF16),
            V((L, 2, FS, D), BF16),
            V((2, L, FF // L, D), F32),
        ],
        "grads": [
            V((MB, TP, 3 * D), BF16),
            V((MB, TP, D), F32),
            V((4 * D, D), F32),
            V((small_rows, D), F32),
            V((R, small_rows, D), BF16),
            V((L, small_rows, D), BF16),
            V((Z, small_rows, D), BF16),
        ],
        "gated": V((MB, S, D), BF16),
        "sums": V((parts * len(rows_of), rows_of[0] // parts, D), BF16),
        "sems": [dma((12,)), dma((len(KINDS), MB, 2)), dma((3, 2)), dma((3, 2)), dma((3,)), dma((2, 2))],
    }
    for kind in KINDS:
        slim = kind in ("gate", "ggrad")
        shape = (MB, G, 1, 128) if slim else (MB, G, CAP, D)
        scratch[kind] = [V(shape, F32 if slim else BF16)] * 2
    scratch["chunks"] = []
    early = EARLY if len(rows_of) > 1 else 0
    for n, rows in enumerate(rows_of):
        pr = rows // parts
        A, B = (Z, L) if n < early else (L, Z)
        scratch["chunks"].append(
            {
                "out": V((parts, pr, D), BF16),
                "l1": V((max(R - 1, 1), A * B, pr, D), BF16),
                "l2s": V((A, B, pr, D), BF16),
                "l2": V((max(A - 1, 1), B, pr, D), BF16),
                "l3s": V((B, pr, D), BF16),
                "l3": V((max(B - 1, 1), pr, D), BF16),
                "recv": dma((6,)),
            }
        )
    leaves, tree = jax.tree.flatten(scratch)
    results = (
        sds((SEQ, MB, D), F32),
        sds((SEQ, MB, D), F32),
        sds((D,), F32),
        sds((D, 3 * D), F32),
        sds((D, D), F32),
        sds((D,), F32),
        sds((G, D), F32),
        sds((L, FS, D), F32),
        sds((L, FS, D), F32),
    )
    n_in, n_out = len(operands), len(results)

    def body(*refs):
        ins, outs = refs[:n_in], refs[n_in : n_in + n_out]
        held = jax.tree.unflatten(tree, refs[n_in + n_out :])
        for ck, blocks, rows in zip(held["chunks"], groups_of_blocks, rows_of):
            ck["blocks"] = blocks
            ck["pr"] = rows // parts
            ck["z_first"] = len(rows_of) > 1 and blocks in groups_of_blocks[:early]
        kernel((L, R, Z, G, FF), ins, outs, held)

    held = pl.pallas_call(
        body,
        out_shape=results,
        in_specs=[hbm] * n_in,
        out_specs=[vmem] * n_out,
        scratch_shapes=leaves,
        compiler_params=pltpu.CompilerParams(
            collective_id=0, has_side_effects=True, vmem_limit_bytes=48 << 20
        ),
        name="block",
    )(*(pltpu.with_memory_space_constraint(a, pltpu.HBM) for a in operands))

    def put_out(*refs):
        ins, outs, sem = refs[:n_out], refs[n_out:-1], refs[-1]
        copies = [
            pltpu.make_async_copy(src, dst, sem.at[n])
            for n, (src, dst) in enumerate(zip(ins, outs))
        ]
        for copy in copies:
            copy.start()
        for copy in copies:
            copy.wait()

    bo, ig, gain1, wqkv, wattn, gain2, router, ein, eout = pl.pallas_call(
        put_out,
        out_shape=results,
        in_specs=[vmem] * n_out,
        out_specs=[hbm] * n_out,
        scratch_shapes=[dma((n_out,))],
        compiler_params=pltpu.CompilerParams(vmem_limit_bytes=1 << 20),
        name="put_out",
    )(*held)
    return (
        stored(bo),
        stored(ig),
        gain1,
        wqkv,
        wattn,
        gain2,
        router.T,
        jnp.transpose(ein, (0, 2, 1)),
        eout,
    )


def solution(mesh):
    rows = P(None, ("dp", "expert"), None)
    split = P("expert", None, None)
    return jax.shard_map(
        functools.partial(on_device, mesh.shape["expert"], mesh.shape["dp"]),
        mesh=mesh,
        in_specs=(
            rows,
            P(),
            P(),
            P(),
            P(),
            P(),
            split,
            split,
            rows,
            rows,
            rows,
            rows,
        ),
        out_specs=(
            rows,
            rows,
            P(),
            P(),
            P(),
            P(),
            P(),
            P("expert", None, "dp"),
            P("expert", "dp", None),
        ),
        check_vma=False,
    )
```

```python
import functools
import math

import jax
import jax.numpy as jnp
from jax import lax
from jax.experimental import pallas as pl
from jax.experimental.pallas import tpu as pltpu
from jax.sharding import PartitionSpec as P

D = 384
HEADS = 6
HD = 64
SEQ = 197
MB = 2
CAP = 16
EPS = 1e-06
TP = 208
TL = 256
SM = 8
ROWS = (256, 128, 128, 256, 256, 256, 256)
START = (0, 256, 384, 512, 768, 1024, 1280)
CHUNKS = ((0,), (1, 2), (3,), (4,), (5,), (6,))
F32 = jnp.float32
BF16 = jnp.bfloat16
MESH = pl.DeviceIdType.MESH
EARLY = 2
Z_TIMES = ((3.5, 1.5), (7.5, 1.5), (11.0, 1.5), (15.5, 1.2))
XY_TIMES = ((3.0, 0.9), (8.0, 0.9), (12.0, 0.8), (15.5, 0.8))
X_TIMES = (7.1, 8.2, 9.1, 10.0)
KINDS = ("rows", "gate", "pull", "ggrad", "back", "made")


def mm(a, b, ca=1, cb=0):
    return lax.dot_general(
        a, b, (((ca,), (cb,)), ((), ())), preferred_element_type=F32
    )


def mm_exact(a, b):
    return lax.dot_general(
        a,
        b,
        (((1,), (0,)), ((), ())),
        preferred_element_type=F32,
        precision=lax.Precision.HIGHEST,
    )


def normed_of(rows):
    mean = jnp.sum(rows, axis=-1, keepdims=True) * (1.0 / D)
    centered = rows - mean
    var = jnp.sum(centered * centered, axis=-1, keepdims=True) * (1.0 / D)
    rstd = lax.rsqrt(var + EPS)
    return centered * rstd, rstd


def norm_pull(hat, rstd, gain, grad):
    scaled = grad * gain
    m1 = jnp.sum(scaled, axis=-1, keepdims=True) * (1.0 / D)
    m2 = jnp.sum(scaled * hat, axis=-1, keepdims=True) * (1.0 / D)
    return rstd * (scaled - m1 - hat * m2)


def kernel(dims, ins, outs, scratch):
    L, R, Z, G, FF = dims
    S = G * CAP
    FS = FF // (L * R)
    (
        x_hbm,
        g_hbm,
        gain1_hbm,
        gain2_hbm,
        wqkv_hbm,
        wattn_hbm,
        wrt_hbm,
        ids_hbm,
        slot_hbm,
        drop_hbm,
        win_hbm,
        wout_hbm,
    ) = ins
    bo_ref, ig_ref, gain1_out, wqkv_out, wattn_out, gain2_out, router_out = outs[:7]
    ein_out, eout_out = outs[7:]
    xin_ref, gin_ref, gain1_ref, gain2_ref = scratch["loads"][:4]
    wqkv_ref, wattn_ref, wrt_ref = scratch["loads"][4:7]
    ids_ref, slot_ref, drop_ref, w1, w2 = scratch["loads"][7:]
    x_ref, g_ref, n1_ref, qkv_ref, p_ref, am_ref, res_ref, n2_ref = scratch["saved"]
    rs_ref, cols_ref, slope_ref, pick_ref = scratch["work"]
    act_ref, hg_ref, xg_ref, x1_ref, xs_ref, eg_ref, gacc_ref = scratch["expert"]
    dq_ref, held_rgrad, acc_ref, small_ref, t1_ref, t2_ref, t3_ref = scratch["grads"]
    lsem, esem, xsem, tsem, ssem, x1sem = scratch["sems"]
    sums_ref = scratch["sums"]
    chunks = scratch["chunks"]
    last = MB - 1
    dp = lax.axis_index("dp")
    z = lax.axis_index("expert")
    j = dp // R
    r = dp % R
    me = z * L + j

    def group_id(e):
        return ((e % L) * R + r, e // L)

    def plane_id(i):
        return (i * R + r, z)

    def part_id(rr):
        return (j * R + rr, z)

    def remote(src, dst, send_sem, recv_sem, device):
        pltpu.make_async_remote_copy(
            src_ref=src,
            dst_ref=dst,
            send_sem=send_sem,
            recv_sem=recv_sem,
            device_id=device,
            device_id_type=MESH,
        ).start()

    def wait_bytes(ref, sem):
        pltpu.make_async_copy(ref, ref, sem).wait()

    for n, ck in enumerate(chunks):
        ck["src"] = sums_ref.at[pl.ds(n * G * R, G * R)]
        plane = (j, L, plane_id)
        along = (z, Z, lambda i: (dp, i))
        ck["dims"] = (along, plane) if ck["z_first"] else (plane, along)

    barrier = pltpu.get_barrier_semaphore()

    @pl.loop(1, G)
    def _(o):
        pl.semaphore_signal(
            barrier, inc=1, device_id=group_id((me + o) % G), device_id_type=MESH
        )

    for o in range(1, R):
        pl.semaphore_signal(
            barrier, inc=1, device_id=part_id((r + o) % R), device_id_type=MESH
        )

    loads = []
    sources = [
        x_hbm,
        g_hbm,
        gain1_hbm,
        gain2_hbm,
        wqkv_hbm,
        wattn_hbm,
        wrt_hbm,
        ids_hbm,
        slot_hbm,
        drop_hbm,
        win_hbm.at[j],
        wout_hbm.at[j],
    ]
    for n, (src, dst) in enumerate(zip(sources, scratch["loads"])):
        loads.append(pltpu.make_async_copy(src, dst, lsem.at[n]))
    for n in (0, 2, 4, 7, 8, 9, 1, 5, 3, 6, 10, 11):
        loads[n].start()

    def ready(*which):
        for n in which:
            loads[n].wait()

    low_half = lax.broadcasted_iota(jnp.int32, (TP, 128), 1) < HD
    key_ok = lax.broadcasted_iota(jnp.int32, (TP, TP), 1) < SEQ
    slot_lane = lax.broadcasted_iota(
        jnp.int32, (G, CAP, 128), 2
    ) == lax.broadcasted_iota(jnp.int32, (G, CAP, 128), 1)

    def exchange(*which):
        legs = []
        for kind, mb in which:
            send, recv = scratch[kind]
            sems = esem.at[KINDS.index(kind), mb]
            legs.append((send.at[mb], recv.at[mb], sems))
        for send, recv, sems in legs:
            pltpu.make_async_copy(send.at[me], recv.at[me], sems.at[1]).start()

        @pl.loop(1, G, unroll=True)
        def _(o):
            e = (me + o) % G
            to = group_id(e)
            for send, recv, sems in legs:
                remote(send.at[e], recv.at[me], sems.at[0], sems.at[1], to)

    def for_core(core, what):
        pl.when(dp % 2 == core)(what)

    def left(*which):
        for kind, mb in which:
            sent = scratch[kind][0].at[mb, pl.ds(0, G - 1)]
            wait_bytes(sent, esem.at[KINDS.index(kind), mb, 0])

    def arrived(kind, mb):
        recv = scratch[kind][1].at[mb]
        wait_bytes(recv, esem.at[KINDS.index(kind), mb, 1])
        return recv

    def row_of_slots(col):
        spread = jnp.where(slot_lane, col.reshape(G, CAP, 1), 0.0)
        return jnp.sum(spread, axis=1, keepdims=True)

    def slots_of_row(row):
        spread = jnp.where(slot_lane, row, 0.0)
        return jnp.sum(spread, axis=-1, keepdims=True).reshape(S, 1)

    def route(mb):
        if mb == 0:
            ready(7, 8, 9, 1)
        g_ref[mb, TP - 16 : TP] = jnp.zeros((16, D), BF16)
        g_ref[mb, 0:SEQ] = gin_ref[:, mb, :]
        ids = ids_ref[mb]
        drop = drop_ref[mb]
        slot = slot_ref[mb]
        flat = jnp.where(drop == 0, ids * CAP + slot, S)
        rs_ref[mb] = jnp.zeros_like(rs_ref[mb])
        rs_ref[mb, G : G + 2, 0:TP] = jnp.full((2, TP), S, F32)
        rs_ref[mb, G : G + 2, 0:SEQ] = flat.astype(F32)
        rs_ref[mb, G + 2 : G + 4, 0:SEQ] = 1.0 - drop.astype(F32)
        rs_ref[mb, G + 4 : G + 6, 0:SEQ] = ids.astype(F32)
        rs_ref[mb, G + 8 : G + 10, 0:SEQ] = slot.astype(F32)
        slot_of = lax.broadcasted_iota(jnp.int32, (S, TP), 0).astype(F32)
        hit0 = slot_of == rs_ref[mb, G : G + 1, 0:TP]
        hit1 = slot_of == rs_ref[mb, G + 1 : G + 2, 0:TP]
        pick = jnp.where(hit0, 1.0, jnp.where(hit1, 1.0, 0.0)).astype(BF16)
        pick_ref[mb] = pick
        scratch["pull"][0][mb] = mm(pick, g_ref[mb]).astype(BF16).reshape(G, CAP, D)

    def project(mb):
        if mb == 0:
            ready(0, 2, 4)
        x_ref[mb, TP - 16 : TP] = jnp.zeros((16, D), F32)
        x_ref[mb, 0:SEQ] = xin_ref[:, mb, :].astype(F32)
        hat, _ = normed_of(x_ref[mb])
        n1 = (hat * gain1_ref[...].reshape(1, D)).astype(BF16)
        n1_ref[mb] = n1
        qkv_ref[mb] = mm(n1, wqkv_ref[...]).astype(BF16)

    def forward(mb):
        for pair in range(HEADS // 2):
            c = pair * 128
            q = qkv_ref[mb, :, c : c + 128] * jnp.asarray(HD**-0.5, BF16)
            k = qkv_ref[mb, :, D + c : D + c + 128]
            v = qkv_ref[mb, :, 2 * D + c : 2 * D + c + 128]
            mixed = []
            for half in range(2):
                mine = low_half if half == 0 else jnp.logical_not(low_half)
                qh = jnp.where(mine, q, jnp.zeros_like(q))
                s = mm(qh, k, 1, 1)
                s = jnp.where(key_ok, s, -1e30)
                e = jnp.exp(s - jnp.max(s, axis=-1, keepdims=True))
                p = e / jnp.sum(e, axis=-1, keepdims=True)
                p_ref[mb, 2 * pair + half] = p
                mixed.append(mm(p.astype(BF16), v))
            am_ref[mb, :, c : c + 128] = jnp.where(
                low_half, mixed[0], mixed[1]
            ).astype(BF16)
        if mb == 0:
            ready(5, 3, 6)
        res = x_ref[mb] + mm(am_ref[mb], wattn_ref[...])
        res_ref[mb] = res
        hat2, _ = normed_of(res)
        n2 = (hat2 * gain2_ref[...].reshape(1, D)).astype(BF16)
        n2_ref[mb] = n2
        logits = mm(wrt_ref[...], n2, 1, 1)
        ex = jnp.exp(logits - jnp.max(logits, axis=0, keepdims=True))
        gp = ex / jnp.sum(ex, axis=0, keepdims=True)
        rs_ref[mb, 0:G, 0:TP] = gp
        expert_of = lax.broadcasted_iota(jnp.int32, (G, TP), 0).astype(F32)
        slot_of = lax.broadcasted_iota(jnp.int32, (S, TP), 0).astype(F32)
        gcol = jnp.zeros((S, 1), F32)
        for kk in range(2):
            flr = rs_ref[mb, G + kk : G + kk + 1, 0:TP]
            keep = rs_ref[mb, G + 2 + kk : G + 3 + kk, 0:TP]
            idr = rs_ref[mb, G + 4 + kk : G + 5 + kk, 0:TP]
            mine = jnp.where(expert_of == idr, gp, 0.0)
            gate = jnp.sum(mine, axis=0, keepdims=True) * keep
            rs_ref[mb, G + 6 + kk : G + 7 + kk, 0:TP] = gate
            hit = slot_of == flr
            gcol = gcol + jnp.sum(jnp.where(hit, gate, 0.0), axis=-1, keepdims=True)
        scratch["rows"][0][mb] = mm(pick_ref[mb], n2).astype(BF16).reshape(G, CAP, D)
        scratch["gate"][0][mb] = row_of_slots(gcol)
        cols_ref[mb] = rs_ref[mb].T

    def experts(mb, halfway=None):
        if mb == last:
            arrived("rows", mb)
        xs = scratch["rows"][1][mb].reshape(S, D)
        step = 384
        produced = jnp.zeros((S, D), F32)
        for c in range(0, FF, step):
            h = mm(xs, w1[:, c : c + step])
            sq = h * h
            t = jnp.tanh(0.7978845608028654 * (h + 0.044715 * (h * sq)))
            half = 0.5 * (1.0 + t)
            act = (h * half).astype(BF16)
            slope_ref[:, c : c + step] = half + 0.5 * h * (1.0 - t * t) * (
                0.7978845608028654 * (1.0 + 0.134145 * sq)
            )
            act_ref[mb, :, c : c + step] = act
            produced = produced + mm(act, w2[c : c + step, :])
        produced = produced.astype(BF16)
        scratch["made"][0][mb] = produced.reshape(G, CAP, D)
        if halfway is not None:
            halfway()
        gates = slots_of_row(arrived("gate", mb)[...])
        grow = arrived("pull", mb)[...].reshape(S, D).astype(F32)
        pg = (gates * grow).astype(BF16)
        scratch["gated"][mb] = pg
        gg = jnp.sum(grow * produced.astype(F32), axis=-1, keepdims=True)
        scratch["ggrad"][0][mb] = row_of_slots(gg)
        back = jnp.zeros((S, D), F32)
        for c in range(0, FF, step):
            ag = mm(pg, w2[c : c + step, :], 1, 1)
            hg = (ag * slope_ref[:, c : c + step]).astype(BF16)
            hg_ref[mb, :, c : c + step] = hg
            back = back + mm(hg, w1[:, c : c + step], 1, 1)
        scratch["back"][0][mb] = back.astype(BF16).reshape(G, CAP, D)

    span = FF // L

    def weight_grads(mb, mats):
        xs = scratch["rows"][1][mb].reshape(S, D)
        pg = scratch["gated"][mb]

        def part(i, carry):
            at = pl.ds(pl.multiple_of(i * span, 128), span)
            for mat in mats:
                left_rows = (hg_ref, act_ref)[mat][mb, :, at]
                grad = mm(left_rows, (xs, pg)[mat], 0, 0)
                if mb > 0:
                    grad = grad + gacc_ref[mat, i]
                if mb < last:
                    gacc_ref[mat, i] = grad
                else:
                    grad = grad.astype(BF16)
                    for rr in range(R):
                        xg_ref[mat, rr, i] = grad[rr * FS : (rr + 1) * FS]
            return carry

        lax.fori_loop(0, L, part, 0)

    def swap_slices(mat):
        for o in range(1, R):
            rr = (r + o) % R
            remote(
                xg_ref.at[mat, rr],
                x1_ref.at[mat, R - o - 1],
                x1sem.at[mat, 0],
                x1sem.at[mat, 1],
                part_id(rr),
            )

    def add_slices(mat):
        if R > 1:
            wait_bytes(x1_ref.at[mat], x1sem.at[mat, 1])

        def part(i, carry):
            total = xg_ref[mat, r, i].astype(F32)
            for o in range(R - 1):
                total = total + x1_ref[mat, o, i].astype(F32)
            xs_ref[i, mat] = total.astype(BF16)
            return carry

        lax.fori_loop(0, L, part, 0)

    pieces = max(1, FS // 48)

    def hand_out(which):
        mat, piece = which
        rows = pl.ds(piece * (FS // pieces), FS // pieces)
        for o in range(1, L):
            i = (j + o) % L
            remote(
                xs_ref.at[i, mat, rows],
                eg_ref.at[j, mat, rows],
                xsem.at[1 + mat, 0],
                xsem.at[1 + mat, 1],
                plane_id(i),
            )
        pltpu.make_async_copy(
            xs_ref.at[j, mat, rows], eg_ref.at[j, mat, rows], xsem.at[1 + mat, 1]
        ).start()

    def slices_out(mat):
        wait_bytes(xs_ref.at[pl.ds(0, L), 0], xsem.at[1 + mat, 1])
        out = (ein_out, eout_out)[mat]

        def part(i, carry):
            out[i] = eg_ref[i, mat].astype(F32)
            return carry

        lax.fori_loop(0, L, part, 0)

    def chunk_of(block):
        for ck in chunks:
            at = 0
            for name in ck["blocks"]:
                if name == block:
                    return ck, at
                at += ROWS[name]

    def add_block(block, value):
        ck, at = chunk_of(block)
        src, pr = ck["src"], ck["pr"]
        at = at // pr
        count = ROWS[block] // pr
        if pr % 8 == 0:
            src[at : at + count] = value.reshape(count, pr, D).astype(BF16)
        else:
            first = START[block]
            acc_ref[first : first + ROWS[block]] = value
            rows = math.lcm(pr, 8)

            @pl.loop(0, ROWS[block] // rows)
            def _(n):
                piece = acc_ref[pl.ds(pl.multiple_of(first + n * rows, 8), rows)]
                piece = piece.astype(BF16)
                for m in range(rows // pr):
                    src[at + n * (rows // pr) + m] = piece[m * pr : (m + 1) * pr]

    def total_of(block):
        ck, at = chunk_of(block)
        out, pr = ck["out"], ck["pr"]
        at = at // pr
        count = ROWS[block] // pr
        if pr % 8 == 0:
            return out[at : at + count].astype(F32).reshape(ROWS[block], D)
        first = START[block]
        rows = math.lcm(pr, 8)

        @pl.loop(0, ROWS[block] // rows)
        def _(n):
            pieces = [out[at + n * (rows // pr) + m] for m in range(rows // pr)]
            spot = pl.ds(pl.multiple_of(first + n * rows, 8), rows)
            acc_ref[spot] = jnp.concatenate(
                [piece.astype(F32) for piece in pieces], axis=0
            )

        return acc_ref[first : first + ROWS[block]]

    def store_totals(ck):
        if R > 1:
            wait_bytes(ck["l1"], ck["recv"].at[5])
        for block in ck["blocks"]:
            total = total_of(block)
            if block < 2:
                wattn_out[START[block] : START[block] + ROWS[block]] = total
            elif block < 4:
                first = START[block] - D
                wqkv_out[first : first + ROWS[block], 2 * D : 3 * D] = total
            else:
                for n in range(2):
                    c = n * D + (block - 4) * 128
                    for m in range(3):
                        wqkv_out[m * 128 : (m + 1) * 128, c : c + 128] = total[
                            n * 128 : (n + 1) * 128, m * 128 : (m + 1) * 128
                        ]

    def sum_start(ck):
        (_, A, _), (_, B, _) = ck["dims"]
        for o in range(1, R):
            rr = (r + o) % R
            remote(
                ck["src"].at[pl.ds(rr * A * B, A * B)],
                ck["l1"].at[R - o - 1],
                ssem.at[0],
                ck["recv"].at[0],
                part_id(rr),
            )

    def sum_pairs(ck):
        (a, A, ident), (_, B, _) = ck["dims"]
        if R > 1:
            wait_bytes(ck["l1"], ck["recv"].at[0])
        for n in range(1, A + 1):
            i = (a + n) % A
            total = ck["src"][pl.ds((r * A + i) * B, B)].astype(F32)
            for o in range(R - 1):
                total = total + ck["l1"][o, pl.ds(i * B, B)].astype(F32)
            ck["l2s"][i] = total.astype(BF16)
            if n < A:
                remote(
                    ck["l2s"].at[i],
                    ck["l2"].at[A - n - 1],
                    ssem.at[0],
                    ck["recv"].at[1],
                    ident(i),
                )

    def sum_first(ck):
        (a, A, _), (b, B, ident) = ck["dims"]
        if A > 1:
            wait_bytes(ck["l2"], ck["recv"].at[1])
        for n in range(B - 1, -1, -1):
            i = (b + n) % B
            total = ck["l2s"][a, i].astype(F32)
            for o in range(A - 1):
                total = total + ck["l2"][o, i].astype(F32)
            ck["l3s"][i] = total.astype(BF16)
            if n > 0:
                remote(
                    ck["l3s"].at[i],
                    ck["l3"].at[B - n - 1],
                    ssem.at[1],
                    ck["recv"].at[2],
                    ident(i),
                )

    def sum_second(ck):
        (a, A, _), (b, B, ident) = ck["dims"]
        out = ck["out"]
        if B > 1:
            wait_bytes(ck["l3"], ck["recv"].at[2])
        total = ck["l3s"][b].astype(F32)
        for o in range(B - 1):
            total = total + ck["l3"][o].astype(F32)
        mine = (r * A + a) * B + b
        out[mine] = total.astype(BF16)
        for n in range(B - 1, 0, -1):
            remote(
                out.at[mine],
                out.at[mine],
                ssem.at[1],
                ck["recv"].at[3],
                ident((b + n) % B),
            )

    def spread_first(ck):
        (a, A, ident), (_, B, _) = ck["dims"]
        out = ck["out"]
        if B > 1:
            wait_bytes(ck["l3"], ck["recv"].at[3])
        mine = pl.ds((r * A + a) * B, B)
        for n in range(1, A):
            remote(
                out.at[mine],
                out.at[mine],
                ssem.at[1],
                ck["recv"].at[4],
                ident((a + n) % A),
            )

    def spread_parts(ck):
        (_, A, _), (_, B, _) = ck["dims"]
        out = ck["out"]
        if A > 1:
            wait_bytes(ck["l2"], ck["recv"].at[4])
        mine = pl.ds(r * A * B, A * B)
        for o in range(1, R):
            remote(
                out.at[mine],
                out.at[mine],
                ssem.at[2],
                ck["recv"].at[5],
                part_id((r + o) % R),
            )

    def sums_left():
        counts = [0, 0, 0]
        for ck in chunks:
            (_, A, _), (_, B, _) = ck["dims"]
            counts[0] += (R - 1) * A * B + (A - 1) * B
            counts[1] += 2 * (B - 1) + (A - 1) * B
            counts[2] += (R - 1) * A * B
        for n, total in enumerate(counts):
            if total:
                wait_bytes(sums_ref.at[pl.ds(0, total)], ssem.at[n])

    levels = ((t1_ref, r, R, part_id), (t2_ref, j, L, plane_id), (t3_ref, z, Z, None))

    def small_start(level):
        buf, at, count, ident = levels[level]
        for o in range(1, count):
            to = (at + o) % count
            remote(
                buf.at[at],
                buf.at[at],
                tsem.at[level, 0],
                tsem.at[level, 1],
                (dp, to) if ident is None else ident(to),
            )

    def small_sum(level):
        buf, _, count, _ = levels[level]
        if count > 1:
            wait_bytes(buf.at[pl.ds(0, count - 1)], tsem.at[level, 1])
        total = buf[0].astype(F32)
        for n in range(1, count):
            total = total + buf[n].astype(F32)
        return total

    def small_next(level):
        total = small_sum(level)
        buf, at, _, _ = levels[level + 1]
        buf[at] = total.astype(BF16)
        small_start(level + 1)

    def small_end():
        total = small_sum(2)
        router_out[...] = total[0:G]
        gain2_out[...] = total[G]
        gain1_out[...] = total[G + 1]
        for level in range(3):
            buf, _, count, _ = levels[level]
            if count > 1:
                wait_bytes(buf.at[pl.ds(0, count - 1)], tsem.at[level, 0])

    def add_grad(mb, block, value):
        at = slice(START[block], START[block] + ROWS[block])
        if mb > 0:
            value = value + acc_ref[at]
        if mb < last:
            acc_ref[at] = value
        else:
            add_block(block, value)

    def add_small(mb, at, value):
        small_ref[at] += value

    def cols_of(mb):
        cols = cols_ref[mb][0:TP]
        col = lambda n: cols[:, n : n + 1]
        return cols, col

    def backward(mb):
        cols, col = cols_of(mb)
        ggr = arrived("ggrad", mb)[...].reshape(G, 128)
        g = g_ref[mb].astype(F32)
        res = res_ref[mb]
        slot_at = lax.broadcasted_iota(jnp.int32, (TP, S), 1).astype(F32)
        lane_at = lax.broadcasted_iota(jnp.int32, (TP, 128), 1).astype(F32)
        expert_at = lax.broadcasted_iota(jnp.int32, (TP, G), 1).astype(F32)
        gp = cols[:, 0:G]
        gates_grad = jnp.zeros((TP, G), F32)
        pick = jnp.zeros((TP, S), F32)
        for kk in range(2):
            keep = col(G + 2 + kk)
            named = jnp.where(expert_at == col(G + 4 + kk), 1.0, 0.0)
            of_slot = jnp.where(
                lane_at == col(G + 8 + kk), mm_exact(named, ggr), 0.0
            )
            gate_grad = jnp.sum(of_slot, axis=-1, keepdims=True) * keep
            gates_grad = gates_grad + named * gate_grad
            pick = pick + jnp.where(slot_at == col(G + kk), 1.0, 0.0)
        inner = jnp.sum(gp * gates_grad, axis=-1, keepdims=True)
        logit_grad = (gp * (gates_grad - inner)).astype(BF16)
        add_small(mb, slice(0, G), mm(logit_grad, n2_ref[mb], 0, 0))
        bgr = arrived("back", mb)[...].reshape(S, D)
        ngrad = mm(pick.astype(BF16), bgr) + mm(logit_grad, wrt_ref[...])
        hat2, rstd2 = normed_of(res)
        add_small(
            mb, slice(G, G + 1), jnp.sum(ngrad * hat2, axis=0, keepdims=True)
        )
        gain2 = gain2_ref[...].reshape(1, D)
        rgrad = g + norm_pull(hat2, rstd2, gain2, ngrad)
        branch = rgrad.astype(BF16)
        piped = mb == last and len(chunks) > 1
        wgrad = mm(am_ref[mb], branch, 0, 0)
        add_grad(mb, 0, wgrad[0:256])
        add_grad(mb, 1, wgrad[256:D])
        if piped:
            sum_start(chunks[0])
        if mb == last - 1:
            add_slices(0)
            for piece in range(pieces):
                hand_out((0, piece))
        mgrad = mm(branch, wattn_ref[...], 1, 1).astype(BF16)
        for pair in range(HEADS // 2):
            c = pair * 128
            mg = mgrad[:, c : c + 128]
            dvs = [
                mm(p_ref[mb, 2 * pair + half].astype(BF16), mg, 0, 0)
                for half in range(2)
            ]
            dq_ref[mb, :, 2 * D + c : 2 * D + c + 128] = jnp.where(
                low_half, dvs[0], dvs[1]
            ).astype(BF16)
        n1 = n1_ref[mb]
        wgrad = mm(n1, dq_ref[mb, :, 2 * D : 3 * D], 0, 0)
        add_grad(mb, 2, wgrad[0:128])
        add_grad(mb, 3, wgrad[128:D])
        if piped:
            sum_start(chunks[1])
            sum_start(chunks[2])
            sum_pairs(chunks[0])
        for pair in range(HEADS // 2):
            c = pair * 128
            q = qkv_ref[mb, :, c : c + 128]
            k = qkv_ref[mb, :, D + c : D + c + 128]
            v = qkv_ref[mb, :, 2 * D + c : 2 * D + c + 128]
            mg = mgrad[:, c : c + 128]
            dqs, dks = [], []
            for half in range(2):
                mine = low_half if half == 0 else jnp.logical_not(low_half)
                mgh = jnp.where(mine, mg, jnp.zeros_like(mg))
                p = p_ref[mb, 2 * pair + half]
                dp_ = mm(mgh, v, 1, 1)
                delta = jnp.sum(p * dp_, axis=-1, keepdims=True)
                ds = (p * (dp_ - delta) * HD**-0.5).astype(BF16)
                dqs.append(mm(ds, k))
                dks.append(mm(ds, q, 0, 0))
            grads = [
                jnp.where(low_half, parts[0], parts[1]).astype(BF16)
                for parts in (dqs, dks)
            ]
            for n in range(2):
                dq_ref[mb, :, n * D + c : n * D + c + 128] = grads[n]
            wgrad = mm(n1, jnp.concatenate(grads, axis=1), 0, 0)
            packed = jnp.concatenate(
                [
                    jnp.concatenate(
                        [
                            wgrad[m * 128 : (m + 1) * 128, n * 128 : (n + 1) * 128]
                            for m in range(3)
                        ],
                        axis=1,
                    )
                    for n in range(2)
                ],
                axis=0,
            )
            add_grad(mb, 4 + pair, packed)
            if piped:
                sum_start(chunks[3 + pair])
                sum_pairs(chunks[1 + pair])
        if mb == last and not piped:
            sum_start(chunks[0])
        held_rgrad[mb] = rgrad

    def finish(mb):
        fgrad = mm(dq_ref[mb], wqkv_ref[...], 1, 1)
        hat, rstd = normed_of(x_ref[mb])
        add_small(
            mb, slice(G + 1, G + 2), jnp.sum(fgrad * hat, axis=0, keepdims=True)
        )
        gain1 = gain1_ref[...].reshape(1, D)
        grad = held_rgrad[mb] + norm_pull(hat, rstd, gain1, fgrad)
        ig_ref[:, mb, :] = grad[0:SEQ]

    def combine(mb):
        _, col = cols_of(mb)
        made = arrived("made", mb)[...].reshape(S, D)
        slot_at = lax.broadcasted_iota(jnp.int32, (TP, S), 1).astype(F32)
        out = res_ref[mb]
        for kk in range(2):
            pick = jnp.where(slot_at == col(G + kk), 1.0, 0.0).astype(BF16)
            out = out + col(G + 6 + kk) * mm(pick, made)
        bo_ref[:, mb, :] = out[0:SEQ]

    project(0)
    route(0)
    pl.semaphore_wait(barrier, G - 1 + R - 1)
    exchange(("pull", 0))
    forward(0)
    exchange(("rows", 0), ("gate", 0))
    for mb in range(1, MB):
        project(mb)
        route(mb)
        forward(mb)
        for_core(0, lambda: exchange(("rows", mb), ("gate", mb)))
        arrived("rows", mb - 1)
        for_core(1, lambda: exchange(("rows", mb), ("gate", mb)))
        for_core(0, lambda: exchange(("pull", mb)))
    ready(10, 11)
    experts(0)
    for_core(1, lambda: exchange(("pull", last)))
    exchange(("ggrad", 0))
    weight_grads(0, (0, 1))
    for_core(0, lambda: exchange(("back", 0)))
    for mb in range(1, MB):
        experts(mb, lambda: for_core(1, lambda: exchange(("back", mb - 1))))
        exchange(("ggrad", mb))
        exchange(("back", mb))
        weight_grads(mb, (0, 1))
    swap_slices(0)
    swap_slices(1)
    exchange(*(("made", mb) for mb in range(last)))
    small_ref[...] = jnp.zeros_like(small_ref)
    sent_early = min(0, pieces)
    for mb in range(MB):
        backward(mb)
        if mb == last - 1:
            add_slices(1)
            for piece in range(sent_early):
                hand_out((1, piece))

    def small_begin():
        t1_ref[r] = small_ref[...].astype(BF16)
        small_start(0)

    plan = []
    count = len(chunks)
    early = sum(ck["z_first"] for ck in chunks)
    for n, ck in enumerate(chunks):
        if n >= count - 2 or count == 1:
            plan.append((0.1 * (n - count), sum_pairs, ck))
        if ck["z_first"]:
            times = [t + s * n for t, s in Z_TIMES]
        else:
            times = [t + s * (n - early) for t, s in XY_TIMES]
        steps = (sum_first, sum_second, spread_first, spread_parts)
        plan.extend((when, step, ck) for when, step in zip(times, steps))
        plan.append((times[3] + 1.2, store_totals, ck))
    for piece in range(sent_early, pieces):
        plan.append((X_TIMES[piece % 4], hand_out, (1, piece)))
    plan.append((-0.15, finish, last))
    for mb in range(last):
        plan.append((0.5, finish, mb))
    plan.append((0.6, lambda _: small_begin(), 0))
    plan.append((0.5, lambda _: exchange(("made", last)), 0))
    plan.append((7.0, combine, 0))
    plan.append((5.8, small_next, 0))
    for mb in range(1, MB):
        plan.append((10.0, combine, mb))
    plan.append((10.7, small_next, 1))
    plan.append((9.2, slices_out, 0))
    plan.append((17.0, slices_out, 1))
    plan.append((17.1, lambda _: small_end(), 0))
    for when, what, which in sorted(plan, key=lambda step: step[0]):
        what(which)
    sums_left()

    for mat in range(2):
        if L > 1:
            wait_bytes(xs_ref.at[pl.ds(0, L - 1), 0], xsem.at[1 + mat, 0])
        if R > 1:
            wait_bytes(x1_ref.at[mat], x1sem.at[mat, 0])
    for mb in range(MB):
        left(("rows", mb), ("gate", mb), ("ggrad", mb), ("made", mb))
        left(("back", mb))
    left(*(("pull", mb) for mb in range(MB)))


def on_device(
    groups,
    replicas,
    inputs,
    first_gain,
    w_qkv,
    w_attn,
    second_gain,
    w_router,
    expert_in,
    expert_out,
    expert_ids,
    slot_ids,
    dropped,
    out_grad,
):
    L, _, FF = expert_in.shape
    Z = groups
    R = replicas // L
    G = L * Z
    S = G * CAP
    FS = FF // replicas
    parts = R * L * Z
    groups_of_blocks = CHUNKS
    if any(sum(ROWS[n] for n in blocks) % (8 * parts) for blocks in CHUNKS):
        groups_of_blocks = [tuple(range(len(ROWS)))]
    rows_of = [sum(ROWS[n] for n in blocks) for blocks in groups_of_blocks]
    small_rows = -(-(G + 2) // SM) * SM
    rs_rows = -(-(G + 10) // 8) * 8
    swap = lambda a: jnp.transpose(a, (0, 2, 1))
    stored = lambda a: jnp.transpose(a, (1, 0, 2))
    operands = (
        stored(inputs),
        stored(out_grad),
        first_gain,
        second_gain,
        w_qkv,
        w_attn,
        w_router.T,
        swap(expert_ids),
        swap(slot_ids),
        swap(dropped),
        expert_in,
        expert_out,
    )
    vmem = pl.BlockSpec(memory_space=pltpu.VMEM)
    hbm = pl.BlockSpec(memory_space=pltpu.HBM)
    sds = jax.ShapeDtypeStruct
    V = pltpu.VMEM
    dma = pltpu.SemaphoreType.DMA
    scratch = {
        "loads": [V(a.shape, a.dtype) for a in operands[:10]]
        + [V((D, FF), BF16), V((FF, D), BF16)],
        "saved": [
            V((MB, TP, D), F32),
            V((MB, TP, D), BF16),
            V((MB, TP, D), BF16),
            V((MB, TP, 3 * D), BF16),
            V((MB, HEADS, TP, TP), F32),
            V((MB, TP, D), BF16),
            V((MB, TP, D), F32),
            V((MB, TP, D), BF16),
        ],
        "work": [
            V((MB, rs_rows, TL), F32),
            V((MB, TL, rs_rows), F32),
            V((S, FF), F32),
            V((MB, S, TP), BF16),
        ],
        "expert": [
            V((MB, S, FF), BF16),
            V((MB, S, FF), BF16),
            V((2, R, L, FS, D), BF16),
            V((2, max(R - 1, 1), L, FS, D), BF16),
            V((L, 2, FS, D), BF16),
            V((L, 2, FS, D), BF16),
            V((2, L, FF // L, D), F32),
        ],
        "grads": [
            V((MB, TP, 3 * D), BF16),
            V((MB, TP, D), F32),
            V((4 * D, D), F32),
            V((small_rows, D), F32),
            V((R, small_rows, D), BF16),
            V((L, small_rows, D), BF16),
            V((Z, small_rows, D), BF16),
        ],
        "gated": V((MB, S, D), BF16),
        "sums": V((parts * len(rows_of), rows_of[0] // parts, D), BF16),
        "sems": [dma((12,)), dma((len(KINDS), MB, 2)), dma((3, 2)), dma((3, 2)), dma((3,)), dma((2, 2))],
    }
    for kind in KINDS:
        slim = kind in ("gate", "ggrad")
        shape = (MB, G, 1, 128) if slim else (MB, G, CAP, D)
        scratch[kind] = [V(shape, F32 if slim else BF16)] * 2
    scratch["chunks"] = []
    early = EARLY if len(rows_of) > 1 else 0
    for n, rows in enumerate(rows_of):
        pr = rows // parts
        A, B = (Z, L) if n < early else (L, Z)
        scratch["chunks"].append(
            {
                "out": V((parts, pr, D), BF16),
                "l1": V((max(R - 1, 1), A * B, pr, D), BF16),
                "l2s": V((A, B, pr, D), BF16),
                "l2": V((max(A - 1, 1), B, pr, D), BF16),
                "l3s": V((B, pr, D), BF16),
                "l3": V((max(B - 1, 1), pr, D), BF16),
                "recv": dma((6,)),
            }
        )
    leaves, tree = jax.tree.flatten(scratch)
    results = (
        sds((SEQ, MB, D), F32),
        sds((SEQ, MB, D), F32),
        sds((D,), F32),
        sds((D, 3 * D), F32),
        sds((D, D), F32),
        sds((D,), F32),
        sds((G, D), F32),
        sds((L, FS, D), F32),
        sds((L, FS, D), F32),
    )
    n_in, n_out = len(operands), len(results)

    def body(*refs):
        ins, outs = refs[:n_in], refs[n_in : n_in + n_out]
        held = jax.tree.unflatten(tree, refs[n_in + n_out :])
        for ck, blocks, rows in zip(held["chunks"], groups_of_blocks, rows_of):
            ck["blocks"] = blocks
            ck["pr"] = rows // parts
            ck["z_first"] = len(rows_of) > 1 and blocks in groups_of_blocks[:early]
        kernel((L, R, Z, G, FF), ins, outs, held)

    held = pl.pallas_call(
        body,
        out_shape=results,
        in_specs=[hbm] * n_in,
        out_specs=[vmem] * n_out,
        scratch_shapes=leaves,
        compiler_params=pltpu.CompilerParams(
            collective_id=0, has_side_effects=True, vmem_limit_bytes=48 << 20
        ),
        name="block",
    )(*(pltpu.with_memory_space_constraint(a, pltpu.HBM) for a in operands))

    def put_out(*refs):
        ins, outs, sem = refs[:n_out], refs[n_out:-1], refs[-1]
        copies = [
            pltpu.make_async_copy(src, dst, sem.at[n])
            for n, (src, dst) in enumerate(zip(ins, outs))
        ]
        for copy in copies:
            copy.start()
        for copy in copies:
            copy.wait()

    bo, ig, gain1, wqkv, wattn, gain2, router, ein, eout = pl.pallas_call(
        put_out,
        out_shape=results,
        in_specs=[vmem] * n_out,
        out_specs=[hbm] * n_out,
        scratch_shapes=[dma((n_out,))],
        compiler_params=pltpu.CompilerParams(vmem_limit_bytes=1 << 20),
        name="put_out",
    )(*held)
    return (
        stored(bo),
        stored(ig),
        gain1,
        wqkv,
        wattn,
        gain2,
        router.T,
        jnp.transpose(ein, (0, 2, 1)),
        eout,
    )


def solution(mesh):
    rows = P(None, ("dp", "expert"), None)
    split = P("expert", None, None)
    return jax.shard_map(
        functools.partial(on_device, mesh.shape["expert"], mesh.shape["dp"]),
        mesh=mesh,
        in_specs=(
            rows,
            P(),
            P(),
            P(),
            P(),
            P(),
            split,
            split,
            rows,
            rows,
            rows,
            rows,
        ),
        out_specs=(
            rows,
            rows,
            P(),
            P(),
            P(),
            P(),
            P(),
            P("expert", None, "dp"),
            P("expert", "dp", None),
        ),
        check_vma=False,
    )
```
